32 devices in a mesh: dp: 8 (over z, y), ep: 4 (over x, core).
Axes of the slice: x: 2, y: 2, z: 4, core: 2. Of those that a mesh axis runs over, the one named last changes fastest.
Arguments:
- x_tokens: bfloat16 [64, 512, 256], P(('dp', 'ep'))
- dy_tokens: bfloat16 [64, 512, 256], P(('dp', 'ep'))
- route_idx: int32 [64, 512, 8], P(('dp', 'ep'))
- norm1_gain: bfloat16 [256], replicated
- norm2_gain: bfloat16 [256], replicated
- w_qkv: bfloat16 [256, 768], replicated
- w_attn_out: bfloat16 [256, 256], replicated
- w_router: bfloat16 [256, 128], replicated
- w_gate: bfloat16 [128, 256, 768], P('ep')
- w_up: bfloat16 [128, 256, 768], P('ep')
- w_down: bfloat16 [128, 768, 256], P('ep')
Outputs:
- output 1: bfloat16 [64, 512, 256], P(('dp', 'ep'))
- output 2: float32 [256], replicated
- output 3: float32 [256], replicated
- output 4: float32 [256, 768], replicated
- output 5: float32 [256, 256], replicated
- output 6: float32 [256, 128], replicated
- output 7: float32 [128, 256, 768], P('ep')
- output 8: float32 [128, 256, 768], P('ep')
- output 9: float32 [128, 768, 256], P('ep')
All inputs are finite; a program needn't handle non-finite values.
Results may differ from the reference program's by a relative error of at most 0.0169938.
Values are sent between devices in bfloat16 or wider.
A program may use at most 1 GiB of HBM per device.

```python
import jax
import jax.numpy as jnp
from jax import lax

D = 256
HEAD_DIM = 128
FF = 768
EXPERTS = 128
TOP = 8
SEQ = 512
SEQS = 2
DEVICES = 32

TOKENS = SEQS * SEQ
BATCH = DEVICES * SEQS
CAP = 8 * ((5 * TOKENS * TOP + 32 * EXPERTS - 1) // (32 * EXPERTS))
HOT_ROWS = CAP + CAP // 4
EPS = 1e-6
ROPE_BASE = 10000.0


def draw_routes(route_key):
    score_key, hot_key = jax.random.split(route_key)
    base_scores = jax.random.randint(score_key, (BATCH, SEQ, EXPERTS), 0, 2 ** 20, jnp.int32)
    hot_expert = jax.random.randint(hot_key, (DEVICES,), 0, EXPERTS, jnp.int32)
    expert_ids = jnp.arange(EXPERTS, dtype=jnp.int32)
    seq_ids = jnp.arange(BATCH, dtype=jnp.int32)
    local_pos = (seq_ids % SEQS)[:, None] * SEQ + jnp.arange(SEQ, dtype=jnp.int32)[None, :]
    hot_of_seq = hot_expert[seq_ids // SEQS]
    forced = (local_pos < HOT_ROWS)[:, :, None] & (expert_ids[None, None, :] == hot_of_seq[:, None, None])
    scores = base_scores * EXPERTS + expert_ids[None, None, :] + jnp.where(forced, 2 ** 29, 0)
    return lax.top_k(scores, TOP)[1].astype(jnp.int32)


def scaled_normal(draw_key, shape_dims, factor):
    return (jax.random.normal(draw_key, shape_dims, jnp.float32) * factor).astype(jnp.bfloat16)


def setup_inputs(seed: int = 0) -> dict:
    key_list = jax.random.split(jax.random.key(seed), 11)
    return {
        'x_tokens': scaled_normal(key_list[0], (BATCH, SEQ, D), 1.0),
        'dy_tokens': scaled_normal(key_list[1], (BATCH, SEQ, D), 1.0),
        'route_idx': draw_routes(key_list[2]),
        'norm1_gain': (1.0 + 0.3 * jax.random.normal(key_list[3], (D,), jnp.float32)).astype(jnp.bfloat16),
        'norm2_gain': (1.0 + 0.3 * jax.random.normal(key_list[4], (D,), jnp.float32)).astype(jnp.bfloat16),
        'w_qkv': scaled_normal(key_list[5], (D, 3 * D), D ** -0.5),
        'w_attn_out': scaled_normal(key_list[6], (D, D), D ** -0.5),
        'w_router': scaled_normal(key_list[7], (D, EXPERTS), D ** -0.5),
        'w_gate': scaled_normal(key_list[8], (EXPERTS, D, FF), D ** -0.5),
        'w_up': scaled_normal(key_list[9], (EXPERTS, D, FF), D ** -0.5),
        'w_down': scaled_normal(key_list[10], (EXPERTS, FF, D), FF ** -0.5),
    }


def mat_f32(left, right):
    return jnp.dot(left.astype(jnp.float32), right.astype(jnp.float32), preferred_element_type=jnp.float32)


def rms_norm(x_rows, gain_vec):
    x_f32 = x_rows.astype(jnp.float32)
    inv_rms = lax.rsqrt(jnp.mean(x_f32 * x_f32, axis=-1, keepdims=True) + EPS)
    return (x_f32 * inv_rms * gain_vec.astype(jnp.float32)).astype(jnp.bfloat16)


def rope_rotate(head_vals):
    seq_len = head_vals.shape[1]
    half_dim = head_vals.shape[-1] // 2
    inv_freq = ROPE_BASE ** (-jnp.arange(half_dim, dtype=jnp.float32) / half_dim)
    angles = jnp.arange(seq_len, dtype=jnp.float32)[:, None] * inv_freq[None, :]
    cos_b = jnp.cos(angles)[None, :, None, :]
    sin_b = jnp.sin(angles)[None, :, None, :]
    lower_half = head_vals[..., :half_dim]
    upper_half = head_vals[..., half_dim:]
    return jnp.concatenate([lower_half * cos_b - upper_half * sin_b, upper_half * cos_b + lower_half * sin_b], axis=-1)


def gate_probs(logits, idx_rows):
    probs_all = jax.nn.softmax(logits, axis=-1)
    picked = jnp.take_along_axis(probs_all, idx_rows, axis=1)
    return picked / jnp.sum(picked, axis=1, keepdims=True)


def route_slots(idx_rows, num_experts, capacity):
    num_tokens, top_k = idx_rows.shape
    hit_count = jnp.sum((idx_rows[:, :, None] == jnp.arange(num_experts)[None, None, :]).astype(jnp.int32), axis=1)
    earlier = jnp.cumsum(hit_count, axis=0) - hit_count
    position = jnp.take_along_axis(earlier, idx_rows, axis=1)
    slot_ids = jnp.where(position < capacity, idx_rows * capacity + position, num_experts * capacity)
    source_ids = jnp.full((num_experts * capacity,), num_tokens * top_k, jnp.int32).at[slot_ids.reshape(-1)].set(jnp.arange(num_tokens * top_k, dtype=jnp.int32), mode='drop')
    return slot_ids, source_ids


def take_rows(table, row_ids):
    return jnp.take(table, row_ids, axis=0, mode='fill', fill_value=0)


def device_layer(weight_set, x_rows, idx_rows):
    norm1_gain, norm2_gain, w_qkv, w_attn_out, w_router, w_gate, w_up, w_down = weight_set
    normed1 = rms_norm(x_rows, norm1_gain)
    qkv_heads = mat_f32(normed1, w_qkv).reshape(SEQS, SEQ, 3, D // HEAD_DIM, HEAD_DIM)
    query_rot = rope_rotate(qkv_heads[:, :, 0]).astype(jnp.bfloat16).astype(jnp.float32)
    key_rot = rope_rotate(qkv_heads[:, :, 1]).astype(jnp.bfloat16).astype(jnp.float32)
    value_h = qkv_heads[:, :, 2].astype(jnp.bfloat16).astype(jnp.float32)
    scores = jnp.einsum('bqhd,bkhd->bhqk', query_rot, key_rot) * HEAD_DIM ** -0.5
    causal = jnp.arange(SEQ)[:, None] >= jnp.arange(SEQ)[None, :]
    attn_probs = jax.nn.softmax(jnp.where(causal, scores, -1e30), axis=-1).astype(jnp.bfloat16).astype(jnp.float32)
    context = jnp.einsum('bhqk,bkhd->bqhd', attn_probs, value_h).astype(jnp.bfloat16).reshape(TOKENS, D)
    h_rows = (x_rows.astype(jnp.float32) + mat_f32(context, w_attn_out)).astype(jnp.bfloat16)
    normed2 = rms_norm(h_rows, norm2_gain)
    gate_vals = gate_probs(mat_f32(normed2, w_router), idx_rows)
    slot_ids, source_ids = route_slots(idx_rows, EXPERTS, CAP)
    slot_rows = take_rows(normed2, source_ids // TOP).reshape(EXPERTS, CAP, D).astype(jnp.float32)
    act_gate = jnp.einsum('ecd,edf->ecf', slot_rows, w_gate)
    act_up = jnp.einsum('ecd,edf->ecf', slot_rows, w_up)
    hidden = (jax.nn.silu(act_gate) * act_up).astype(jnp.bfloat16).astype(jnp.float32)
    expert_out = jnp.einsum('ecf,efd->ecd', hidden, w_down).astype(jnp.bfloat16).reshape(EXPERTS * CAP, D)
    choice_rows = take_rows(expert_out, slot_ids.reshape(-1)).reshape(TOKENS, TOP, D)
    moe_out = jnp.sum(gate_vals[:, :, None] * choice_rows.astype(jnp.float32), axis=1)
    return (h_rows.astype(jnp.float32) + moe_out).astype(jnp.bfloat16)


def reference(x_tokens, dy_tokens, route_idx, norm1_gain, norm2_gain, w_qkv, w_attn_out, w_router, w_gate, w_up, w_down):
    weight_set = tuple(weight_arr.astype(jnp.float32) for weight_arr in (norm1_gain, norm2_gain, w_qkv, w_attn_out, w_router, w_gate, w_up, w_down))
    x_dev = x_tokens.reshape(DEVICES, TOKENS, D)
    dy_dev = dy_tokens.reshape(DEVICES, TOKENS, D)
    idx_dev = route_idx.reshape(DEVICES, TOKENS, TOP)

    def device_step(totals, per_device):
        x_rows, dy_rows, idx_rows = per_device
        pullback = jax.vjp(lambda weights_in, x_in: device_layer(weights_in, x_in, idx_rows), weight_set, x_rows)[1]
        d_weights, d_x = pullback(dy_rows)
        return jax.tree.map(lambda a, b: a + b, totals, d_weights), d_x

    zero_set = tuple(jnp.zeros_like(weight_arr) for weight_arr in weight_set)
    totals, d_x_dev = lax.scan(device_step, zero_set, (x_dev, dy_dev, idx_dev))
    return (d_x_dev.reshape(x_tokens.shape), totals[0], totals[1], totals[2], totals[3], totals[4], totals[5], totals[6], totals[7])
```

```python
import functools

import jax
import jax.numpy as jnp
from jax import lax
from jax.experimental import pallas as pl
from jax.experimental.pallas import tpu as pltpu
from jax.sharding import PartitionSpec as P


F32 = jnp.float32
BF16 = jnp.bfloat16
EPS = 1e-6
HEAD_DIM = 128
ROPE_BASE = 10000.0


def capacity_rows(num_tokens, top_k, num_experts):
    return 8 * ((5 * num_tokens * top_k + 32 * num_experts - 1) // (32 * num_experts))


def rms_norm(x_rows, gain_vec):
    x_f32 = x_rows.astype(jnp.float32)
    inv_rms = lax.rsqrt(jnp.mean(x_f32 * x_f32, axis=-1, keepdims=True) + EPS)
    return (x_f32 * inv_rms * gain_vec.astype(jnp.float32)).astype(jnp.bfloat16)


def rms_norm_bwd(x_rows, gain_vec, d_out):
    x_f32 = x_rows.astype(jnp.float32)
    inv_rms = lax.rsqrt(jnp.mean(x_f32 * x_f32, axis=-1, keepdims=True) + EPS)
    d_gain = jnp.sum(d_out * x_f32 * inv_rms, axis=0)
    d_scaled = d_out * gain_vec.astype(jnp.float32)
    d_x = inv_rms * d_scaled - x_f32 * inv_rms ** 3 * jnp.mean(d_scaled * x_f32, axis=-1, keepdims=True)
    return d_x, d_gain


def rope_rotate(head_vals):
    seq_len = head_vals.shape[1]
    half_dim = head_vals.shape[-1] // 2
    inv_freq = ROPE_BASE ** (-jnp.arange(half_dim, dtype=jnp.float32) / half_dim)
    angles = jnp.arange(seq_len, dtype=jnp.float32)[:, None] * inv_freq[None, :]
    cos_b = jnp.cos(angles)[None, :, None, :]
    sin_b = jnp.sin(angles)[None, :, None, :]
    lower_half = head_vals[..., :half_dim]
    upper_half = head_vals[..., half_dim:]
    return jnp.concatenate([lower_half * cos_b - upper_half * sin_b, upper_half * cos_b + lower_half * sin_b], axis=-1)


def attention_core(qkv_rows, num_seqs):
    num_tokens = qkv_rows.shape[0]
    seq_len = num_tokens // num_seqs
    model_width = qkv_rows.shape[1] // 3
    qkv_heads = qkv_rows.reshape(num_seqs, seq_len, 3, model_width // HEAD_DIM, HEAD_DIM)
    query_rot = rope_rotate(qkv_heads[:, :, 0]).astype(jnp.bfloat16)
    key_rot = rope_rotate(qkv_heads[:, :, 1]).astype(jnp.bfloat16)
    value_h = qkv_heads[:, :, 2].astype(jnp.bfloat16)
    scores = jnp.einsum('bqhd,bkhd->bhqk', query_rot, key_rot, preferred_element_type=jnp.float32) * HEAD_DIM ** -0.5
    causal = jnp.arange(seq_len)[:, None] >= jnp.arange(seq_len)[None, :]
    attn_probs = jax.nn.softmax(jnp.where(causal, scores, -1e30), axis=-1).astype(jnp.bfloat16)
    context = jnp.einsum('bhqk,bkhd->bqhd', attn_probs, value_h, preferred_element_type=jnp.float32)
    return context.astype(jnp.bfloat16).reshape(num_tokens, model_width)


def gate_probs(logits, idx_cols):
    probs_all = jax.nn.softmax(logits, axis=-1)
    chosen = idx_cols[:, :, None] == jnp.arange(logits.shape[1], dtype=jnp.int32)[None, None, :]
    picked = jnp.sum(jnp.where(chosen, probs_all[None], 0.0), axis=2)
    return picked / jnp.sum(picked, axis=0, keepdims=True)


def slot_positions(local_idx, local_experts, capacity):
    num_tokens = local_idx.shape[-1]
    expert_ids = jnp.arange(local_experts, dtype=jnp.int32)
    member = jnp.any(local_idx[None] == expert_ids[:, None, None, None], axis=2)
    before = (jnp.arange(num_tokens)[:, None] < jnp.arange(num_tokens)[None, :]).astype(BF16)
    earlier = jnp.einsum('est,tv->esv', member.astype(BF16), before, preferred_element_type=F32)
    return jnp.where(member & (earlier < capacity), earlier.astype(jnp.int32), -1)


def mat_nn(left, right):
    return lax.dot_general(left, right, (((1,), (0,)), ((), ())), preferred_element_type=F32)


def mat_nt(left, right):
    return lax.dot_general(left, right, (((1,), (1,)), ((), ())), preferred_element_type=F32)


def mat_tn(left, right):
    return lax.dot_general(left, right, (((0,), (0,)), ((), ())), preferred_element_type=F32)


def select_slots(capacity, group, pos_ref, idx_ref, gate_ref, source, first):
    num_tokens = pos_ref.shape[-1]
    slot_iota = lax.broadcasted_iota(jnp.int32, (capacity, num_tokens), 0)
    selectors, gate_cols = [], []
    for member in range(group):
        hit = slot_iota == pos_ref[member, pl.ds(source, 1), :]
        gate_row = jnp.sum(jnp.where(idx_ref[source] == first + member, gate_ref[source], 0.0), axis=0, keepdims=True)
        gate_cols.append(jnp.sum(jnp.where(hit, gate_row, 0.0), axis=1, keepdims=True))
        selectors.append(jnp.where(hit, 1.0, 0.0).astype(BF16))
    return jnp.concatenate(selectors, axis=0), jnp.concatenate(gate_cols, axis=0)


def swiglu_bwd(act_gate, act_up, d_hidden):
    sig = 0.5 * jnp.tanh(0.5 * act_gate) + 0.5
    silu = act_gate * sig
    hidden = (silu * act_up).astype(BF16)
    d_act_up = (d_hidden * silu).astype(BF16)
    d_act_gate = (d_hidden * act_up * (sig + silu * (1.0 - sig))).astype(BF16)
    return hidden, d_act_gate, d_act_up


def token_grad_kernel(capacity, group, pos_ref, idx_ref, gate_ref, rows_ref, dy_ref, w_gate_ref, w_up_ref, w_down_ref,
                      d_rows_ref, d_gates_ref, select_scr, in_scr, raw_scr, dout_scr, din_scr):
    sources = rows_ref.shape[0]
    num_tokens = rows_ref.shape[1]
    first = pl.program_id(0) * group

    @pl.when(pl.program_id(0) == 0)
    def _():
        d_rows_ref[...] = jnp.zeros_like(d_rows_ref)
        d_gates_ref[...] = jnp.zeros_like(d_gates_ref)

    @pl.loop(0, sources)
    def _(source):
        selector, gate_col = select_slots(capacity, group, pos_ref, idx_ref, gate_ref, source, first)
        select_scr[source] = selector
        slot_rows = mat_nn(selector, rows_ref[source]).astype(BF16)
        raw_dy = mat_nn(selector, dy_ref[source])
        scaled_dy = (raw_dy * gate_col).astype(BF16)
        raw_dy = raw_dy.astype(BF16)
        for member in range(group):
            span = pl.ds(source * capacity, capacity)
            part = slice(member * capacity, (member + 1) * capacity)
            in_scr[member, span] = slot_rows[part]
            raw_scr[member, span] = raw_dy[part]
            dout_scr[member, span] = scaled_dy[part]

    slot_iota = lax.broadcasted_iota(jnp.int32, (capacity, num_tokens), 0)
    for member in range(group):
        slot_rows = in_scr[member]
        d_out = dout_scr[member]
        act_gate = mat_nn(slot_rows, w_gate_ref[member])
        act_up = mat_nn(slot_rows, w_up_ref[member])
        d_hidden = mat_nt(d_out, w_down_ref[member])
        hidden, d_act_gate, d_act_up = swiglu_bwd(act_gate, act_up, d_hidden)
        expert_out = mat_nn(hidden, w_down_ref[member]).astype(BF16)
        d_gate = jnp.sum(raw_scr[member].astype(F32) * expert_out.astype(F32), axis=1, keepdims=True)
        d_in = (mat_nt(d_act_gate, w_gate_ref[member]) + mat_nt(d_act_up, w_up_ref[member])).astype(BF16)
        for source in range(sources):
            part = slice(source * capacity, (source + 1) * capacity)
            din_scr[source, member * capacity:(member + 1) * capacity] = d_in[part]
            hit = slot_iota == pos_ref[member, source:source + 1, :]
            d_gate_row = jnp.sum(jnp.where(hit, d_gate[part], 0.0), axis=0, keepdims=True)
            d_gates_ref[source] += jnp.where(idx_ref[source] == first + member, d_gate_row, 0.0)

    @pl.loop(0, sources)
    def _(source):
        d_rows_ref[source] += mat_tn(select_scr[source], din_scr[source])


def token_grads(positions, local_idx, gates, rows, dy_rows, w_gate, w_up, w_down, capacity):
    group = 4
    sources, num_tokens, width = rows.shape
    num_experts, _, _ = w_gate.shape
    slots = sources * capacity

    def whole(arr):
        return pl.BlockSpec(arr.shape, lambda step: (0,) * arr.ndim, pipeline_mode=pl.Buffered(1))

    def per_step(arr):
        return pl.BlockSpec((group,) + arr.shape[1:], lambda step: (step, 0, 0))

    return pl.pallas_call(
        functools.partial(token_grad_kernel, capacity, group),
        grid=(num_experts // group,),
        in_specs=[per_step(positions), whole(local_idx), whole(gates), whole(rows), whole(dy_rows),
                  per_step(w_gate), per_step(w_up), per_step(w_down)],
        out_specs=[pl.BlockSpec(rows.shape, lambda step: (0, 0, 0)), pl.BlockSpec(gates.shape, lambda step: (0, 0, 0))],
        out_shape=[jax.ShapeDtypeStruct(rows.shape, F32), jax.ShapeDtypeStruct(gates.shape, F32)],
        scratch_shapes=[pltpu.VMEM((sources, group * capacity, num_tokens), BF16),
                        pltpu.VMEM((group, slots, width), BF16), pltpu.VMEM((group, slots, width), BF16),
                        pltpu.VMEM((group, slots, width), BF16), pltpu.VMEM((sources, group * capacity, width), BF16)],
        compiler_params=pltpu.CompilerParams(vmem_limit_bytes=60_000_000, dimension_semantics=("arbitrary",)),
        cost_estimate=pl.CostEstimate(flops=45_000_000_000, bytes_accessed=60_000_000, transcendentals=0),
        name="expert_token_grads",
    )(positions, local_idx, gates, rows, dy_rows, w_gate, w_up, w_down)


def weight_grad_kernel(capacity, group, chunk, pos_ref, idx_ref, gate_ref, rows_ref, dy_ref, w_gate_ref, w_up_ref, w_down_ref,
                       d_w_gate_ref, d_w_up_ref, d_w_down_ref, in_scr, dout_scr, down_scr):
    expert = pl.program_id(0)
    member = lax.rem(expert, group)
    sources = rows_ref.shape[0]

    @pl.when(member == 0)
    def _():
        @pl.loop(0, sources)
        def _(source):
            selector, gate_col = select_slots(capacity, group, pos_ref, idx_ref, gate_ref, source, expert)
            slot_rows = mat_nn(selector, rows_ref[source]).astype(BF16)
            scaled_dy = (mat_nn(selector, dy_ref[source]) * gate_col).astype(BF16)
            for k in range(group):
                span = pl.ds(source * capacity, capacity)
                part = slice(k * capacity, (k + 1) * capacity)
                in_scr[k, span] = slot_rows[part]
                dout_scr[k, span] = scaled_dy[part]

    d_w_gate_ref[...] = jnp.zeros_like(d_w_gate_ref)
    d_w_up_ref[...] = jnp.zeros_like(d_w_up_ref)
    down_scr[...] = jnp.zeros_like(down_scr)

    def forward(start):
        span = pl.ds(start, chunk)
        slot_rows = in_scr[member, span]
        d_out = dout_scr[member, span]
        return slot_rows, d_out, mat_nn(slot_rows, w_gate_ref[0]), mat_nn(slot_rows, w_up_ref[0]), mat_nt(d_out, w_down_ref[0])

    ahead = forward(0)
    for start in range(0, sources * capacity, chunk):
        slot_rows, d_out, act_gate, act_up, d_hidden = ahead
        if start + chunk < sources * capacity:
            ahead = forward(start + chunk)
        hidden, d_act_gate, d_act_up = swiglu_bwd(act_gate, act_up, d_hidden)
        d_w_gate_ref[0] += mat_tn(slot_rows, d_act_gate)
        d_w_up_ref[0] += mat_tn(slot_rows, d_act_up)
        down_scr[...] += mat_tn(d_out, hidden)

    d_w_down_ref[0] = down_scr[...].T


def weight_grads(positions, local_idx, gates, rows, dy_rows, w_gate, w_up, w_down, capacity):
    group = 4
    chunk = 256
    sources, num_tokens, width = rows.shape
    num_experts, _, ff = w_gate.shape
    slots = sources * capacity

    def whole(arr):
        return pl.BlockSpec(arr.shape, lambda step: (0,) * arr.ndim, pipeline_mode=pl.Buffered(1))

    def per_step(arr):
        return pl.BlockSpec((1,) + arr.shape[1:], lambda step: (step, 0, 0))

    return pl.pallas_call(
        functools.partial(weight_grad_kernel, capacity, group, chunk),
        grid=(num_experts,),
        in_specs=[pl.BlockSpec((group, sources, num_tokens), lambda step: (step // group, 0, 0)), whole(local_idx), whole(gates),
                  whole(rows), whole(dy_rows), per_step(w_gate), per_step(w_up), per_step(w_down)],
        out_specs=[per_step(w_gate), per_step(w_up), per_step(w_down)],
        out_shape=[jax.ShapeDtypeStruct(arr.shape, F32) for arr in (w_gate, w_up, w_down)],
        scratch_shapes=[pltpu.VMEM((group, slots, width), BF16), pltpu.VMEM((group, slots, width), BF16), pltpu.VMEM((width, ff), F32)],
        compiler_params=pltpu.CompilerParams(vmem_limit_bytes=67_000_000, dimension_semantics=("arbitrary",)),
        cost_estimate=pl.CostEstimate(flops=280_000_000_000, bytes_accessed=150_000_000, transcendentals=0),
        name="expert_weight_grads",
    )(positions, local_idx, gates, rows, dy_rows, w_gate, w_up, w_down)


def dense_forward(x_rows, idx_cols, num_seqs, norm1_gain, norm2_gain, w_qkv, w_attn_out, w_router):
    normed1 = rms_norm(x_rows, norm1_gain)
    qkv_rows = jnp.dot(normed1, w_qkv, preferred_element_type=jnp.float32)
    context, attn_pullback = jax.vjp(lambda qkv_in: attention_core(qkv_in, num_seqs), qkv_rows)
    h_rows = (x_rows.astype(jnp.float32) + jnp.dot(context, w_attn_out, preferred_element_type=jnp.float32)).astype(jnp.bfloat16)
    normed2 = rms_norm(h_rows, norm2_gain)
    logits = jnp.dot(normed2, w_router, preferred_element_type=jnp.float32)
    gate_vals, gate_pullback = jax.vjp(lambda logit_in: gate_probs(logit_in, idx_cols), logits)
    saved_state = (normed1, attn_pullback, context, h_rows, normed2, gate_pullback)
    return normed2, gate_vals, saved_state


def dense_backward(saved_state, x_rows, dy_rows, d_gates, d_normed2_moe, norm1_gain, norm2_gain, w_qkv, w_attn_out, w_router):
    normed1, attn_pullback, context, h_rows, normed2, gate_pullback = saved_state
    d_logits = gate_pullback(d_gates)[0].astype(jnp.bfloat16)
    d_w_router = jnp.einsum('td,te->de', normed2, d_logits, preferred_element_type=jnp.float32)
    d_normed2 = d_normed2_moe + jnp.einsum('te,de->td', d_logits, w_router, preferred_element_type=jnp.float32)
    d_h_part, d_norm2_gain = rms_norm_bwd(h_rows, norm2_gain, d_normed2)
    d_h = (dy_rows.astype(jnp.float32) + d_h_part).astype(jnp.bfloat16)
    d_w_attn_out = jnp.einsum('td,te->de', context, d_h, preferred_element_type=jnp.float32)
    d_context = jnp.einsum('te,de->td', d_h, w_attn_out, preferred_element_type=jnp.float32).astype(jnp.bfloat16)
    d_qkv = attn_pullback(d_context)[0].astype(jnp.bfloat16)
    d_w_qkv = jnp.einsum('td,te->de', normed1, d_qkv, preferred_element_type=jnp.float32)
    d_normed1 = jnp.einsum('te,de->td', d_qkv, w_qkv, preferred_element_type=jnp.float32)
    d_x_part, d_norm1_gain = rms_norm_bwd(x_rows, norm1_gain, d_normed1)
    d_x = (d_h.astype(jnp.float32) + d_x_part).astype(jnp.bfloat16)
    return d_x, (d_norm1_gain, d_norm2_gain, d_w_qkv, d_w_attn_out, d_w_router)


def solution(mesh):
    ep_size = mesh.shape['ep']
    tok_spec = P(('dp', 'ep'), None, None)
    rep_spec = P()
    exp_spec = P('ep', None, None)

    def local_step(x_tokens, dy_tokens, route_idx, norm1_gain, norm2_gain, w_qkv, w_attn_out, w_router, w_gate, w_up, w_down):
        num_seqs, seq_len, model_width = x_tokens.shape
        num_tokens = num_seqs * seq_len
        top_k = route_idx.shape[-1]
        local_experts = w_gate.shape[0]
        num_experts = local_experts * ep_size
        capacity = capacity_rows(num_tokens, top_k, num_experts)
        x_rows = x_tokens.reshape(num_tokens, model_width)
        dy_rows = dy_tokens.reshape(num_tokens, model_width)
        idx_cols = route_idx.reshape(num_tokens, top_k).T
        dy_all = lax.all_gather(dy_rows, ('dp', 'ep'))
        idx_all = lax.all_gather(idx_cols, ('dp', 'ep'))
        local_idx = idx_all - lax.axis_index('ep') * local_experts
        positions = slot_positions(local_idx, local_experts, capacity)
        normed2, gate_vals, saved_state = dense_forward(x_rows, idx_cols, num_seqs, norm1_gain, norm2_gain, w_qkv, w_attn_out, w_router)
        near_rows = lax.all_gather(normed2, 'ep')
        near_gates = lax.all_gather(gate_vals, 'ep')
        rows_all = lax.all_gather(normed2, ('dp', 'ep'))
        gates_all = lax.all_gather(gate_vals, ('dp', 'ep'))
        near = lax.axis_index('dp') * ep_size
        d_near, d_gate_near = token_grads(lax.dynamic_slice_in_dim(positions, near, ep_size, 1), lax.dynamic_slice_in_dim(local_idx, near, ep_size, 0),
                                          near_gates, near_rows, lax.all_gather(dy_rows, 'ep'), w_gate, w_up, w_down, capacity)
        d_normed2_moe = jnp.sum(lax.all_to_all(d_near, 'ep', 0, 0, tiled=True), axis=0)
        d_gates = jnp.sum(lax.all_to_all(d_gate_near, 'ep', 0, 0, tiled=True), axis=0)
        d_x, dense_grads = dense_backward(saved_state, x_rows, dy_rows, d_gates, d_normed2_moe, norm1_gain, norm2_gain, w_qkv, w_attn_out, w_router)
        gain_cols = jnp.zeros((model_width, 128), F32).at[:, 0].set(dense_grads[0]).at[:, 1].set(dense_grads[1])
        packed = jnp.concatenate(dense_grads[2:] + (gain_cols,), axis=1)
        packed, gates_all = lax.optimization_barrier((packed, gates_all))
        expert_grads = weight_grads(positions, local_idx, gates_all, rows_all, dy_all, w_gate, w_up, w_down, capacity)
        packed = lax.psum(packed, ('dp', 'ep'))
        qkv_end = w_qkv.shape[1]
        out_end = qkv_end + w_attn_out.shape[1]
        router_end = out_end + num_experts
        dense_out = (packed[:, router_end], packed[:, router_end + 1], packed[:, :qkv_end], packed[:, qkv_end:out_end], packed[:, out_end:router_end])
        return (d_x.reshape(x_tokens.shape),) + dense_out + tuple(expert_grads)

    return jax.shard_map(local_step, mesh=mesh,
                          in_specs=(tok_spec, tok_spec, tok_spec, rep_spec, rep_spec, rep_spec, rep_spec, rep_spec, exp_spec, exp_spec, exp_spec),
                          out_specs=(tok_spec, rep_spec, rep_spec, rep_spec, rep_spec, rep_spec, exp_spec, exp_spec, exp_spec),
                          check_vma=False)
```

```python
import functools

import jax
import jax.numpy as jnp
from jax import lax
from jax.experimental import pallas as pl
from jax.experimental.pallas import tpu as pltpu
from jax.sharding import PartitionSpec as P


F32 = jnp.float32
BF16 = jnp.bfloat16
EPS = 1e-6
HEAD_DIM = 128
ROPE_BASE = 10000.0


def capacity_rows(num_tokens, top_k, num_experts):
    return 8 * ((5 * num_tokens * top_k + 32 * num_experts - 1) // (32 * num_experts))


def rms_norm(x_rows, gain_vec):
    x_f32 = x_rows.astype(jnp.float32)
    inv_rms = lax.rsqrt(jnp.mean(x_f32 * x_f32, axis=-1, keepdims=True) + EPS)
    return (x_f32 * inv_rms * gain_vec.astype(jnp.float32)).astype(jnp.bfloat16)


def rms_norm_bwd(x_rows, gain_vec, d_out):
    x_f32 = x_rows.astype(jnp.float32)
    inv_rms = lax.rsqrt(jnp.mean(x_f32 * x_f32, axis=-1, keepdims=True) + EPS)
    d_gain = jnp.sum(d_out * x_f32 * inv_rms, axis=0)
    d_scaled = d_out * gain_vec.astype(jnp.float32)
    d_x = inv_rms * d_scaled - x_f32 * inv_rms ** 3 * jnp.mean(d_scaled * x_f32, axis=-1, keepdims=True)
    return d_x, d_gain


def rope_rotate(head_vals):
    seq_len = head_vals.shape[1]
    half_dim = head_vals.shape[-1] // 2
    inv_freq = ROPE_BASE ** (-jnp.arange(half_dim, dtype=jnp.float32) / half_dim)
    angles = jnp.arange(seq_len, dtype=jnp.float32)[:, None] * inv_freq[None, :]
    cos_b = jnp.cos(angles)[None, :, None, :]
    sin_b = jnp.sin(angles)[None, :, None, :]
    lower_half = head_vals[..., :half_dim]
    upper_half = head_vals[..., half_dim:]
    return jnp.concatenate([lower_half * cos_b - upper_half * sin_b, upper_half * cos_b + lower_half * sin_b], axis=-1)


def attention_core(qkv_rows, num_seqs):
    num_tokens = qkv_rows.shape[0]
    seq_len = num_tokens // num_seqs
    model_width = qkv_rows.shape[1] // 3
    qkv_heads = qkv_rows.reshape(num_seqs, seq_len, 3, model_width // HEAD_DIM, HEAD_DIM)
    query_rot = rope_rotate(qkv_heads[:, :, 0]).astype(jnp.bfloat16)
    key_rot = rope_rotate(qkv_heads[:, :, 1]).astype(jnp.bfloat16)
    value_h = qkv_heads[:, :, 2].astype(jnp.bfloat16)
    scores = jnp.einsum('bqhd,bkhd->bhqk', query_rot, key_rot, preferred_element_type=jnp.float32) * HEAD_DIM ** -0.5
    causal = jnp.arange(seq_len)[:, None] >= jnp.arange(seq_len)[None, :]
    attn_probs = jax.nn.softmax(jnp.where(causal, scores, -1e30), axis=-1).astype(jnp.bfloat16)
    context = jnp.einsum('bhqk,bkhd->bqhd', attn_probs, value_h, preferred_element_type=jnp.float32)
    return context.astype(jnp.bfloat16).reshape(num_tokens, model_width)


def gate_probs(logits, idx_cols):
    probs_all = jax.nn.softmax(logits, axis=-1)
    chosen = idx_cols[:, :, None] == jnp.arange(logits.shape[1], dtype=jnp.int32)[None, None, :]
    picked = jnp.sum(jnp.where(chosen, probs_all[None], 0.0), axis=2)
    return picked / jnp.sum(picked, axis=0, keepdims=True)


def slot_positions(local_idx, local_experts, capacity):
    num_tokens = local_idx.shape[-1]
    expert_ids = jnp.arange(local_experts, dtype=jnp.int32)
    member = jnp.any(local_idx[None] == expert_ids[:, None, None, None], axis=2)
    before = (jnp.arange(num_tokens)[:, None] < jnp.arange(num_tokens)[None, :]).astype(BF16)
    earlier = jnp.einsum('est,tv->esv', member.astype(BF16), before, preferred_element_type=F32)
    return jnp.where(member & (earlier < capacity), earlier.astype(jnp.int32), -1)


def mat_nn(left, right):
    return lax.dot_general(left, right, (((1,), (0,)), ((), ())), preferred_element_type=F32)


def mat_nt(left, right):
    return lax.dot_general(left, right, (((1,), (1,)), ((), ())), preferred_element_type=F32)


def mat_tn(left, right):
    return lax.dot_general(left, right, (((0,), (0,)), ((), ())), preferred_element_type=F32)


def swiglu_bwd(act_gate, act_up, d_hidden):
    sig = 0.5 * jnp.tanh(0.5 * act_gate) + 0.5
    silu = act_gate * sig
    hidden = (silu * act_up).astype(BF16)
    d_act_up = (d_hidden * silu).astype(BF16)
    d_act_gate = (d_hidden * act_up * (sig + silu * (1.0 - sig))).astype(BF16)
    return hidden, d_act_gate, d_act_up


def token_grad_kernel(capacity, group, pos_ref, idx_ref, gate_ref, rows_ref, dy_ref, w_gate_ref, w_up_ref, w_down_ref,
                      d_rows_ref, d_gates_ref, slot_gate_ref, select_scr, in_scr, raw_scr, dout_scr, din_scr):
    sources, num_tokens, _ = rows_ref.shape
    first = pl.program_id(0) * group
    slot_iota = lax.broadcasted_iota(jnp.int32, (capacity, num_tokens), 0)
    diagonal = lax.broadcasted_iota(jnp.int32, (capacity, 128), 0) == lax.broadcasted_iota(jnp.int32, (capacity, 128), 1)

    @pl.when(pl.program_id(0) == 0)
    def _():
        d_rows_ref[...] = jnp.zeros_like(d_rows_ref)
        d_gates_ref[...] = jnp.zeros_like(d_gates_ref)

    def select(source):
        selectors, gate_cols = [], []
        for member in range(group):
            hit = slot_iota == pos_ref[member, source:source + 1, :]
            gate_row = jnp.sum(jnp.where(idx_ref[source] == first + member, gate_ref[source], 0.0), axis=0, keepdims=True)
            gate_col = jnp.sum(jnp.where(hit, gate_row, 0.0), axis=1, keepdims=True)
            slot_gate_ref[member, source:source + 1, :] = jnp.sum(jnp.where(diagonal, gate_col, 0.0), axis=0, keepdims=True)
            gate_cols.append(gate_col)
            selectors.append(jnp.where(hit, 1.0, 0.0).astype(BF16))
        return jnp.concatenate(selectors, axis=0), jnp.concatenate(gate_cols, axis=0)

    ahead = select(0)
    for source in range(sources):
        selector, gate_col = ahead
        if source + 1 < sources:
            ahead = select(source + 1)
        select_scr[source] = selector
        slot_rows = mat_nn(selector, rows_ref[source]).astype(BF16)
        raw_dy = mat_nn(selector, dy_ref[source, :num_tokens])
        scaled_dy = (raw_dy * gate_col).astype(BF16)
        raw_dy = raw_dy.astype(BF16)
        for member in range(group):
            span = slice(source * capacity, (source + 1) * capacity)
            part = slice(member * capacity, (member + 1) * capacity)
            in_scr[member, span] = slot_rows[part]
            raw_scr[member, span] = raw_dy[part]
            dout_scr[member, span] = scaled_dy[part]

    def forward(member):
        slot_rows = in_scr[member]
        return mat_nn(slot_rows, w_gate_ref[member]), mat_nn(slot_rows, w_up_ref[member]), mat_nt(dout_scr[member], w_down_ref[member])

    ahead = forward(0)
    for member in range(group):
        act_gate, act_up, d_hidden = ahead
        if member + 1 < group:
            ahead = forward(member + 1)
        hidden, d_act_gate, d_act_up = swiglu_bwd(act_gate, act_up, d_hidden)
        expert_out = mat_nn(hidden, w_down_ref[member]).astype(BF16)
        d_gate = jnp.sum(raw_scr[member].astype(F32) * expert_out.astype(F32), axis=1, keepdims=True)
        d_in = (mat_nt(d_act_gate, w_gate_ref[member]) + mat_nt(d_act_up, w_up_ref[member])).astype(BF16)
        for source in range(sources):
            part = slice(source * capacity, (source + 1) * capacity)
            din_scr[source, member * capacity:(member + 1) * capacity] = d_in[part]
            hit = slot_iota == pos_ref[member, source:source + 1, :]
            d_gate_row = jnp.sum(jnp.where(hit, d_gate[part], 0.0), axis=0, keepdims=True)
            d_gates_ref[source] += jnp.where(idx_ref[source] == first + member, d_gate_row, 0.0)

    for source in range(sources):
        d_rows_ref[source] += mat_tn(select_scr[source], din_scr[source])


def token_grads(positions, local_idx, gates, rows, dy_rows, w_gate, w_up, w_down, capacity):
    group = 4
    sources, num_tokens, width = rows.shape
    num_experts = w_gate.shape[0]
    slots = sources * capacity

    def whole(arr):
        return pl.BlockSpec(arr.shape, lambda step: (0,) * arr.ndim, pipeline_mode=pl.Buffered(1))

    def per_step(arr):
        return pl.BlockSpec((group,) + arr.shape[1:], lambda step: (step, 0, 0))

    slot_gates = jax.ShapeDtypeStruct((num_experts, sources, 128), F32)
    return pl.pallas_call(
        functools.partial(token_grad_kernel, capacity, group),
        grid=(num_experts // group,),
        in_specs=[per_step(positions), whole(local_idx), whole(gates), whole(rows), whole(dy_rows),
                  per_step(w_gate), per_step(w_up), per_step(w_down)],
        out_specs=[pl.BlockSpec(rows.shape, lambda step: (0, 0, 0)), pl.BlockSpec(gates.shape, lambda step: (0, 0, 0)), per_step(slot_gates)],
        out_shape=[jax.ShapeDtypeStruct(rows.shape, F32), jax.ShapeDtypeStruct(gates.shape, F32), slot_gates],
        scratch_shapes=[pltpu.VMEM((sources, group * capacity, num_tokens), BF16),
                        pltpu.VMEM((group, slots, width), BF16), pltpu.VMEM((group, slots, width), BF16),
                        pltpu.VMEM((group, slots, width), BF16), pltpu.VMEM((sources, group * capacity, width), BF16)],
        compiler_params=pltpu.CompilerParams(vmem_limit_bytes=60_000_000, dimension_semantics=("arbitrary",)),
        cost_estimate=pl.CostEstimate(flops=45_000_000_000, bytes_accessed=60_000_000, transcendentals=0),
        name="expert_token_grads",
    )(positions, local_idx, gates, rows, dy_rows, w_gate, w_up, w_down)


def near_peers():
    ep = lax.axis_index('ep')
    return {'ep': ep + 1 - 2 * lax.rem(ep, 2)}, {'ep': lax.rem(ep + 2, 4)}


def meet(peers):
    barrier = pltpu.get_barrier_semaphore()
    for peer in peers:
        pl.semaphore_signal(barrier, inc=1, device_id=peer, device_id_type=pl.DeviceIdType.MESH)
    pl.semaphore_wait(barrier, len(peers))


def remote(src, dst, send_sem, recv_sem, peer):
    return pltpu.make_async_remote_copy(src_ref=src, dst_ref=dst, send_sem=send_sem, recv_sem=recv_sem,
                                        device_id=peer, device_id_type=pl.DeviceIdType.MESH)


def near_gather_kernel(rows_ref, gates_ref, rows_out, gates_out, send_sem, recv_sem):
    core_peer, chip_peer = near_peers()
    meet((core_peer, chip_peer))
    half = rows_ref.shape[0] // 2
    pieces = [(rows_ref.at[pl.ds(0, half)], lambda slot: rows_out.at[slot, pl.ds(0, half)]),
              (rows_ref.at[pl.ds(half, half)], lambda slot: rows_out.at[slot, pl.ds(half, half)]),
              (gates_ref, lambda slot: gates_out.at[slot])]
    across = [remote(src, place(2), send_sem.at[0, i], recv_sem.at[0, i], chip_peer) for i, (src, place) in enumerate(pieces)]
    beside = [remote(src, place(1), send_sem.at[1, i], recv_sem.at[1, i], core_peer) for i, (src, place) in enumerate(pieces)]
    onward = [remote(place(2), place(3), send_sem.at[2, i], recv_sem.at[2, i], core_peer) for i, (_, place) in enumerate(pieces)]
    for copy in across + beside:
        copy.start()
    rows_out[0] = rows_ref[...]
    gates_out[0] = gates_ref[...]
    for copy, forward in zip(across, onward):
        copy.wait_recv()
        forward.start()
    for copy in beside + onward:
        copy.wait()
    for copy in across:
        copy.wait_send()


def near_gather(rows, gates):
    vmem = pl.BlockSpec(memory_space=pltpu.VMEM)
    return pl.pallas_call(
        near_gather_kernel,
        in_specs=[vmem, vmem], out_specs=[vmem, vmem],
        out_shape=[jax.ShapeDtypeStruct((4,) + rows.shape, rows.dtype), jax.ShapeDtypeStruct((4,) + gates.shape, gates.dtype)],
        scratch_shapes=[pltpu.SemaphoreType.DMA((3, 3)), pltpu.SemaphoreType.DMA((3, 3))],
        compiler_params=pltpu.CompilerParams(collective_id=0, has_side_effects=True),
        cost_estimate=pl.CostEstimate(flops=10_000_000_000, bytes_accessed=10_000_000, transcendentals=0),
        name="near_gather",
    )(rows, gates)


def near_return_kernel(d_rows_ref, d_gates_ref, slot_gates_ref, rows_out, gates_out, slot_gates_out,
                       own_rows, pass_rows, sum_rows, last_rows, own_gates, pass_gates, sum_gates, last_gates,
                       send_sem, recv_sem, far_send_sem, far_recv_sem):
    core_peer, chip_peer = near_peers()
    dp = lax.axis_index('dp')
    dp_size = slot_gates_out.shape[0]
    far_peers = [{'dp': lax.rem(dp + k, dp_size)} for k in range(1, dp_size)]
    meet([core_peer, chip_peer] + far_peers)
    first = [remote(d_rows_ref.at[3], pass_rows, send_sem.at[0], recv_sem.at[0], core_peer),
             remote(d_gates_ref.at[3], pass_gates, send_sem.at[1], recv_sem.at[1], core_peer)]
    second = [remote(d_rows_ref.at[1], own_rows, send_sem.at[2], recv_sem.at[2], core_peer),
              remote(d_gates_ref.at[1], own_gates, send_sem.at[3], recv_sem.at[3], core_peer)]
    third = [remote(sum_rows, last_rows, send_sem.at[4], recv_sem.at[4], chip_peer),
             remote(sum_gates, last_gates, send_sem.at[5], recv_sem.at[5], chip_peer)]
    far = [remote(slot_gates_ref, slot_gates_out.at[dp], far_send_sem.at[k], far_recv_sem.at[k], peer) for k, peer in enumerate(far_peers)]
    for copy in first + second:
        copy.start()
    for copy in first:
        copy.wait_recv()
    sum_rows[...] = d_rows_ref[2] + pass_rows[...]
    sum_gates[...] = d_gates_ref[2] + pass_gates[...]
    for copy in second:
        copy.wait_recv()
    rows_out[...] = d_rows_ref[0] + own_rows[...]
    gates_out[...] = d_gates_ref[0] + own_gates[...]
    for copy in third + far:
        copy.start()
    slot_gates_out[dp] = slot_gates_ref[...]
    for copy in third:
        copy.wait_recv()
    rows_out[...] += last_rows[...]
    gates_out[...] += last_gates[...]
    for copy in far:
        copy.wait()
    for copy in first + second + third:
        copy.wait_send()


def near_return(d_rows, d_gates, slot_gates, dp_size):
    vmem = pl.BlockSpec(memory_space=pltpu.VMEM)
    rows = jax.ShapeDtypeStruct(d_rows.shape[1:], F32)
    gates = jax.ShapeDtypeStruct(d_gates.shape[1:], F32)
    return pl.pallas_call(
        near_return_kernel,
        in_specs=[vmem] * 3, out_specs=[vmem] * 3,
        out_shape=[rows, gates, jax.ShapeDtypeStruct((dp_size,) + slot_gates.shape, F32)],
        scratch_shapes=[pltpu.VMEM(rows.shape, F32)] * 4 + [pltpu.VMEM(gates.shape, F32)] * 4
        + [pltpu.SemaphoreType.DMA((6,)), pltpu.SemaphoreType.DMA((6,)), pltpu.SemaphoreType.DMA((dp_size - 1,)), pltpu.SemaphoreType.DMA((dp_size - 1,))],
        compiler_params=pltpu.CompilerParams(collective_id=1, has_side_effects=True, vmem_limit_bytes=40_000_000),
        cost_estimate=pl.CostEstimate(flops=15_000_000_000, bytes_accessed=20_000_000, transcendentals=0),
        name="near_return",
    )(d_rows, d_gates, slot_gates)


def weight_grad_kernel(capacity, group, chunk, pos_ref, slot_gate_ref, rows_ref, dy_ref, w_gate_ref, w_up_ref, w_down_ref,
                       d_w_gate_ref, d_w_up_ref, d_w_down_ref, in_scr, dout_scr, down_scr):
    expert = pl.program_id(0)
    member = lax.rem(expert, group)
    sources, num_tokens, _ = rows_ref.shape
    ep = lax.axis_index('ep')
    slot_iota = lax.broadcasted_iota(jnp.int32, (capacity, num_tokens), 0)
    diagonal = lax.broadcasted_iota(jnp.int32, (capacity, 128), 0) == lax.broadcasted_iota(jnp.int32, (capacity, 128), 1)

    def select(source):
        gate_at = source - lax.rem(source, 4) + jnp.bitwise_xor(lax.rem(source, 4), ep)
        selectors, gate_cols = [], []
        for k in range(group):
            selectors.append(jnp.where(slot_iota == pos_ref[k, pl.ds(source, 1), :], 1.0, 0.0).astype(BF16))
            gate_cols.append(jnp.sum(jnp.where(diagonal, slot_gate_ref[k, pl.ds(gate_at, 1), :], 0.0), axis=1, keepdims=True))
        return jnp.concatenate(selectors, axis=0), jnp.concatenate(gate_cols, axis=0)

    @pl.when(member == 0)
    def _():
        unroll = 2

        @pl.loop(0, sources // unroll)
        def _(step):
            ahead = select(step * unroll)
            for j in range(unroll):
                source = step * unroll + j
                selector, gate_col = ahead
                if j + 1 < unroll:
                    ahead = select(source + 1)
                slot_rows = mat_nn(selector, rows_ref[source]).astype(BF16)
                scaled_dy = (mat_nn(selector, dy_ref[source, :num_tokens]) * gate_col).astype(BF16)
                for k in range(group):
                    span = pl.ds(source * capacity, capacity)
                    part = slice(k * capacity, (k + 1) * capacity)
                    in_scr[k, span] = slot_rows[part]
                    dout_scr[k, span] = scaled_dy[part]

    d_w_gate_ref[...] = jnp.zeros_like(d_w_gate_ref)
    d_w_up_ref[...] = jnp.zeros_like(d_w_up_ref)
    down_scr[...] = jnp.zeros_like(down_scr)

    def forward(start):
        span = pl.ds(start, chunk)
        slot_rows = in_scr[member, span]
        d_out = dout_scr[member, span]
        return slot_rows, d_out, mat_nn(slot_rows, w_gate_ref[0]), mat_nn(slot_rows, w_up_ref[0]), mat_nt(d_out, w_down_ref[0])

    ahead = forward(0)
    for start in range(0, sources * capacity, chunk):
        slot_rows, d_out, act_gate, act_up, d_hidden = ahead
        if start + chunk < sources * capacity:
            ahead = forward(start + chunk)
        hidden, d_act_gate, d_act_up = swiglu_bwd(act_gate, act_up, d_hidden)
        d_w_gate_ref[0] += mat_tn(slot_rows, d_act_gate)
        d_w_up_ref[0] += mat_tn(slot_rows, d_act_up)
        down_scr[...] += mat_tn(d_out, hidden)

    d_w_down_ref[0] = down_scr[...].T


def weight_grads(positions, slot_gates, rows, dy_rows, w_gate, w_up, w_down, capacity):
    group = 4
    chunk = 256
    sources, num_tokens, width = rows.shape
    num_experts, _, ff = w_gate.shape
    slots = sources * capacity

    def whole(arr):
        return pl.BlockSpec(arr.shape, lambda step: (0,) * arr.ndim, pipeline_mode=pl.Buffered(1))

    def per_step(arr):
        return pl.BlockSpec((1,) + arr.shape[1:], lambda step: (step, 0, 0))

    return pl.pallas_call(
        functools.partial(weight_grad_kernel, capacity, group, chunk),
        grid=(num_experts,),
        in_specs=[pl.BlockSpec((group, sources, num_tokens), lambda step: (step // group, 0, 0)),
                  pl.BlockSpec((group, sources, 128), lambda step: (step // group, 0, 0)),
                  whole(rows), whole(dy_rows), per_step(w_gate), per_step(w_up), per_step(w_down)],
        out_specs=[per_step(w_gate), per_step(w_up), per_step(w_down)],
        out_shape=[jax.ShapeDtypeStruct(arr.shape, F32) for arr in (w_gate, w_up, w_down)],
        scratch_shapes=[pltpu.VMEM((group, slots, width), BF16), pltpu.VMEM((group, slots, width), BF16), pltpu.VMEM((width, ff), F32)],
        compiler_params=pltpu.CompilerParams(vmem_limit_bytes=67_000_000, dimension_semantics=("arbitrary",)),
        cost_estimate=pl.CostEstimate(flops=280_000_000_000, bytes_accessed=150_000_000, transcendentals=0),
        name="expert_weight_grads",
    )(positions, slot_gates, rows, dy_rows, w_gate, w_up, w_down)


def dense_forward(x_rows, idx_cols, num_seqs, norm1_gain, norm2_gain, w_qkv, w_attn_out, w_router):
    normed1 = rms_norm(x_rows, norm1_gain)
    qkv_rows = jnp.dot(normed1, w_qkv, preferred_element_type=jnp.float32)
    context, attn_pullback = jax.vjp(lambda qkv_in: attention_core(qkv_in, num_seqs), qkv_rows)
    h_rows = (x_rows.astype(jnp.float32) + jnp.dot(context, w_attn_out, preferred_element_type=jnp.float32)).astype(jnp.bfloat16)
    normed2 = rms_norm(h_rows, norm2_gain)
    logits = jnp.dot(normed2, w_router, preferred_element_type=jnp.float32)
    gate_vals, gate_pullback = jax.vjp(lambda logit_in: gate_probs(logit_in, idx_cols), logits)
    saved_state = (normed1, attn_pullback, context, h_rows, normed2, gate_pullback)
    return normed2, gate_vals, saved_state


def dense_backward(saved_state, x_rows, dy_rows, d_gates, d_normed2_moe, norm1_gain, norm2_gain, w_qkv, w_attn_out, w_router):
    normed1, attn_pullback, context, h_rows, normed2, gate_pullback = saved_state
    d_logits = gate_pullback(d_gates)[0].astype(jnp.bfloat16)
    d_w_router = jnp.einsum('td,te->de', normed2, d_logits, preferred_element_type=jnp.float32)
    d_normed2 = d_normed2_moe + jnp.einsum('te,de->td', d_logits, w_router, preferred_element_type=jnp.float32)
    d_h_part, d_norm2_gain = rms_norm_bwd(h_rows, norm2_gain, d_normed2)
    d_h = (dy_rows.astype(jnp.float32) + d_h_part).astype(jnp.bfloat16)
    d_w_attn_out = jnp.einsum('td,te->de', context, d_h, preferred_element_type=jnp.float32)
    d_context = jnp.einsum('te,de->td', d_h, w_attn_out, preferred_element_type=jnp.float32).astype(jnp.bfloat16)
    d_qkv = attn_pullback(d_context)[0].astype(jnp.bfloat16)
    d_w_qkv = jnp.einsum('td,te->de', normed1, d_qkv, preferred_element_type=jnp.float32)
    d_normed1 = jnp.einsum('te,de->td', d_qkv, w_qkv, preferred_element_type=jnp.float32)
    d_x_part, d_norm1_gain = rms_norm_bwd(x_rows, norm1_gain, d_normed1)
    d_x = (d_h.astype(jnp.float32) + d_x_part).astype(jnp.bfloat16)
    return d_x, (d_norm1_gain, d_norm2_gain, d_w_qkv, d_w_attn_out, d_w_router)


def solution(mesh):
    ep_size = mesh.shape['ep']
    tok_spec = P(('dp', 'ep'), None, None)
    rep_spec = P()
    exp_spec = P('ep', None, None)

    def local_step(x_tokens, dy_tokens, route_idx, norm1_gain, norm2_gain, w_qkv, w_attn_out, w_router, w_gate, w_up, w_down):
        num_seqs, seq_len, model_width = x_tokens.shape
        num_tokens = num_seqs * seq_len
        top_k = route_idx.shape[-1]
        local_experts = w_gate.shape[0]
        num_experts = local_experts * ep_size
        capacity = capacity_rows(num_tokens, top_k, num_experts)
        x_rows = x_tokens.reshape(num_tokens, model_width)
        dy_rows = dy_tokens.reshape(num_tokens, model_width)
        idx_cols = route_idx.reshape(num_tokens, top_k).T
        routes = idx_cols.astype(BF16).reshape(-1, model_width)
        payload = jnp.concatenate([dy_rows, routes], axis=0)
        dy_all = lax.all_gather(payload, ('dp', 'ep'))
        moved = [lax.ppermute(payload, 'ep', [(i, i ^ k) for i in range(ep_size)]) for k in range(1, ep_size)]
        dy_near = jnp.stack([payload] + moved)

        def expert_of(gathered):
            return gathered[:, num_tokens:].reshape(-1, top_k, num_tokens).astype(jnp.int32) - lax.axis_index('ep') * local_experts

        idx_near = expert_of(dy_near)
        positions_near = slot_positions(idx_near, local_experts, capacity)
        normed2, gate_vals, saved_state = dense_forward(x_rows, idx_cols, num_seqs, norm1_gain, norm2_gain, w_qkv, w_attn_out, w_router)
        rows_all = lax.all_gather(normed2, ('dp', 'ep'))
        rows_near, gates_near = near_gather(normed2, gate_vals)
        d_near, d_gate_near, slot_gates = token_grads(positions_near, idx_near, gates_near, rows_near, dy_near, w_gate, w_up, w_down, capacity)
        d_normed2_moe, d_gates, slot_gates_all = near_return(d_near, d_gate_near, slot_gates, mesh.shape['dp'])
        slot_gates_all = slot_gates_all.transpose(1, 0, 2, 3).reshape(local_experts, -1, 128)
        d_x, dense_grads = dense_backward(saved_state, x_rows, dy_rows, d_gates, d_normed2_moe, norm1_gain, norm2_gain, w_qkv, w_attn_out, w_router)
        gain_cols = jnp.zeros((model_width, 128), F32).at[:, 0].set(dense_grads[0]).at[:, 1].set(dense_grads[1])
        packed = jnp.concatenate(dense_grads[2:] + (gain_cols,), axis=1)
        packed, slot_gates_all = lax.optimization_barrier((packed, slot_gates_all))
        positions = slot_positions(expert_of(dy_all), local_experts, capacity)
        expert_grads = weight_grads(positions, slot_gates_all, rows_all, dy_all, w_gate, w_up, w_down, capacity)
        packed = lax.psum(packed, ('dp', 'ep'))
        qkv_end = w_qkv.shape[1]
        out_end = qkv_end + w_attn_out.shape[1]
        router_end = out_end + num_experts
        dense_out = (packed[:, router_end], packed[:, router_end + 1], packed[:, :qkv_end], packed[:, qkv_end:out_end], packed[:, out_end:router_end])
        return (d_x.reshape(x_tokens.shape),) + dense_out + tuple(expert_grads)

    return jax.shard_map(local_step, mesh=mesh,
                          in_specs=(tok_spec, tok_spec, tok_spec, rep_spec, rep_spec, rep_spec, rep_spec, rep_spec, exp_spec, exp_spec, exp_spec),
                          out_specs=(tok_spec, rep_spec, rep_spec, rep_spec, rep_spec, rep_spec, exp_spec, exp_spec, exp_spec),
                          check_vma=False)
```

```python
import functools

import jax
import jax.numpy as jnp
from jax import lax
from jax.experimental import pallas as pl
from jax.experimental.pallas import tpu as pltpu
from jax.sharding import PartitionSpec as P


F32 = jnp.float32
BF16 = jnp.bfloat16
EPS = 1e-6
HEAD_DIM = 128
ROPE_BASE = 10000.0


def capacity_rows(num_tokens, top_k, num_experts):
    return 8 * ((5 * num_tokens * top_k + 32 * num_experts - 1) // (32 * num_experts))


def rms_norm(x_rows, gain_vec):
    x_f32 = x_rows.astype(jnp.float32)
    inv_rms = lax.rsqrt(jnp.mean(x_f32 * x_f32, axis=-1, keepdims=True) + EPS)
    return (x_f32 * inv_rms * gain_vec.astype(jnp.float32)).astype(jnp.bfloat16)


def rms_norm_bwd(x_rows, gain_vec, d_out):
    x_f32 = x_rows.astype(jnp.float32)
    inv_rms = lax.rsqrt(jnp.mean(x_f32 * x_f32, axis=-1, keepdims=True) + EPS)
    d_gain = jnp.sum(d_out * x_f32 * inv_rms, axis=0)
    d_scaled = d_out * gain_vec.astype(jnp.float32)
    d_x = inv_rms * d_scaled - x_f32 * inv_rms ** 3 * jnp.mean(d_scaled * x_f32, axis=-1, keepdims=True)
    return d_x, d_gain


def rope_rotate(head_vals):
    seq_len = head_vals.shape[1]
    half_dim = head_vals.shape[-1] // 2
    inv_freq = ROPE_BASE ** (-jnp.arange(half_dim, dtype=jnp.float32) / half_dim)
    angles = jnp.arange(seq_len, dtype=jnp.float32)[:, None] * inv_freq[None, :]
    cos_b = jnp.cos(angles)[None, :, None, :]
    sin_b = jnp.sin(angles)[None, :, None, :]
    lower_half = head_vals[..., :half_dim]
    upper_half = head_vals[..., half_dim:]
    return jnp.concatenate([lower_half * cos_b - upper_half * sin_b, upper_half * cos_b + lower_half * sin_b], axis=-1)


def attention_core(qkv_rows, num_seqs):
    num_tokens = qkv_rows.shape[0]
    seq_len = num_tokens // num_seqs
    model_width = qkv_rows.shape[1] // 3
    qkv_heads = qkv_rows.reshape(num_seqs, seq_len, 3, model_width // HEAD_DIM, HEAD_DIM)
    query_rot = rope_rotate(qkv_heads[:, :, 0]).astype(jnp.bfloat16)
    key_rot = rope_rotate(qkv_heads[:, :, 1]).astype(jnp.bfloat16)
    value_h = qkv_heads[:, :, 2].astype(jnp.bfloat16)
    scores = jnp.einsum('bqhd,bkhd->bhqk', query_rot, key_rot, preferred_element_type=jnp.float32) * HEAD_DIM ** -0.5
    causal = jnp.arange(seq_len)[:, None] >= jnp.arange(seq_len)[None, :]
    attn_probs = jax.nn.softmax(jnp.where(causal, scores, -1e30), axis=-1).astype(jnp.bfloat16)
    context = jnp.einsum('bhqk,bkhd->bqhd', attn_probs, value_h, preferred_element_type=jnp.float32)
    return context.astype(jnp.bfloat16).reshape(num_tokens, model_width)


def gate_probs(logits, idx_cols):
    probs_all = jax.nn.softmax(logits, axis=-1)
    chosen = idx_cols[:, :, None] == jnp.arange(logits.shape[1], dtype=jnp.int32)[None, None, :]
    picked = jnp.sum(jnp.where(chosen, probs_all[None], 0.0), axis=2)
    return picked / jnp.sum(picked, axis=0, keepdims=True)


def slot_positions(local_idx, local_experts, capacity):
    num_tokens = local_idx.shape[-1]
    expert_ids = jnp.arange(local_experts, dtype=jnp.int32)
    member = jnp.any(local_idx[None] == expert_ids[:, None, None, None], axis=2)
    before = (jnp.arange(num_tokens)[:, None] < jnp.arange(num_tokens)[None, :]).astype(BF16)
    earlier = jnp.einsum('est,tv->esv', member.astype(BF16), before, preferred_element_type=F32)
    return jnp.where(member & (earlier < capacity), earlier.astype(jnp.int32), -1)


def mat_nn(left, right):
    return lax.dot_general(left, right, (((1,), (0,)), ((), ())), preferred_element_type=F32)


def mat_nt(left, right):
    return lax.dot_general(left, right, (((1,), (1,)), ((), ())), preferred_element_type=F32)


def mat_tn(left, right):
    return lax.dot_general(left, right, (((0,), (0,)), ((), ())), preferred_element_type=F32)


def swiglu_bwd(half_gate, act_up, d_hidden):
    twice_sig = 1.0 + jnp.tanh(half_gate)
    silu = half_gate * twice_sig
    hidden = (silu * act_up).astype(BF16)
    d_act_up = (d_hidden * silu).astype(BF16)
    twice_d_act_gate = (d_hidden * act_up * (twice_sig + silu * (2.0 - twice_sig))).astype(BF16)
    return hidden, twice_d_act_gate, d_act_up


def token_grad_kernel(capacity, group, f_tile, pos_ref, idx_ref, gate_ref, rows_ref, dy_ref, w_gate_ref, w_up_ref, w_down_ref,
                      d_rows_ref, d_gates_ref, slot_gate_ref, d_w_gate_ref, d_w_up_ref, d_w_down_ref,
                      select_scr, in_scr, raw_scr, dout_scr, din_scr):
    sources, num_tokens, _ = rows_ref.shape
    ff = w_gate_ref.shape[2]
    first = pl.program_id(0) * group
    slot_iota = lax.broadcasted_iota(jnp.int32, (capacity, num_tokens), 0)
    diagonal = lax.broadcasted_iota(jnp.int32, (capacity, 128), 0) == lax.broadcasted_iota(jnp.int32, (capacity, 128), 1)

    @pl.when(pl.program_id(0) == 0)
    def _():
        d_rows_ref[...] = jnp.zeros_like(d_rows_ref)
        d_gates_ref[...] = jnp.zeros_like(d_gates_ref)

    def select(source):
        selectors, gate_cols = [], []
        for member in range(group):
            hit = slot_iota == pos_ref[member, source:source + 1, :]
            gate_row = jnp.sum(jnp.where(idx_ref[source] == first + member, gate_ref[source], 0.0), axis=0, keepdims=True)
            gate_col = jnp.sum(jnp.where(hit, gate_row, 0.0), axis=1, keepdims=True)
            slot_gate_ref[member, source:source + 1, :] = jnp.sum(jnp.where(diagonal, gate_col, 0.0), axis=0, keepdims=True)
            gate_cols.append(gate_col)
            selectors.append(jnp.where(hit, 1.0, 0.0).astype(BF16))
        return jnp.concatenate(selectors, axis=0), jnp.concatenate(gate_cols, axis=0)

    ahead = select(0)
    for source in range(sources):
        selector, gate_col = ahead
        if source + 1 < sources:
            ahead = select(source + 1)
        select_scr[source] = selector
        slot_rows = mat_nn(selector, rows_ref[source]).astype(BF16)
        raw_dy = mat_nn(selector, dy_ref[source, :num_tokens])
        scaled_dy = (raw_dy * gate_col).astype(BF16)
        raw_dy = raw_dy.astype(BF16)
        for member in range(group):
            span = slice(source * capacity, (source + 1) * capacity)
            part = slice(member * capacity, (member + 1) * capacity)
            in_scr[member, span] = slot_rows[part]
            raw_scr[member, span] = raw_dy[part]
            dout_scr[member, span] = scaled_dy[part]

    def forward(member, cols):
        slot_rows = in_scr[member]
        half_w_gate = w_gate_ref[member, :, cols] * jnp.asarray(0.5, BF16)
        return (half_w_gate, mat_nn(slot_rows, half_w_gate), mat_nn(slot_rows, w_up_ref[member, :, cols]),
                mat_nt(dout_scr[member], w_down_ref[member, cols, :]))

    steps = [(member, slice(f, f + f_tile)) for member in range(group) for f in range(0, ff, f_tile)]
    ahead = forward(*steps[0])
    for at, (member, cols) in enumerate(steps):
        half_w_gate, half_gate, act_up, d_hidden = ahead
        if at + 1 < len(steps):
            ahead = forward(*steps[at + 1])
        hidden, twice_d_act_gate, d_act_up = swiglu_bwd(half_gate, act_up, d_hidden)
        out_part = mat_nn(hidden, w_down_ref[member, cols, :])
        in_part = mat_nt(twice_d_act_gate, half_w_gate) + mat_nt(d_act_up, w_up_ref[member, :, cols])
        d_w_gate_ref[member, :, cols] = 0.5 * mat_tn(in_scr[member], twice_d_act_gate)
        d_w_up_ref[member, :, cols] = mat_tn(in_scr[member], d_act_up)
        d_w_down_ref[member, cols, :] = mat_tn(hidden, dout_scr[member])
        out_sum, in_sum = (out_part, in_part) if cols.start == 0 else (out_sum + out_part, in_sum + in_part)
        if cols.stop == ff:
            d_gate = jnp.sum(raw_scr[member].astype(F32) * out_sum.astype(BF16).astype(F32), axis=1, keepdims=True)
            d_in = in_sum.astype(BF16)
            for source in range(sources):
                part = slice(source * capacity, (source + 1) * capacity)
                din_scr[source, member * capacity:(member + 1) * capacity] = d_in[part]
                hit = slot_iota == pos_ref[member, source:source + 1, :]
                d_gate_row = jnp.sum(jnp.where(hit, d_gate[part], 0.0), axis=0, keepdims=True)
                d_gates_ref[source] += jnp.where(idx_ref[source] == first + member, d_gate_row, 0.0)

    for source in range(sources):
        d_rows_ref[source] += mat_tn(select_scr[source], din_scr[source])


def token_grads(positions, local_idx, gates, rows, dy_rows, w_gate, w_up, w_down, capacity):
    group = 4
    sources, num_tokens, width = rows.shape
    num_experts = w_gate.shape[0]
    slots = sources * capacity

    def whole(arr):
        return pl.BlockSpec(arr.shape, lambda step: (0,) * arr.ndim, pipeline_mode=pl.Buffered(1))

    def per_step(arr):
        return pl.BlockSpec((group,) + arr.shape[1:], lambda step: (step, 0, 0))

    slot_gates = jax.ShapeDtypeStruct((num_experts, sources, 128), F32)
    weights = [jax.ShapeDtypeStruct(arr.shape, F32) for arr in (w_gate, w_up, w_down)]
    return pl.pallas_call(
        functools.partial(token_grad_kernel, capacity, group, 256),
        grid=(num_experts // group,),
        in_specs=[per_step(positions), whole(local_idx), whole(gates), whole(rows), whole(dy_rows),
                  per_step(w_gate), per_step(w_up), per_step(w_down)],
        out_specs=[pl.BlockSpec(rows.shape, lambda step: (0, 0, 0)), pl.BlockSpec(gates.shape, lambda step: (0, 0, 0)),
                   per_step(slot_gates)] + [per_step(arr) for arr in weights],
        out_shape=[jax.ShapeDtypeStruct(rows.shape, F32), jax.ShapeDtypeStruct(gates.shape, F32), slot_gates] + weights,
        scratch_shapes=[pltpu.VMEM((sources, group * capacity, num_tokens), BF16),
                        pltpu.VMEM((group, slots, width), BF16), pltpu.VMEM((group, slots, width), BF16),
                        pltpu.VMEM((group, slots, width), BF16), pltpu.VMEM((sources, group * capacity, width), BF16)],
        compiler_params=pltpu.CompilerParams(vmem_limit_bytes=64_000_000, dimension_semantics=("arbitrary",)),
        cost_estimate=pl.CostEstimate(flops=60_000_000_000, bytes_accessed=130_000_000, transcendentals=0),
        name="expert_token_grads",
    )(positions, local_idx, gates, rows, dy_rows, w_gate, w_up, w_down)


def near_peers():
    ep = lax.axis_index('ep')
    return {'ep': ep + 1 - 2 * lax.rem(ep, 2)}, {'ep': lax.rem(ep + 2, 4)}


def meet(peers):
    barrier = pltpu.get_barrier_semaphore()
    for peer in peers:
        pl.semaphore_signal(barrier, inc=1, device_id=peer, device_id_type=pl.DeviceIdType.MESH)
    pl.semaphore_wait(barrier, len(peers))


def remote(src, dst, send_sem, recv_sem, peer):
    return pltpu.make_async_remote_copy(src_ref=src, dst_ref=dst, send_sem=send_sem, recv_sem=recv_sem,
                                        device_id=peer, device_id_type=pl.DeviceIdType.MESH)


def near_gather_kernel(rows_ref, gates_ref, rows_out, gates_out, send_sem, recv_sem):
    core_peer, chip_peer = near_peers()
    meet((core_peer, chip_peer))
    half = rows_ref.shape[0] // 2
    pieces = [(rows_ref.at[pl.ds(0, half)], lambda slot: rows_out.at[slot, pl.ds(0, half)]),
              (rows_ref.at[pl.ds(half, half)], lambda slot: rows_out.at[slot, pl.ds(half, half)]),
              (gates_ref, lambda slot: gates_out.at[slot])]
    across = [remote(src, place(2), send_sem.at[0, i], recv_sem.at[0, i], chip_peer) for i, (src, place) in enumerate(pieces)]
    beside = [remote(src, place(1), send_sem.at[1, i], recv_sem.at[1, i], core_peer) for i, (src, place) in enumerate(pieces)]
    onward = [remote(place(2), place(3), send_sem.at[2, i], recv_sem.at[2, i], core_peer) for i, (_, place) in enumerate(pieces)]
    for copy in across + beside:
        copy.start()
    rows_out[0] = rows_ref[...]
    gates_out[0] = gates_ref[...]
    for copy, forward in zip(across, onward):
        copy.wait_recv()
        forward.start()
    for copy in beside + onward:
        copy.wait()
    for copy in across:
        copy.wait_send()


def near_gather(rows, gates):
    vmem = pl.BlockSpec(memory_space=pltpu.VMEM)
    return pl.pallas_call(
        near_gather_kernel,
        in_specs=[vmem, vmem], out_specs=[vmem, vmem],
        out_shape=[jax.ShapeDtypeStruct((4,) + rows.shape, rows.dtype), jax.ShapeDtypeStruct((4,) + gates.shape, gates.dtype)],
        scratch_shapes=[pltpu.SemaphoreType.DMA((3, 3)), pltpu.SemaphoreType.DMA((3, 3))],
        compiler_params=pltpu.CompilerParams(collective_id=0, has_side_effects=True),
        cost_estimate=pl.CostEstimate(flops=10_000_000_000, bytes_accessed=10_000_000, transcendentals=0),
        name="near_gather",
    )(rows, gates)


def near_return_kernel(d_rows_ref, d_gates_ref, slot_gates_ref, rows_out, gates_out, slot_gates_out,
                       own_rows, pass_rows, sum_rows, last_rows, own_gates, pass_gates, sum_gates, last_gates,
                       send_sem, recv_sem, far_send_sem, far_recv_sem):
    core_peer, chip_peer = near_peers()
    dp = lax.axis_index('dp')
    dp_size = slot_gates_out.shape[0] + 1
    far_peers = [{'dp': lax.rem(dp + k, dp_size)} for k in range(1, dp_size)]
    meet([core_peer, chip_peer] + far_peers)
    first = [remote(d_rows_ref.at[3], pass_rows, send_sem.at[0], recv_sem.at[0], core_peer),
             remote(d_gates_ref.at[3], pass_gates, send_sem.at[1], recv_sem.at[1], core_peer)]
    second = [remote(d_rows_ref.at[1], own_rows, send_sem.at[2], recv_sem.at[2], core_peer),
              remote(d_gates_ref.at[1], own_gates, send_sem.at[3], recv_sem.at[3], core_peer)]
    third = [remote(sum_rows, last_rows, send_sem.at[4], recv_sem.at[4], chip_peer),
             remote(sum_gates, last_gates, send_sem.at[5], recv_sem.at[5], chip_peer)]
    far = [remote(slot_gates_ref, slot_gates_out.at[dp_size - 2 - k], far_send_sem.at[k], far_recv_sem.at[k], peer) for k, peer in enumerate(far_peers)]
    for copy in first + second:
        copy.start()
    for copy in first:
        copy.wait_recv()
    sum_rows[...] = d_rows_ref[2] + pass_rows[...]
    sum_gates[...] = d_gates_ref[2] + pass_gates[...]
    for copy in second:
        copy.wait_recv()
    rows_out[...] = d_rows_ref[0] + own_rows[...]
    gates_out[...] = d_gates_ref[0] + own_gates[...]
    for copy in third + far:
        copy.start()
    for copy in third:
        copy.wait_recv()
    rows_out[...] += last_rows[...]
    gates_out[...] += last_gates[...]
    for copy in far:
        copy.wait()
    for copy in first + second + third:
        copy.wait_send()


def near_return(d_rows, d_gates, slot_gates, dp_size):
    vmem = pl.BlockSpec(memory_space=pltpu.VMEM)
    rows = jax.ShapeDtypeStruct(d_rows.shape[1:], F32)
    gates = jax.ShapeDtypeStruct(d_gates.shape[1:], F32)
    return pl.pallas_call(
        near_return_kernel,
        in_specs=[vmem] * 3, out_specs=[vmem] * 3,
        out_shape=[rows, gates, jax.ShapeDtypeStruct((dp_size - 1,) + slot_gates.shape, F32)],
        scratch_shapes=[pltpu.VMEM(rows.shape, F32)] * 4 + [pltpu.VMEM(gates.shape, F32)] * 4
        + [pltpu.SemaphoreType.DMA((6,)), pltpu.SemaphoreType.DMA((6,)), pltpu.SemaphoreType.DMA((dp_size - 1,)), pltpu.SemaphoreType.DMA((dp_size - 1,))],
        compiler_params=pltpu.CompilerParams(collective_id=1, has_side_effects=True, vmem_limit_bytes=40_000_000),
        cost_estimate=pl.CostEstimate(flops=15_000_000_000, bytes_accessed=20_000_000, transcendentals=0),
        name="near_return",
    )(d_rows, d_gates, slot_gates)


def position_kernel(capacity, num_experts, idx_ref, pos_ref, member_scr):
    choices, sources, num_tokens = idx_ref.shape
    block = 256

    @pl.loop(0, num_experts)
    def _(expert):
        hit = idx_ref[0] == expert
        for choice in range(1, choices):
            hit = hit | (idx_ref[choice] == expert)
        member_scr[pl.ds(expert * sources, sources)] = jnp.where(hit, 1.0, 0.0).astype(BF16)

    before = jnp.where(lax.broadcasted_iota(jnp.int32, (num_tokens, num_tokens), 0) < lax.broadcasted_iota(jnp.int32, (num_tokens, num_tokens), 1), 1.0, 0.0).astype(BF16)

    @pl.loop(0, num_experts * sources // block)
    def _(step):
        span = pl.ds(pl.multiple_of(step * block, block), block)
        member = member_scr[span]
        earlier = mat_nn(member, before)
        pos_ref[span] = jnp.where((member.astype(F32) > 0.5) & (earlier < capacity), earlier, -1.0).astype(jnp.int32)


def all_positions(idx_by_choice, num_experts, capacity):
    _, sources, num_tokens = idx_by_choice.shape
    flat = pl.pallas_call(
        functools.partial(position_kernel, capacity, num_experts),
        out_shape=jax.ShapeDtypeStruct((num_experts * sources, num_tokens), jnp.int32),
        scratch_shapes=[pltpu.VMEM((num_experts * sources, num_tokens), BF16)],
        compiler_params=pltpu.CompilerParams(vmem_limit_bytes=32_000_000),
        cost_estimate=pl.CostEstimate(flops=4_000_000_000, bytes_accessed=5_000_000, transcendentals=0),
        name="slot_positions",
    )(idx_by_choice)
    return flat.reshape(num_experts, sources, num_tokens)


def weight_grad_kernel(capacity, group, f_tile, near, chunks, tail, count_ref, place_ref, pos_ref, slot_gate_ref, table_hbm,
                       w_gate_ref, w_up_ref, w_down_ref, near_gate_ref, near_up_ref, near_down_ref,
                       d_w_gate_ref, d_w_up_ref, d_w_down_ref, rows_scr, dy_scr, in_scr, dout_scr, down_scr, total_scr, load_sem):
    expert = pl.program_id(0)
    member = lax.rem(expert, group)
    far, num_tokens, _ = rows_scr.shape
    sources = far + near
    ff = w_gate_ref.shape[2]
    slot_iota = lax.broadcasted_iota(jnp.int32, (capacity, num_tokens), 0)
    diagonal = lax.broadcasted_iota(jnp.int32, (capacity, 128), 0) == lax.broadcasted_iota(jnp.int32, (capacity, 128), 1)

    def source_of(index):
        return lax.rem(place_ref[0] * near + near + index - lax.rem(index, near), sources) + jnp.bitwise_xor(lax.rem(index, near), place_ref[1])

    def loads(index):
        source = source_of(index)
        return (pltpu.make_async_copy(table_hbm.at[source, pl.ds(0, num_tokens)], rows_scr.at[index], load_sem.at[0, index]),
                pltpu.make_async_copy(table_hbm.at[source, pl.ds(num_tokens, num_tokens)], dy_scr.at[index], load_sem.at[1, index]))

    @pl.when(expert == 0)
    def _():
        @pl.loop(0, far)
        def _(index):
            for copy in loads(index):
                copy.start()

    def select(index):
        source = source_of(index)
        selectors, gate_cols = [], []
        for k in range(group):
            selectors.append(jnp.where(slot_iota == pos_ref[k, pl.ds(source, 1), :], 1.0, 0.0).astype(BF16))
            gate_cols.append(jnp.sum(jnp.where(diagonal, slot_gate_ref[k, pl.ds(index, 1), :], 0.0), axis=1, keepdims=True))
        return jnp.concatenate(selectors, axis=0), jnp.concatenate(gate_cols, axis=0)

    @pl.when(member == 0)
    def _():
        unroll = 2

        def body(step, starts):
            @pl.when(expert == 0)
            def _():
                for j in range(unroll):
                    for copy in loads(step * unroll + j):
                        copy.wait()

            ahead = select(step * unroll)
            for j in range(unroll):
                index = step * unroll + j
                selector, gate_col = ahead
                if j + 1 < unroll:
                    ahead = select(index + 1)
                slot_rows = mat_nn(selector, rows_scr[index]).astype(BF16)
                scaled_dy = (mat_nn(selector, dy_scr[index]) * gate_col).astype(BF16)
                for k in range(group):
                    span = pl.ds(pl.multiple_of(starts[k], 16), capacity)
                    part = slice(k * capacity, (k + 1) * capacity)
                    in_scr[k, span] = slot_rows[part]
                    dout_scr[k, span] = scaled_dy[part]
                starts = tuple(starts[k] + count_ref[expert + k, source_of(index)] for k in range(group))
            return starts

        ends = lax.fori_loop(0, far // unroll, body, (jnp.int32(0),) * group)
        empty = jnp.zeros((tail, in_scr.shape[2]), BF16)
        for k in range(group):
            total_scr[k] = ends[k]
            span = pl.ds(pl.multiple_of(ends[k], 16), tail)
            in_scr[k, span] = empty
            dout_scr[k, span] = empty

            @pl.loop((ends[k] + tail - 1) // tail, sum(chunks) // tail)
            def _(block):
                span = pl.ds(pl.multiple_of(block * tail, tail), tail)
                in_scr[k, span] = empty
                dout_scr[k, span] = empty

    def forward(start, size, cols):
        slot_rows = in_scr[member, pl.ds(start, size)]
        d_out = dout_scr[member, pl.ds(start, size)]
        return (slot_rows, d_out, mat_nn(slot_rows, w_gate_ref[0, :, cols] * jnp.asarray(0.5, BF16)), mat_nn(slot_rows, w_up_ref[0, :, cols]),
                mat_nt(d_out, w_down_ref[0, cols, :]))

    def accumulate(steps):
        ahead = forward(*steps[0])
        for at, (start, _, cols) in enumerate(steps):
            slot_rows, d_out, half_gate, act_up, d_hidden = ahead
            if at + 1 < len(steps):
                ahead = forward(*steps[at + 1])
            hidden, twice_d_act_gate, d_act_up = swiglu_bwd(half_gate, act_up, d_hidden)
            gate_base, up_base = (near_gate_ref, near_up_ref) if start == 0 else (d_w_gate_ref, d_w_up_ref)
            d_w_gate_ref[0, :, cols] = gate_base[0, :, cols] + 0.5 * mat_tn(slot_rows, twice_d_act_gate)
            d_w_up_ref[0, :, cols] = up_base[0, :, cols] + mat_tn(slot_rows, d_act_up)
            down_part = mat_tn(d_out, hidden)
            down_scr[:, cols] = down_part if start == 0 else down_scr[:, cols] + down_part

    tiles = [slice(f, f + f_tile) for f in range(0, ff, f_tile)]
    accumulate([(sum(chunks[:c]), size, cols) for c, size in enumerate(chunks) for cols in tiles])

    @pl.when(total_scr[member] > sum(chunks))
    def _():
        for start in range(sum(chunks), far * capacity, tail):
            accumulate([(start, tail, cols) for cols in tiles])

    d_w_down_ref[0] = near_down_ref[0] + down_scr[...].T


def weight_grads(positions, counts, place, slot_gates, table, w_gate, w_up, w_down, near_grads, capacity):
    group = 4
    near = 4
    tail = 256
    sources, num_tokens = positions.shape[1:]
    width = table.shape[2]
    far = sources - near
    num_experts, _, ff = w_gate.shape
    chunks = (1024, 1024)
    slots = far * capacity + tail

    def per_step(arr):
        return pl.BlockSpec((1,) + arr.shape[1:], lambda step, *_: (step, 0, 0))

    hbm = pl.BlockSpec(memory_space=pl.ANY)
    weights = (w_gate, w_up, w_down)
    return pl.pallas_call(
        functools.partial(weight_grad_kernel, capacity, group, 256, near, chunks, tail),
        grid_spec=pltpu.PrefetchScalarGridSpec(
            num_scalar_prefetch=2, grid=(num_experts,),
            in_specs=[pl.BlockSpec((group, sources, num_tokens), lambda step, *_: (step // group, 0, 0)),
                      pl.BlockSpec((group, far, 128), lambda step, *_: (step // group, 0, 0)),
                      hbm] + [per_step(arr) for arr in weights] * 2,
            out_specs=[per_step(arr) for arr in weights],
            scratch_shapes=[pltpu.VMEM((far, num_tokens, width), BF16), pltpu.VMEM((far, num_tokens, width), BF16),
                            pltpu.VMEM((group, slots, width), BF16), pltpu.VMEM((group, slots, width), BF16),
                            pltpu.VMEM((width, ff), F32), pltpu.SMEM((group,), jnp.int32), pltpu.SemaphoreType.DMA((2, far))]),
        out_shape=[jax.ShapeDtypeStruct(arr.shape, F32) for arr in weights],
        compiler_params=pltpu.CompilerParams(vmem_limit_bytes=67_000_000, dimension_semantics=("arbitrary",)),
        cost_estimate=pl.CostEstimate(flops=280_000_000_000, bytes_accessed=225_000_000, transcendentals=0),
        name="expert_weight_grads",
    )(counts, place, positions, slot_gates, table, w_gate, w_up, w_down, *near_grads)


def dense_forward(x_rows, idx_cols, num_seqs, norm1_gain, norm2_gain, w_qkv, w_attn_out, w_router):
    normed1 = rms_norm(x_rows, norm1_gain)
    qkv_rows = jnp.dot(normed1, w_qkv, preferred_element_type=jnp.float32)
    context, attn_pullback = jax.vjp(lambda qkv_in: attention_core(qkv_in, num_seqs), qkv_rows)
    h_rows = (x_rows.astype(jnp.float32) + jnp.dot(context, w_attn_out, preferred_element_type=jnp.float32)).astype(jnp.bfloat16)
    normed2 = rms_norm(h_rows, norm2_gain)
    logits = jnp.dot(normed2, w_router, preferred_element_type=jnp.float32)
    gate_vals, gate_pullback = jax.vjp(lambda logit_in: gate_probs(logit_in, idx_cols), logits)
    saved_state = (normed1, attn_pullback, context, h_rows, normed2, gate_pullback)
    return normed2, gate_vals, saved_state


def dense_backward(saved_state, x_rows, dy_rows, d_gates, d_normed2_moe, norm1_gain, norm2_gain, w_qkv, w_attn_out, w_router):
    normed1, attn_pullback, context, h_rows, normed2, gate_pullback = saved_state
    d_logits = gate_pullback(d_gates)[0].astype(jnp.bfloat16)
    d_w_router = jnp.einsum('td,te->de', normed2, d_logits, preferred_element_type=jnp.float32)
    d_normed2 = d_normed2_moe + jnp.einsum('te,de->td', d_logits, w_router, preferred_element_type=jnp.float32)
    d_h_part, d_norm2_gain = rms_norm_bwd(h_rows, norm2_gain, d_normed2)
    d_h = (dy_rows.astype(jnp.float32) + d_h_part).astype(jnp.bfloat16)
    d_w_attn_out = jnp.einsum('td,te->de', context, d_h, preferred_element_type=jnp.float32)
    d_context = jnp.einsum('te,de->td', d_h, w_attn_out, preferred_element_type=jnp.float32).astype(jnp.bfloat16)
    d_qkv = attn_pullback(d_context)[0].astype(jnp.bfloat16)
    d_w_qkv = jnp.einsum('td,te->de', normed1, d_qkv, preferred_element_type=jnp.float32)
    d_normed1 = jnp.einsum('te,de->td', d_qkv, w_qkv, preferred_element_type=jnp.float32)
    d_x_part, d_norm1_gain = rms_norm_bwd(x_rows, norm1_gain, d_normed1)
    d_x = (d_h.astype(jnp.float32) + d_x_part).astype(jnp.bfloat16)
    return d_x, (d_norm1_gain, d_norm2_gain, d_w_qkv, d_w_attn_out, d_w_router)


def solution(mesh):
    ep_size = mesh.shape['ep']
    tok_spec = P(('dp', 'ep'), None, None)
    rep_spec = P()
    exp_spec = P('ep', None, None)

    def local_step(x_tokens, dy_tokens, route_idx, norm1_gain, norm2_gain, w_qkv, w_attn_out, w_router, w_gate, w_up, w_down):
        num_seqs, seq_len, model_width = x_tokens.shape
        num_tokens = num_seqs * seq_len
        top_k = route_idx.shape[-1]
        local_experts = w_gate.shape[0]
        num_experts = local_experts * ep_size
        capacity = capacity_rows(num_tokens, top_k, num_experts)
        x_rows = x_tokens.reshape(num_tokens, model_width)
        dy_rows = dy_tokens.reshape(num_tokens, model_width)
        idx_cols = route_idx.reshape(num_tokens, top_k).T
        routes = idx_cols.astype(BF16).reshape(-1, model_width)
        payload = jnp.concatenate([dy_rows, routes], axis=0)
        moved = [lax.ppermute(payload, 'ep', [(i, i ^ k) for i in range(ep_size)]) for k in range(1, ep_size)]
        dy_near = jnp.stack([payload] + moved)

        def expert_of(gathered):
            return gathered.reshape(-1, top_k, num_tokens).astype(jnp.int32) - lax.axis_index('ep') * local_experts

        idx_near = expert_of(dy_near[:, num_tokens:])
        positions_near = slot_positions(idx_near, local_experts, capacity)
        normed2, gate_vals, saved_state = dense_forward(x_rows, idx_cols, num_seqs, norm1_gain, norm2_gain, w_qkv, w_attn_out, w_router)
        table = lax.all_gather(jnp.concatenate([normed2, payload], axis=0), ('dp', 'ep'))
        rows_near, gates_near = near_gather(normed2, gate_vals)
        d_near, d_gate_near, slot_gates, *near_grads = token_grads(positions_near, idx_near, gates_near, rows_near, dy_near, w_gate, w_up, w_down, capacity)
        d_normed2_moe, d_gates, slot_gates_all = near_return(d_near, d_gate_near, slot_gates, mesh.shape['dp'])
        slot_gates_all = slot_gates_all.transpose(1, 0, 2, 3).reshape(local_experts, -1, 128)
        d_x, dense_grads = dense_backward(saved_state, x_rows, dy_rows, d_gates, d_normed2_moe, norm1_gain, norm2_gain, w_qkv, w_attn_out, w_router)
        gain_cols = jnp.zeros((model_width, 128), F32).at[:, 0].set(dense_grads[0]).at[:, 1].set(dense_grads[1])
        packed = jnp.concatenate(dense_grads[2:] + (gain_cols,), axis=1)
        packed, slot_gates_all = lax.optimization_barrier((packed, slot_gates_all))
        positions = all_positions(expert_of(table[:, 2 * num_tokens:]).transpose(1, 0, 2), local_experts, capacity)
        counts = (jnp.max(positions, axis=2) + 16) // 16 * 16
        place = jnp.stack([lax.axis_index('dp'), lax.axis_index('ep')]).astype(jnp.int32)
        expert_grads = weight_grads(positions, counts, place, slot_gates_all, table, w_gate, w_up, w_down, near_grads, capacity)
        packed = lax.psum(packed, ('dp', 'ep'))
        qkv_end = w_qkv.shape[1]
        out_end = qkv_end + w_attn_out.shape[1]
        router_end = out_end + num_experts
        dense_out = (packed[:, router_end], packed[:, router_end + 1], packed[:, :qkv_end], packed[:, qkv_end:out_end], packed[:, out_end:router_end])
        return (d_x.reshape(x_tokens.shape),) + dense_out + tuple(expert_grads)

    return jax.shard_map(local_step, mesh=mesh,
                          in_specs=(tok_spec, tok_spec, tok_spec, rep_spec, rep_spec, rep_spec, rep_spec, rep_spec, exp_spec, exp_spec, exp_spec),
                          out_specs=(tok_spec, rep_spec, rep_spec, rep_spec, rep_spec, rep_spec, exp_spec, exp_spec, exp_spec),
                          check_vma=False)
```

```python
import functools

import jax
import jax.numpy as jnp
from jax import lax
from jax.experimental import pallas as pl
from jax.experimental.pallas import tpu as pltpu
from jax.sharding import PartitionSpec as P


F32 = jnp.float32
BF16 = jnp.bfloat16
EPS = 1e-6
HEAD_DIM = 128
ROPE_BASE = 10000.0


def capacity_rows(num_tokens, top_k, num_experts):
    return 8 * ((5 * num_tokens * top_k + 32 * num_experts - 1) // (32 * num_experts))


def slot_positions(local_idx, local_experts, capacity):
    num_tokens = local_idx.shape[-1]
    expert_ids = jnp.arange(local_experts, dtype=jnp.int32)
    member = jnp.any(local_idx[None] == expert_ids[:, None, None, None], axis=2)
    before = (jnp.arange(num_tokens)[:, None] < jnp.arange(num_tokens)[None, :]).astype(BF16)
    earlier = jnp.einsum('est,tv->esv', member.astype(BF16), before, preferred_element_type=F32)
    return jnp.where(member & (earlier < capacity), earlier.astype(jnp.int32), -1)


def mat_nn(left, right):
    return lax.dot_general(left, right, (((1,), (0,)), ((), ())), preferred_element_type=F32)


def mat_nt(left, right):
    return lax.dot_general(left, right, (((1,), (1,)), ((), ())), preferred_element_type=F32)


def mat_tn(left, right):
    return lax.dot_general(left, right, (((0,), (0,)), ((), ())), preferred_element_type=F32)


def swiglu_bwd(half_gate, act_up, d_hidden):
    twice_sig = 1.0 + jnp.tanh(half_gate)
    silu = half_gate * twice_sig
    hidden = (silu * act_up).astype(BF16)
    d_act_up = (d_hidden * silu).astype(BF16)
    twice_d_act_gate = (d_hidden * act_up * (twice_sig + silu * (2.0 - twice_sig))).astype(BF16)
    return hidden, twice_d_act_gate, d_act_up


def token_grad_kernel(capacity, group, f_tile, pos_ref, idx_ref, gate_ref, rows_ref, dy_ref, w_gate_ref, w_up_ref, w_down_ref,
                      d_rows_ref, d_gates_ref, slot_gate_ref, d_w_gate_ref, d_w_up_ref, d_w_down_ref,
                      select_scr, in_scr, raw_scr, dout_scr, din_scr):
    sources, num_tokens, _ = rows_ref.shape
    ff = w_gate_ref.shape[2]
    first = pl.program_id(0) * group
    slot_iota = lax.broadcasted_iota(jnp.int32, (capacity, num_tokens), 0)
    diagonal = lax.broadcasted_iota(jnp.int32, (capacity, 128), 0) == lax.broadcasted_iota(jnp.int32, (capacity, 128), 1)

    @pl.when(pl.program_id(0) == 0)
    def _():
        d_rows_ref[...] = jnp.zeros_like(d_rows_ref)
        d_gates_ref[...] = jnp.zeros_like(d_gates_ref)

    def select(source):
        selectors, gate_cols = [], []
        for member in range(group):
            hit = slot_iota == pos_ref[member, source:source + 1, :]
            gate_row = jnp.sum(jnp.where(idx_ref[source] == first + member, gate_ref[source], 0.0), axis=0, keepdims=True)
            gate_col = jnp.sum(jnp.where(hit, gate_row, 0.0), axis=1, keepdims=True)
            slot_gate_ref[member, source:source + 1, :] = jnp.sum(jnp.where(diagonal, gate_col, 0.0), axis=0, keepdims=True)
            gate_cols.append(gate_col)
            selectors.append(jnp.where(hit, 1.0, 0.0).astype(BF16))
        return jnp.concatenate(selectors, axis=0), jnp.concatenate(gate_cols, axis=0)

    ahead = select(0)
    for source in range(sources):
        selector, gate_col = ahead
        if source + 1 < sources:
            ahead = select(source + 1)
        select_scr[source] = selector
        slot_rows = mat_nn(selector, rows_ref[source]).astype(BF16)
        raw_dy = mat_nn(selector, dy_ref[source, :num_tokens])
        scaled_dy = (raw_dy * gate_col).astype(BF16)
        raw_dy = raw_dy.astype(BF16)
        for member in range(group):
            span = slice(source * capacity, (source + 1) * capacity)
            part = slice(member * capacity, (member + 1) * capacity)
            in_scr[member, span] = slot_rows[part]
            raw_scr[member, span] = raw_dy[part]
            dout_scr[member, span] = scaled_dy[part]

    def forward(member, cols):
        slot_rows = in_scr[member]
        half_w_gate = w_gate_ref[member, :, cols] * jnp.asarray(0.5, BF16)
        return (half_w_gate, mat_nn(slot_rows, half_w_gate), mat_nn(slot_rows, w_up_ref[member, :, cols]),
                mat_nt(dout_scr[member], w_down_ref[member, cols, :]))

    steps = [(member, slice(f, f + f_tile)) for member in range(group) for f in range(0, ff, f_tile)]
    ahead = forward(*steps[0])
    for at, (member, cols) in enumerate(steps):
        half_w_gate, half_gate, act_up, d_hidden = ahead
        if at + 1 < len(steps):
            ahead = forward(*steps[at + 1])
        hidden, twice_d_act_gate, d_act_up = swiglu_bwd(half_gate, act_up, d_hidden)
        out_part = mat_nn(hidden, w_down_ref[member, cols, :])
        in_part = mat_nt(twice_d_act_gate, half_w_gate) + mat_nt(d_act_up, w_up_ref[member, :, cols])
        d_w_gate_ref[member, :, cols] = 0.5 * mat_tn(in_scr[member], twice_d_act_gate)
        d_w_up_ref[member, :, cols] = mat_tn(in_scr[member], d_act_up)
        d_w_down_ref[member, cols, :] = mat_tn(hidden, dout_scr[member])
        out_sum, in_sum = (out_part, in_part) if cols.start == 0 else (out_sum + out_part, in_sum + in_part)
        if cols.stop == ff:
            d_gate = jnp.sum(raw_scr[member].astype(F32) * out_sum.astype(BF16).astype(F32), axis=1, keepdims=True)
            d_in = in_sum.astype(BF16)
            for source in range(sources):
                part = slice(source * capacity, (source + 1) * capacity)
                din_scr[source, member * capacity:(member + 1) * capacity] = d_in[part]
                hit = slot_iota == pos_ref[member, source:source + 1, :]
                d_gate_row = jnp.sum(jnp.where(hit, d_gate[part], 0.0), axis=0, keepdims=True)
                d_gates_ref[source] += jnp.where(idx_ref[source] == first + member, d_gate_row, 0.0)

    for source in range(sources):
        d_rows_ref[source] += mat_tn(select_scr[source], din_scr[source])


def token_grads(positions, local_idx, gates, rows, dy_rows, w_gate, w_up, w_down, capacity):
    group = 4
    sources, num_tokens, width = rows.shape
    num_experts = w_gate.shape[0]
    slots = sources * capacity

    def whole(arr):
        return pl.BlockSpec(arr.shape, lambda step: (0,) * arr.ndim, pipeline_mode=pl.Buffered(1))

    def per_step(arr):
        return pl.BlockSpec((group,) + arr.shape[1:], lambda step: (step, 0, 0))

    slot_gates = jax.ShapeDtypeStruct((num_experts, sources, 128), F32)
    weights = [jax.ShapeDtypeStruct(arr.shape, F32) for arr in (w_gate, w_up, w_down)]
    return pl.pallas_call(
        functools.partial(token_grad_kernel, capacity, group, 256),
        grid=(num_experts // group,),
        in_specs=[per_step(positions), whole(local_idx), whole(gates), whole(rows), whole(dy_rows),
                  per_step(w_gate), per_step(w_up), per_step(w_down)],
        out_specs=[pl.BlockSpec(rows.shape, lambda step: (0, 0, 0)), pl.BlockSpec(gates.shape, lambda step: (0, 0, 0)),
                   per_step(slot_gates)] + [per_step(arr) for arr in weights],
        out_shape=[jax.ShapeDtypeStruct(rows.shape, F32), jax.ShapeDtypeStruct(gates.shape, F32), slot_gates] + weights,
        scratch_shapes=[pltpu.VMEM((sources, group * capacity, num_tokens), BF16),
                        pltpu.VMEM((group, slots, width), BF16), pltpu.VMEM((group, slots, width), BF16),
                        pltpu.VMEM((group, slots, width), BF16), pltpu.VMEM((sources, group * capacity, width), BF16)],
        compiler_params=pltpu.CompilerParams(vmem_limit_bytes=64_000_000, dimension_semantics=("arbitrary",)),
        cost_estimate=pl.CostEstimate(flops=60_000_000_000, bytes_accessed=130_000_000, transcendentals=0),
        name="expert_token_grads",
    )(positions, local_idx, gates, rows, dy_rows, w_gate, w_up, w_down)


def near_peers():
    ep = lax.axis_index('ep')
    return {'ep': ep + 1 - 2 * lax.rem(ep, 2)}, {'ep': lax.rem(ep + 2, 4)}


def meet(peers):
    barrier = pltpu.get_barrier_semaphore()
    for peer in peers:
        pl.semaphore_signal(barrier, inc=1, device_id=peer, device_id_type=pl.DeviceIdType.MESH)
    pl.semaphore_wait(barrier, len(peers))


def remote(src, dst, send_sem, recv_sem, peer):
    return pltpu.make_async_remote_copy(src_ref=src, dst_ref=dst, send_sem=send_sem, recv_sem=recv_sem,
                                        device_id=peer, device_id_type=pl.DeviceIdType.MESH)


def near_gather_kernel(rows_ref, gates_ref, rows_out, gates_out, send_sem, recv_sem):
    core_peer, chip_peer = near_peers()
    meet((core_peer, chip_peer))
    num_tokens = rows_out.shape[1]
    half = num_tokens // 2
    pieces = [(rows_ref.at[pl.ds(0, half)], lambda slot: rows_out.at[slot, pl.ds(0, half)]),
              (rows_ref.at[pl.ds(half, half)], lambda slot: rows_out.at[slot, pl.ds(half, half)]),
              (gates_ref, lambda slot: gates_out.at[slot])]
    across = [remote(src, place(2), send_sem.at[0, i], recv_sem.at[0, i], chip_peer) for i, (src, place) in enumerate(pieces)]
    beside = [remote(src, place(1), send_sem.at[1, i], recv_sem.at[1, i], core_peer) for i, (src, place) in enumerate(pieces)]
    onward = [remote(place(2), place(3), send_sem.at[2, i], recv_sem.at[2, i], core_peer) for i, (_, place) in enumerate(pieces)]
    for copy in across + beside:
        copy.start()
    rows_out[0] = rows_ref[0:num_tokens]
    gates_out[0] = gates_ref[...]
    for copy, forward in zip(across, onward):
        copy.wait_recv()
        forward.start()
    for copy in beside + onward:
        copy.wait()
    for copy in across:
        copy.wait_send()


def near_gather(rows, gates, num_tokens):
    vmem = pl.BlockSpec(memory_space=pltpu.VMEM)
    return pl.pallas_call(
        near_gather_kernel,
        in_specs=[vmem, vmem], out_specs=[vmem, vmem],
        out_shape=[jax.ShapeDtypeStruct((4, num_tokens, rows.shape[1]), rows.dtype), jax.ShapeDtypeStruct((4,) + gates.shape, gates.dtype)],
        scratch_shapes=[pltpu.SemaphoreType.DMA((3, 3)), pltpu.SemaphoreType.DMA((3, 3))],
        compiler_params=pltpu.CompilerParams(collective_id=0, has_side_effects=True),
        cost_estimate=pl.CostEstimate(flops=10_000_000_000, bytes_accessed=10_000_000, transcendentals=0),
        name="near_gather",
    )(rows, gates)


def near_return_kernel(d_rows_ref, d_gates_ref, slot_gates_ref, routes_ref, rows_out, gates_out, slot_gates_out, routes_out,
                       own_rows, pass_rows, sum_rows, last_rows, own_gates, pass_gates, sum_gates, last_gates,
                       send_sem, recv_sem, far_send_sem, far_recv_sem):
    core_peer, chip_peer = near_peers()
    dp = lax.axis_index('dp')
    dp_size = slot_gates_out.shape[0] + 1
    far_peers = [{'dp': lax.rem(dp + k, dp_size)} for k in range(1, dp_size)]
    meet([core_peer, chip_peer] + far_peers)
    first = [remote(d_rows_ref.at[3], pass_rows, send_sem.at[0], recv_sem.at[0], core_peer),
             remote(d_gates_ref.at[3], pass_gates, send_sem.at[1], recv_sem.at[1], core_peer)]
    second = [remote(d_rows_ref.at[1], own_rows, send_sem.at[2], recv_sem.at[2], core_peer),
              remote(d_gates_ref.at[1], own_gates, send_sem.at[3], recv_sem.at[3], core_peer)]
    third = [remote(sum_rows, last_rows, send_sem.at[4], recv_sem.at[4], chip_peer),
             remote(sum_gates, last_gates, send_sem.at[5], recv_sem.at[5], chip_peer)]
    far = [remote(slot_gates_ref, slot_gates_out.at[dp_size - 2 - k], far_send_sem.at[0, k], far_recv_sem.at[0, k], peer) for k, peer in enumerate(far_peers)]
    far += [remote(routes_ref, routes_out.at[dp_size - 1 - k], far_send_sem.at[1, k], far_recv_sem.at[1, k], peer) for k, peer in enumerate(far_peers)]
    for copy in first + second:
        copy.start()
    for copy in first:
        copy.wait_recv()
    sum_rows[...] = d_rows_ref[2] + pass_rows[...]
    sum_gates[...] = d_gates_ref[2] + pass_gates[...]
    for copy in second:
        copy.wait_recv()
    rows_out[...] = d_rows_ref[0] + own_rows[...]
    gates_out[...] = d_gates_ref[0] + own_gates[...]
    for copy in third + far:
        copy.start()
    routes_out[0] = routes_ref[...]
    for copy in third:
        copy.wait_recv()
    rows_out[...] += last_rows[...]
    gates_out[...] += last_gates[...]
    for copy in far:
        copy.wait()
    for copy in first + second + third:
        copy.wait_send()


def near_return(d_rows, d_gates, slot_gates, routes, dp_size):
    vmem = pl.BlockSpec(memory_space=pltpu.VMEM)
    rows = jax.ShapeDtypeStruct(d_rows.shape[1:], F32)
    gates = jax.ShapeDtypeStruct(d_gates.shape[1:], F32)
    return pl.pallas_call(
        near_return_kernel,
        in_specs=[vmem] * 4, out_specs=[vmem] * 4,
        out_shape=[rows, gates, jax.ShapeDtypeStruct((dp_size - 1,) + slot_gates.shape, F32), jax.ShapeDtypeStruct((dp_size,) + routes.shape, BF16)],
        scratch_shapes=[pltpu.VMEM(rows.shape, F32)] * 4 + [pltpu.VMEM(gates.shape, F32)] * 4
        + [pltpu.SemaphoreType.DMA((6,)), pltpu.SemaphoreType.DMA((6,)), pltpu.SemaphoreType.DMA((2, dp_size - 1)), pltpu.SemaphoreType.DMA((2, dp_size - 1))],
        compiler_params=pltpu.CompilerParams(collective_id=1, has_side_effects=True, vmem_limit_bytes=40_000_000),
        cost_estimate=pl.CostEstimate(flops=15_000_000_000, bytes_accessed=20_000_000, transcendentals=0),
        name="near_return",
    )(d_rows, d_gates, slot_gates, routes)


def position_kernel(capacity, num_experts, idx_ref, pos_ref, member_scr):
    choices, sources, num_tokens = idx_ref.shape
    block = 256

    @pl.loop(0, num_experts)
    def _(expert):
        hit = idx_ref[0] == expert
        for choice in range(1, choices):
            hit = hit | (idx_ref[choice] == expert)
        member_scr[pl.ds(expert * sources, sources)] = jnp.where(hit, 1.0, 0.0).astype(BF16)

    before = jnp.where(lax.broadcasted_iota(jnp.int32, (num_tokens, num_tokens), 0) < lax.broadcasted_iota(jnp.int32, (num_tokens, num_tokens), 1), 1.0, 0.0).astype(BF16)

    @pl.loop(0, num_experts * sources // block)
    def _(step):
        span = pl.ds(pl.multiple_of(step * block, block), block)
        member = member_scr[span]
        earlier = mat_nn(member, before)
        pos_ref[span] = jnp.where((member.astype(F32) > 0.5) & (earlier < capacity), earlier, -1.0).astype(jnp.int32)


def all_positions(idx_by_choice, num_experts, capacity):
    _, sources, num_tokens = idx_by_choice.shape
    flat = pl.pallas_call(
        functools.partial(position_kernel, capacity, num_experts),
        out_shape=jax.ShapeDtypeStruct((num_experts * sources, num_tokens), jnp.int32),
        scratch_shapes=[pltpu.VMEM((num_experts * sources, num_tokens), BF16)],
        compiler_params=pltpu.CompilerParams(vmem_limit_bytes=32_000_000),
        cost_estimate=pl.CostEstimate(flops=4_000_000_000, bytes_accessed=5_000_000, transcendentals=0),
        name="slot_positions",
    )(idx_by_choice)
    return flat.reshape(num_experts, sources, num_tokens)


def weight_grad_kernel(capacity, group, f_tile, near, chunks, tail, count_ref, place_ref, pos_ref, slot_gate_ref, table_hbm,
                       w_gate_ref, w_up_ref, w_down_ref, near_gate_ref, near_up_ref, near_down_ref,
                       d_w_gate_ref, d_w_up_ref, d_w_down_ref, rows_scr, dy_scr, in_scr, dout_scr, total_scr, load_sem):
    expert = pl.program_id(0)
    member = lax.rem(expert, group)
    far, num_tokens, _ = rows_scr.shape
    sources = far + near
    ff = w_gate_ref.shape[2]
    slot_iota = lax.broadcasted_iota(jnp.int32, (capacity, num_tokens), 0)
    diagonal = lax.broadcasted_iota(jnp.int32, (capacity, 128), 0) == lax.broadcasted_iota(jnp.int32, (capacity, 128), 1)

    def source_of(index):
        return lax.rem(place_ref[0] * near + near + index - lax.rem(index, near), sources) + jnp.bitwise_xor(lax.rem(index, near), place_ref[1])

    def loads(index):
        source = source_of(index)
        return (pltpu.make_async_copy(table_hbm.at[source, pl.ds(0, num_tokens)], rows_scr.at[index], load_sem.at[0, index]),
                pltpu.make_async_copy(table_hbm.at[source, pl.ds(num_tokens, num_tokens)], dy_scr.at[index], load_sem.at[1, index]))

    @pl.when(expert == 0)
    def _():
        @pl.loop(0, far)
        def _(index):
            for copy in loads(index):
                copy.start()

    def select(index):
        selectors, gate_cols = [], []
        for k in range(group):
            selectors.append(jnp.where(slot_iota == pos_ref[k, pl.ds(index + near, 1), :], 1.0, 0.0).astype(BF16))
            gate_cols.append(jnp.sum(jnp.where(diagonal, slot_gate_ref[k, pl.ds(index, 1), :], 0.0), axis=1, keepdims=True))
        return jnp.concatenate(selectors, axis=0), jnp.concatenate(gate_cols, axis=0)

    @pl.when(member == 0)
    def _():
        unroll = 7

        def body(step, starts):
            @pl.when(expert == 0)
            def _():
                for j in range(unroll):
                    for copy in loads(step * unroll + j):
                        copy.wait()

            ahead = select(step * unroll)
            for j in range(unroll):
                index = step * unroll + j
                selector, gate_col = ahead
                if j + 1 < unroll:
                    ahead = select(index + 1)
                slot_rows = mat_nn(selector, rows_scr[index]).astype(BF16)
                scaled_dy = (mat_nn(selector, dy_scr[index]) * gate_col).astype(BF16)
                for k in range(group):
                    span = pl.ds(pl.multiple_of(starts[k], 16), capacity)
                    part = slice(k * capacity, (k + 1) * capacity)
                    in_scr[k, span] = slot_rows[part]
                    dout_scr[k, span] = scaled_dy[part]
                starts = tuple(starts[k] + count_ref[expert + k, index + near] for k in range(group))
            return starts

        ends = lax.fori_loop(0, far // unroll, body, (jnp.int32(0),) * group)
        empty = jnp.zeros((tail, in_scr.shape[2]), BF16)
        for k in range(group):
            total_scr[k] = ends[k]
            span = pl.ds(pl.multiple_of(ends[k], 16), tail)
            in_scr[k, span] = empty
            dout_scr[k, span] = empty

            @pl.loop((ends[k] + tail - 1) // tail, sum(chunks) // tail)
            def _(block):
                span = pl.ds(pl.multiple_of(block * tail, tail), tail)
                in_scr[k, span] = empty
                dout_scr[k, span] = empty

    def forward(start, size, cols):
        slot_rows = in_scr[member, pl.ds(start, size)]
        d_out = dout_scr[member, pl.ds(start, size)]
        return (slot_rows, d_out, mat_nn(slot_rows, w_gate_ref[0, :, cols] * jnp.asarray(0.5, BF16)), mat_nn(slot_rows, w_up_ref[0, :, cols]),
                mat_nt(d_out, w_down_ref[0, cols, :]))

    def accumulate(steps):
        ahead = forward(*steps[0])
        for at, (start, _, cols) in enumerate(steps):
            slot_rows, d_out, half_gate, act_up, d_hidden = ahead
            if at + 1 < len(steps):
                ahead = forward(*steps[at + 1])
            hidden, twice_d_act_gate, d_act_up = swiglu_bwd(half_gate, act_up, d_hidden)
            gate_base, up_base = (near_gate_ref, near_up_ref) if start == 0 else (d_w_gate_ref, d_w_up_ref)
            d_w_gate_ref[0, :, cols] = gate_base[0, :, cols] + 0.5 * mat_tn(slot_rows, twice_d_act_gate)
            d_w_up_ref[0, :, cols] = up_base[0, :, cols] + mat_tn(slot_rows, d_act_up)
            d_w_down_ref[0, cols, :] = (near_down_ref if start == 0 else d_w_down_ref)[0, cols, :] + mat_tn(hidden, d_out)

    tiles = [slice(f, f + f_tile) for f in range(0, ff, f_tile)]
    accumulate([(sum(chunks[:c]), size, cols) for c, size in enumerate(chunks) for cols in tiles])

    @pl.when(total_scr[member] > sum(chunks))
    def _():
        for start in range(sum(chunks), far * capacity, tail):
            accumulate([(start, tail, cols) for cols in tiles])


def weight_grads(positions, counts, place, slot_gates, table, w_gate, w_up, w_down, near_grads, capacity):
    group = 4
    near = 4
    tail = 256
    sources, num_tokens = positions.shape[1:]
    width = table.shape[2]
    far = sources - near
    num_experts, _, _ = w_gate.shape
    chunks = (1024, 1024)
    slots = far * capacity + tail

    def per_step(arr):
        return pl.BlockSpec((1,) + arr.shape[1:], lambda step, *_: (step, 0, 0))

    hbm = pl.BlockSpec(memory_space=pl.ANY)
    weights = (w_gate, w_up, w_down)
    return pl.pallas_call(
        functools.partial(weight_grad_kernel, capacity, group, 256, near, chunks, tail),
        grid_spec=pltpu.PrefetchScalarGridSpec(
            num_scalar_prefetch=2, grid=(num_experts,),
            in_specs=[pl.BlockSpec((group, sources, num_tokens), lambda step, *_: (step // group, 0, 0)),
                      pl.BlockSpec((group, far, 128), lambda step, *_: (step // group, 0, 0)),
                      hbm] + [per_step(arr) for arr in weights] * 2,
            out_specs=[per_step(arr) for arr in weights],
            scratch_shapes=[pltpu.VMEM((far, num_tokens, width), BF16), pltpu.VMEM((far, num_tokens, width), BF16),
                            pltpu.VMEM((group, slots, width), BF16), pltpu.VMEM((group, slots, width), BF16),
                            pltpu.SMEM((group,), jnp.int32), pltpu.SemaphoreType.DMA((2, far))]),
        out_shape=[jax.ShapeDtypeStruct(arr.shape, F32) for arr in weights],
        compiler_params=pltpu.CompilerParams(vmem_limit_bytes=67_000_000, dimension_semantics=("arbitrary",)),
        cost_estimate=pl.CostEstimate(flops=280_000_000_000, bytes_accessed=225_000_000, transcendentals=0),
        name="expert_weight_grads",
    )(counts, place, positions, slot_gates, table, w_gate, w_up, w_down, *near_grads)


def rms_parts(x_f32):
    return lax.rsqrt(jnp.mean(x_f32 * x_f32, axis=-1, keepdims=True) + EPS)


def rms_back(x_f32, inv_rms, gain_row, d_out):
    d_gain = jnp.sum(d_out * x_f32 * inv_rms, axis=0, keepdims=True)
    d_scaled = d_out * gain_row
    d_x = inv_rms * d_scaled - x_f32 * inv_rms ** 3 * jnp.mean(d_scaled * x_f32, axis=-1, keepdims=True)
    return d_x, d_gain


def rope_tables(seq_len):
    half_dim = HEAD_DIM // 2
    inv_freq = ROPE_BASE ** (-jnp.arange(half_dim, dtype=F32) / half_dim)
    angles = jnp.arange(seq_len, dtype=F32)[:, None] * inv_freq[None, :]
    cos, sin = jnp.cos(angles), jnp.sin(angles)
    return jnp.concatenate([cos, cos], axis=1), jnp.concatenate([-sin, sin], axis=1)


def causal_probs(query, keys, start):
    scores = mat_nt(query, keys) * HEAD_DIM ** -0.5
    rows = lax.broadcasted_iota(jnp.int32, scores.shape, 0) + start
    scores = jnp.where(rows >= lax.broadcasted_iota(jnp.int32, scores.shape, 1), scores, -1e30)
    weights = jnp.exp(scores - jnp.max(scores, axis=1, keepdims=True))
    return weights / jnp.sum(weights, axis=1, keepdims=True)


def router_probs(rows, w_router_t):
    logits = mat_nt(w_router_t, rows)
    weights = jnp.exp(logits - jnp.max(logits, axis=0, keepdims=True))
    return weights / jnp.sum(weights, axis=0, keepdims=True)


def forward_kernel(num_seqs, x_ref, dy_ref, idx_ref, gains_ref, w_qkv_ref, w_out_ref, w_router_t_ref, cos_ref, sin_ref,
                   payload_ref, gates_ref, qkv_ref, context_ref, h_ref, x_scr, w_qkv_scr, w_out_scr, load_sem):
    num_tokens, width = x_ref.shape
    seq_len = num_tokens // num_seqs
    block = 256
    loads = [pltpu.make_async_copy(src, dst, load_sem.at[i]) for i, (src, dst) in enumerate([
        (x_ref, x_scr), (w_qkv_ref, w_qkv_scr), (w_out_ref, w_out_scr), (dy_ref, payload_ref.at[pl.ds(num_tokens, num_tokens)])])]
    for copy in loads:
        copy.start()
    loads[0].wait()
    x_ref = x_scr
    x_f32 = x_ref[...].astype(F32)
    normed1 = (x_f32 * rms_parts(x_f32) * gains_ref[0:1].astype(F32)).astype(BF16)
    loads[1].wait()
    for head_col in range(0, 3 * width, HEAD_DIM):
        vals = mat_nn(normed1, w_qkv_scr[:, head_col:head_col + HEAD_DIM])
        for seq in range(num_seqs):
            span = slice(seq * seq_len, (seq + 1) * seq_len)
            part = vals[span]
            if head_col < 2 * width:
                part = part * cos_ref[...] + pltpu.roll(part, HEAD_DIM // 2, 1) * sin_ref[...]
            qkv_ref[span, head_col:head_col + HEAD_DIM] = part.astype(BF16)
    for seq in range(num_seqs):
        for head in range(width // HEAD_DIM):
            cols = [slice(part * width + head * HEAD_DIM, part * width + (head + 1) * HEAD_DIM) for part in range(3)]
            for start in range(0, seq_len, block):
                rows = slice(seq * seq_len + start, seq * seq_len + start + block)
                seen = slice(seq * seq_len, seq * seq_len + start + block)
                probs = causal_probs(qkv_ref[rows, cols[0]], qkv_ref[seen, cols[1]], start).astype(BF16)
                context_ref[rows, cols[0]] = mat_nn(probs, qkv_ref[seen, cols[2]]).astype(BF16)
    loads[2].wait()
    h_rows = (x_f32 + mat_nn(context_ref[...], w_out_scr[...])).astype(BF16)
    h_ref[...] = h_rows
    h_f32 = h_rows.astype(F32)
    normed2 = (h_f32 * rms_parts(h_f32) * gains_ref[1:2].astype(F32)).astype(BF16)
    payload_ref[0:num_tokens] = normed2
    probs = router_probs(normed2, w_router_t_ref[...])
    expert_iota = lax.broadcasted_iota(jnp.int32, probs.shape, 0)
    picked = [jnp.sum(jnp.where(expert_iota == idx_ref[choice:choice + 1], probs, 0.0), axis=0, keepdims=True) for choice in range(idx_ref.shape[0])]
    total = functools.reduce(lambda a, b: a + b, picked)
    for choice, part in enumerate(picked):
        gates_ref[choice:choice + 1] = part / total
    loads[3].wait()


def dense_forward(x_rows, dy_rows, idx_cols, num_seqs, gains, w_qkv, w_attn_out, w_router_t, tables):
    num_tokens, width = x_rows.shape
    rows = jax.ShapeDtypeStruct(x_rows.shape, BF16)
    hbm, vmem = pl.BlockSpec(memory_space=pl.ANY), pl.BlockSpec(memory_space=pltpu.VMEM)
    return pl.pallas_call(
        functools.partial(forward_kernel, num_seqs),
        in_specs=[hbm, hbm, vmem, vmem, hbm, hbm, vmem, vmem, vmem],
        scratch_shapes=[pltpu.VMEM(x_rows.shape, BF16), pltpu.VMEM(w_qkv.shape, BF16), pltpu.VMEM(w_attn_out.shape, BF16), pltpu.SemaphoreType.DMA((4,))],
        out_shape=[jax.ShapeDtypeStruct((2 * num_tokens, width), BF16), jax.ShapeDtypeStruct(idx_cols.shape, F32),
                   jax.ShapeDtypeStruct((num_tokens, 3 * width), BF16), rows, rows],
        compiler_params=pltpu.CompilerParams(vmem_limit_bytes=66_000_000),
        cost_estimate=pl.CostEstimate(flops=10_000_000_000, bytes_accessed=8_000_000, transcendentals=0),
        name="dense_forward",
    )(x_rows, dy_rows, idx_cols, gains, w_qkv, w_attn_out, w_router_t, *tables)


def backward_kernel(num_seqs, x_ref, dy_ref, d_rows_ref, d_gates_ref, idx_ref, payload_ref, qkv_ref, context_ref, h_ref,
                    gains_ref, w_qkv_ref, w_out_ref, w_router_t_ref, cos_ref, sin_ref, d_x_ref, d_w_qkv_ref, d_w_out_ref, packed_ref, d_qkv_scr):
    num_tokens, width = x_ref.shape
    seq_len = num_tokens // num_seqs
    num_experts = w_router_t_ref.shape[0]
    block = 256
    normed2 = payload_ref[0:num_tokens]
    probs = router_probs(normed2, w_router_t_ref[...])
    expert_iota = lax.broadcasted_iota(jnp.int32, probs.shape, 0)
    chosen = jnp.zeros(probs.shape, F32)
    d_gate = jnp.zeros(probs.shape, F32)
    for choice in range(idx_ref.shape[0]):
        hit = expert_iota == idx_ref[choice:choice + 1]
        chosen = jnp.where(hit, probs, chosen)
        d_gate = jnp.where(hit, d_gates_ref[choice:choice + 1], d_gate)
    total = jnp.sum(chosen, axis=0, keepdims=True)
    mixed = jnp.sum(d_gate * chosen, axis=0, keepdims=True) / total
    d_weighted = chosen * ((d_gate - mixed) / total)
    d_logits = (d_weighted - probs * jnp.sum(d_weighted, axis=0, keepdims=True)).astype(BF16)
    packed_ref[0:width] = mat_nn(d_logits, normed2).T
    d_normed2 = d_rows_ref[...] + mat_tn(d_logits, w_router_t_ref[...])
    h_f32 = h_ref[...].astype(F32)
    d_h_part, d_gain2 = rms_back(h_f32, rms_parts(h_f32), gains_ref[1:2].astype(F32), d_normed2)
    d_h = (dy_ref[...].astype(F32) + d_h_part).astype(BF16)
    d_w_out_ref[...] = mat_tn(context_ref[...], d_h)
    d_context = mat_nt(d_h, w_out_ref[...]).astype(BF16)
    for seq in range(num_seqs):
        whole = slice(seq * seq_len, (seq + 1) * seq_len)
        for head in range(width // HEAD_DIM):
            cols = [slice(part * width + head * HEAD_DIM, part * width + (head + 1) * HEAD_DIM) for part in range(3)]
            d_key = jnp.zeros((seq_len, HEAD_DIM), F32)
            d_value = jnp.zeros((seq_len, HEAD_DIM), F32)
            for start in reversed(range(0, seq_len, block)):
                rows = slice(seq * seq_len + start, seq * seq_len + start + block)
                seen = slice(seq * seq_len, seq * seq_len + start + block)
                query, keys = qkv_ref[rows, cols[0]], qkv_ref[seen, cols[1]]
                weights = causal_probs(query, keys, start)
                d_out = d_context[rows, cols[0]]
                d_weights = mat_nt(d_out, qkv_ref[seen, cols[2]]).astype(BF16).astype(F32)
                d_scores = (weights * (d_weights - jnp.sum(weights * d_weights, axis=1, keepdims=True)) * HEAD_DIM ** -0.5).astype(BF16)
                d_query = mat_nn(d_scores, keys).astype(BF16).astype(F32)
                at = slice(start, start + block)
                d_query = d_query * cos_ref[at] - pltpu.roll(d_query, HEAD_DIM // 2, 1) * sin_ref[at]
                d_qkv_scr[rows, cols[0]] = d_query.astype(BF16)
                key_part, value_part = mat_tn(d_scores, query), mat_tn(weights.astype(BF16), d_out)
                if start + block == seq_len:
                    d_key, d_value = key_part, value_part
                else:
                    d_key = jnp.concatenate([d_key[:start + block] + key_part, d_key[start + block:]], axis=0)
                    d_value = jnp.concatenate([d_value[:start + block] + value_part, d_value[start + block:]], axis=0)
            d_key = d_key.astype(BF16).astype(F32)
            d_key = d_key * cos_ref[...] - pltpu.roll(d_key, HEAD_DIM // 2, 1) * sin_ref[...]
            d_qkv_scr[whole, cols[1]] = d_key.astype(BF16)
            d_qkv_scr[whole, cols[2]] = d_value.astype(BF16)
    d_qkv = d_qkv_scr[...]
    x_f32 = x_ref[...].astype(F32)
    inv_rms = rms_parts(x_f32)
    gain1 = gains_ref[0:1].astype(F32)
    d_w_qkv_ref[...] = mat_tn((x_f32 * inv_rms * gain1).astype(BF16), d_qkv)
    d_x_part, d_gain1 = rms_back(x_f32, inv_rms, gain1, mat_nt(d_qkv, w_qkv_ref[...]))
    d_x_ref[...] = (d_h.astype(F32) + d_x_part).astype(BF16)
    packed_ref[width:] = jnp.zeros((packed_ref.shape[0] - width, num_experts), F32)
    for row, d_gain in enumerate((d_gain1, d_gain2)):
        for part in range(width // num_experts):
            at = width + row * (width // num_experts) + part
            packed_ref[at:at + 1] = d_gain[:, part * num_experts:(part + 1) * num_experts]


def dense_backward(x_rows, dy_rows, d_rows, d_gates, idx_cols, saved, num_seqs, gains, w_qkv, w_attn_out, w_router_t, tables):
    width = x_rows.shape[1]
    num_experts = w_router_t.shape[0]
    return pl.pallas_call(
        functools.partial(backward_kernel, num_seqs),
        out_shape=[jax.ShapeDtypeStruct(x_rows.shape, BF16), jax.ShapeDtypeStruct(w_qkv.shape, F32),
                   jax.ShapeDtypeStruct(w_attn_out.shape, F32), jax.ShapeDtypeStruct((width + 8 * pl.cdiv(2 * width, 8 * num_experts), num_experts), F32)],
        scratch_shapes=[pltpu.VMEM((x_rows.shape[0], 3 * width), BF16)],
        compiler_params=pltpu.CompilerParams(vmem_limit_bytes=48_000_000),
        cost_estimate=pl.CostEstimate(flops=15_000_000_000, bytes_accessed=12_000_000, transcendentals=0),
        name="dense_backward",
    )(x_rows, dy_rows, d_rows, d_gates, idx_cols, *saved, gains, w_qkv, w_attn_out, w_router_t, *tables)


def solution(mesh):
    ep_size = mesh.shape['ep']
    tok_spec = P(('dp', 'ep'), None, None)
    rep_spec = P()
    exp_spec = P('ep', None, None)

    def local_step(x_tokens, dy_tokens, route_idx, norm1_gain, norm2_gain, w_qkv, w_attn_out, w_router, w_gate, w_up, w_down):
        num_seqs, seq_len, model_width = x_tokens.shape
        num_tokens = num_seqs * seq_len
        top_k = route_idx.shape[-1]
        local_experts = w_gate.shape[0]
        num_experts = local_experts * ep_size
        capacity = capacity_rows(num_tokens, top_k, num_experts)
        x_rows = x_tokens.reshape(num_tokens, model_width)
        dy_rows = dy_tokens.reshape(num_tokens, model_width)
        idx_cols = route_idx.reshape(num_tokens, top_k).T
        routes = idx_cols.astype(BF16).reshape(-1, model_width)
        near_part = jnp.concatenate([dy_rows, routes], axis=0)
        from_core, from_chip = [lax.ppermute(near_part, 'ep', [(i, i ^ k) for i in range(ep_size)]) for k in (1, 2)]
        from_far = lax.ppermute(from_chip, 'ep', [(i, i ^ 1) for i in range(ep_size)])
        dy_near = jnp.stack([near_part, from_core, from_chip, from_far])

        def expert_of(gathered):
            return gathered.reshape(-1, top_k, num_tokens).astype(jnp.int32) - lax.axis_index('ep') * local_experts

        idx_near = expert_of(dy_near[:, num_tokens:])
        positions_near = slot_positions(idx_near, local_experts, capacity)
        tables = rope_tables(seq_len)
        w_router_t = w_router.T
        dense_weights = (num_seqs, jnp.stack([norm1_gain, norm2_gain]), w_qkv, w_attn_out, w_router_t, tables)
        payload, gate_vals, qkv_rows, context, h_rows = dense_forward(x_rows, dy_rows, idx_cols, *dense_weights)
        table = lax.all_gather(payload, ('dp', 'ep'))
        rows_near, gates_near = near_gather(payload, gate_vals, num_tokens)
        d_near, d_gate_near, slot_gates, *near_grads = token_grads(positions_near, idx_near, gates_near, rows_near, dy_near, w_gate, w_up, w_down, capacity)
        d_rows, d_gates, slot_gates_all, routes_all = near_return(d_near, d_gate_near, slot_gates, dy_near[:, num_tokens:], mesh.shape['dp'])
        slot_gates_all = slot_gates_all.transpose(1, 0, 2, 3).reshape(local_experts, -1, 128)
        d_x, *dense_grads = dense_backward(x_rows, dy_rows, d_rows, d_gates, idx_cols, (payload, qkv_rows, context, h_rows), *dense_weights)
        dense_grads, slot_gates_all = lax.optimization_barrier((dense_grads, slot_gates_all))
        positions = all_positions(expert_of(routes_all).transpose(1, 0, 2), local_experts, capacity)
        counts = (jnp.max(positions, axis=2) + 16) // 16 * 16
        place = jnp.stack([lax.axis_index('dp'), lax.axis_index('ep')]).astype(jnp.int32)
        expert_grads = weight_grads(positions, counts, place, slot_gates_all, table, w_gate, w_up, w_down, near_grads, capacity)
        d_w_qkv, d_w_out, packed = lax.psum(tuple(dense_grads), ('dp', 'ep'))
        gain_rows = packed[model_width:model_width + 2 * model_width // num_experts].reshape(2, model_width)
        dense_out = (gain_rows[0], gain_rows[1], d_w_qkv, d_w_out, packed[:model_width])
        return (d_x.reshape(x_tokens.shape),) + dense_out + tuple(expert_grads)

    return jax.shard_map(local_step, mesh=mesh,
                          in_specs=(tok_spec, tok_spec, tok_spec, rep_spec, rep_spec, rep_spec, rep_spec, rep_spec, exp_spec, exp_spec, exp_spec),
                          out_specs=(tok_spec, rep_spec, rep_spec, rep_spec, rep_spec, rep_spec, exp_spec, exp_spec, exp_spec),
                          check_vma=False)
```

```python
import functools

import jax
import jax.numpy as jnp
from jax import lax
from jax.experimental import pallas as pl
from jax.experimental.pallas import tpu as pltpu
from jax.sharding import PartitionSpec as P


F32 = jnp.float32
BF16 = jnp.bfloat16
EPS = 1e-6
HEAD_DIM = 128
ROPE_BASE = 10000.0


def capacity_rows(num_tokens, top_k, num_experts):
    return 8 * ((5 * num_tokens * top_k + 32 * num_experts - 1) // (32 * num_experts))


def slot_positions(local_idx, local_experts, capacity):
    num_tokens = local_idx.shape[-1]
    expert_ids = jnp.arange(local_experts, dtype=jnp.int32)
    member = jnp.any(local_idx[None] == expert_ids[:, None, None, None], axis=2)
    before = (jnp.arange(num_tokens)[:, None] < jnp.arange(num_tokens)[None, :]).astype(BF16)
    earlier = jnp.einsum('est,tv->esv', member.astype(BF16), before, preferred_element_type=F32)
    return jnp.where(member & (earlier < capacity), earlier.astype(jnp.int32), -1)


def mat_nn(left, right):
    return lax.dot_general(left, right, (((1,), (0,)), ((), ())), preferred_element_type=F32)


def mat_nt(left, right):
    return lax.dot_general(left, right, (((1,), (1,)), ((), ())), preferred_element_type=F32)


def mat_tn(left, right):
    return lax.dot_general(left, right, (((0,), (0,)), ((), ())), preferred_element_type=F32)


def swiglu_bwd(half_gate, act_up, d_hidden):
    twice_sig = 1.0 + jnp.tanh(half_gate)
    silu = half_gate * twice_sig
    hidden = (silu * act_up).astype(BF16)
    d_act_up = (d_hidden * silu).astype(BF16)
    twice_d_act_gate = (d_hidden * act_up * (twice_sig + silu * (2.0 - twice_sig))).astype(BF16)
    return hidden, twice_d_act_gate, d_act_up


def token_grad_kernel(capacity, group, f_tile, pos_ref, idx_ref, gate_ref, rows_ref, dy_ref, w_gate_ref, w_up_ref, w_down_ref,
                      d_rows_ref, d_gates_ref, slot_gate_ref, d_w_gate_ref, d_w_up_ref, d_w_down_ref,
                      select_scr, in_scr, raw_scr, dout_scr, din_scr):
    sources, num_tokens, _ = rows_ref.shape
    ff = w_gate_ref.shape[2]
    first = pl.program_id(0) * group
    slot_iota = lax.broadcasted_iota(jnp.int32, (capacity, num_tokens), 0)
    diagonal = lax.broadcasted_iota(jnp.int32, (capacity, 128), 0) == lax.broadcasted_iota(jnp.int32, (capacity, 128), 1)

    @pl.when(pl.program_id(0) == 0)
    def _():
        d_rows_ref[...] = jnp.zeros_like(d_rows_ref)
        d_gates_ref[...] = jnp.zeros_like(d_gates_ref)

    def select(source):
        selectors, gate_cols = [], []
        for member in range(group):
            hit = slot_iota == pos_ref[member, source:source + 1, :]
            gate_row = jnp.sum(jnp.where(idx_ref[source] == first + member, gate_ref[source], 0.0), axis=0, keepdims=True)
            gate_col = jnp.sum(jnp.where(hit, gate_row, 0.0), axis=1, keepdims=True)
            slot_gate_ref[member, source:source + 1, :] = jnp.sum(jnp.where(diagonal, gate_col, 0.0), axis=0, keepdims=True)
            gate_cols.append(gate_col)
            selectors.append(jnp.where(hit, 1.0, 0.0).astype(BF16))
        return jnp.concatenate(selectors, axis=0), jnp.concatenate(gate_cols, axis=0)

    ahead = select(0)
    for source in range(sources):
        selector, gate_col = ahead
        if source + 1 < sources:
            ahead = select(source + 1)
        select_scr[source] = selector
        slot_rows = mat_nn(selector, rows_ref[source]).astype(BF16)
        raw_dy = mat_nn(selector, dy_ref[source, :num_tokens])
        scaled_dy = (raw_dy * gate_col).astype(BF16)
        raw_dy = raw_dy.astype(BF16)
        for member in range(group):
            span = slice(source * capacity, (source + 1) * capacity)
            part = slice(member * capacity, (member + 1) * capacity)
            in_scr[member, span] = slot_rows[part]
            raw_scr[member, span] = raw_dy[part]
            dout_scr[member, span] = scaled_dy[part]

    def forward(member, cols):
        slot_rows = in_scr[member]
        half_w_gate = w_gate_ref[member, :, cols] * jnp.asarray(0.5, BF16)
        return (half_w_gate, mat_nn(slot_rows, half_w_gate), mat_nn(slot_rows, w_up_ref[member, :, cols]),
                mat_nt(dout_scr[member], w_down_ref[member, cols, :]))

    steps = [(member, slice(f, f + f_tile)) for member in range(group) for f in range(0, ff, f_tile)]
    ahead = forward(*steps[0])
    for at, (member, cols) in enumerate(steps):
        half_w_gate, half_gate, act_up, d_hidden = ahead
        if at + 1 < len(steps):
            ahead = forward(*steps[at + 1])
        hidden, twice_d_act_gate, d_act_up = swiglu_bwd(half_gate, act_up, d_hidden)
        out_part = mat_nn(hidden, w_down_ref[member, cols, :])
        in_part = mat_nt(twice_d_act_gate, half_w_gate) + mat_nt(d_act_up, w_up_ref[member, :, cols])
        d_w_gate_ref[member, :, cols] = 0.5 * mat_tn(in_scr[member], twice_d_act_gate)
        d_w_up_ref[member, :, cols] = mat_tn(in_scr[member], d_act_up)
        d_w_down_ref[member, cols, :] = mat_tn(hidden, dout_scr[member])
        out_sum, in_sum = (out_part, in_part) if cols.start == 0 else (out_sum + out_part, in_sum + in_part)
        if cols.stop == ff:
            d_gate = jnp.sum(raw_scr[member].astype(F32) * out_sum.astype(BF16).astype(F32), axis=1, keepdims=True)
            d_in = in_sum.astype(BF16)
            for source in range(sources):
                part = slice(source * capacity, (source + 1) * capacity)
                din_scr[source, member * capacity:(member + 1) * capacity] = d_in[part]
                hit = slot_iota == pos_ref[member, source:source + 1, :]
                d_gate_row = jnp.sum(jnp.where(hit, d_gate[part], 0.0), axis=0, keepdims=True)
                d_gates_ref[source] += jnp.where(idx_ref[source] == first + member, d_gate_row, 0.0)

    for source in range(sources):
        d_rows_ref[source] += mat_tn(select_scr[source], din_scr[source])


def token_grads(positions, local_idx, gates, rows, dy_rows, w_gate, w_up, w_down, capacity):
    group = 4
    sources, num_tokens, width = rows.shape
    num_experts = w_gate.shape[0]
    slots = sources * capacity

    def whole(arr):
        return pl.BlockSpec(arr.shape, lambda step: (0,) * arr.ndim, pipeline_mode=pl.Buffered(1))

    def per_step(arr):
        return pl.BlockSpec((group,) + arr.shape[1:], lambda step: (step, 0, 0))

    slot_gates = jax.ShapeDtypeStruct((num_experts, sources, 128), F32)
    weights = [jax.ShapeDtypeStruct(arr.shape, F32) for arr in (w_gate, w_up, w_down)]
    return pl.pallas_call(
        functools.partial(token_grad_kernel, capacity, group, 256),
        grid=(num_experts // group,),
        in_specs=[per_step(positions), whole(local_idx), whole(gates), whole(rows), whole(dy_rows),
                  per_step(w_gate), per_step(w_up), per_step(w_down)],
        out_specs=[pl.BlockSpec(rows.shape, lambda step: (0, 0, 0)), pl.BlockSpec(gates.shape, lambda step: (0, 0, 0)),
                   per_step(slot_gates)] + [per_step(arr) for arr in weights],
        out_shape=[jax.ShapeDtypeStruct(rows.shape, F32), jax.ShapeDtypeStruct(gates.shape, F32), slot_gates] + weights,
        scratch_shapes=[pltpu.VMEM((sources, group * capacity, num_tokens), BF16),
                        pltpu.VMEM((group, slots, width), BF16), pltpu.VMEM((group, slots, width), BF16),
                        pltpu.VMEM((group, slots, width), BF16), pltpu.VMEM((sources, group * capacity, width), BF16)],
        compiler_params=pltpu.CompilerParams(vmem_limit_bytes=64_000_000, dimension_semantics=("arbitrary",)),
        cost_estimate=pl.CostEstimate(flops=60_000_000_000, bytes_accessed=130_000_000, transcendentals=0),
        name="expert_token_grads",
    )(positions, local_idx, gates, rows, dy_rows, w_gate, w_up, w_down)


def near_peers():
    ep = lax.axis_index('ep')
    return {'ep': ep + 1 - 2 * lax.rem(ep, 2)}, {'ep': lax.rem(ep + 2, 4)}


def meet(peers):
    barrier = pltpu.get_barrier_semaphore()
    for peer in peers:
        pl.semaphore_signal(barrier, inc=1, device_id=peer, device_id_type=pl.DeviceIdType.MESH)
    pl.semaphore_wait(barrier, len(peers))


def remote(src, dst, send_sem, recv_sem, peer):
    return pltpu.make_async_remote_copy(src_ref=src, dst_ref=dst, send_sem=send_sem, recv_sem=recv_sem,
                                        device_id=peer, device_id_type=pl.DeviceIdType.MESH)


def near_gather_kernel(rows_ref, gates_ref, rows_out, gates_out, send_sem, recv_sem):
    core_peer, chip_peer = near_peers()
    meet((core_peer, chip_peer))
    num_tokens = rows_out.shape[1]
    half = num_tokens // 2
    pieces = [(rows_ref.at[pl.ds(0, half)], lambda slot: rows_out.at[slot, pl.ds(0, half)]),
              (rows_ref.at[pl.ds(half, half)], lambda slot: rows_out.at[slot, pl.ds(half, half)]),
              (gates_ref, lambda slot: gates_out.at[slot])]
    across = [remote(src, place(2), send_sem.at[0, i], recv_sem.at[0, i], chip_peer) for i, (src, place) in enumerate(pieces)]
    beside = [remote(src, place(1), send_sem.at[1, i], recv_sem.at[1, i], core_peer) for i, (src, place) in enumerate(pieces)]
    onward = [remote(place(2), place(3), send_sem.at[2, i], recv_sem.at[2, i], core_peer) for i, (_, place) in enumerate(pieces)]
    for copy in across + beside:
        copy.start()
    rows_out[0] = rows_ref[0:num_tokens]
    gates_out[0] = gates_ref[...]
    for copy, forward in zip(across, onward):
        copy.wait_recv()
        forward.start()
    for copy in beside + onward:
        copy.wait()
    for copy in across:
        copy.wait_send()


def near_gather(rows, gates, num_tokens):
    vmem = pl.BlockSpec(memory_space=pltpu.VMEM)
    return pl.pallas_call(
        near_gather_kernel,
        in_specs=[vmem, vmem], out_specs=[vmem, vmem],
        out_shape=[jax.ShapeDtypeStruct((4, num_tokens, rows.shape[1]), rows.dtype), jax.ShapeDtypeStruct((4,) + gates.shape, gates.dtype)],
        scratch_shapes=[pltpu.SemaphoreType.DMA((3, 3)), pltpu.SemaphoreType.DMA((3, 3))],
        compiler_params=pltpu.CompilerParams(collective_id=0, has_side_effects=True),
        cost_estimate=pl.CostEstimate(flops=10_000_000_000, bytes_accessed=10_000_000, transcendentals=0),
        name="near_gather",
    )(rows, gates)


def near_return_kernel(d_rows_ref, d_gates_ref, slot_gates_ref, routes_ref, rows_out, gates_out, slot_gates_out, routes_out,
                       own_rows, pass_rows, sum_rows, last_rows, own_gates, pass_gates, sum_gates, last_gates,
                       send_sem, recv_sem, far_send_sem, far_recv_sem):
    core_peer, chip_peer = near_peers()
    dp = lax.axis_index('dp')
    dp_size = slot_gates_out.shape[0] + 1
    far_peers = [{'dp': lax.rem(dp + k, dp_size)} for k in range(1, dp_size)]
    meet([core_peer, chip_peer] + far_peers)
    half = d_rows_ref.shape[1] // 2
    halves = [pl.ds(0, half), pl.ds(half, half)]
    far = [remote(slot_gates_ref, slot_gates_out.at[dp_size - 2 - k], far_send_sem.at[0, k], far_recv_sem.at[0, k], peer) for k, peer in enumerate(far_peers)]
    far += [remote(routes_ref, routes_out.at[dp_size - 1 - k], far_send_sem.at[1, k], far_recv_sem.at[1, k], peer) for k, peer in enumerate(far_peers)]
    first = [remote(d_rows_ref.at[3, span], pass_rows.at[span], send_sem.at[i], recv_sem.at[i], core_peer) for i, span in enumerate(halves)]
    first.append(remote(d_gates_ref.at[3], pass_gates, send_sem.at[2], recv_sem.at[2], core_peer))
    second = [remote(d_rows_ref.at[1], own_rows, send_sem.at[3], recv_sem.at[3], core_peer),
              remote(d_gates_ref.at[1], own_gates, send_sem.at[4], recv_sem.at[4], core_peer)]
    third = [remote(sum_rows.at[span], last_rows.at[span], send_sem.at[5 + i], recv_sem.at[5 + i], chip_peer) for i, span in enumerate(halves)]
    third.append(remote(sum_gates, last_gates, send_sem.at[7], recv_sem.at[7], chip_peer))
    for copy in first + second + far:
        copy.start()
    first[0].wait_recv()
    sum_rows[halves[0]] = d_rows_ref[2, halves[0]] + pass_rows[halves[0]]
    first[1].wait_recv()
    first[2].wait_recv()
    sum_gates[...] = d_gates_ref[2] + pass_gates[...]
    third[0].start()
    sum_rows[halves[1]] = d_rows_ref[2, halves[1]] + pass_rows[halves[1]]
    for copy in second:
        copy.wait_recv()
    rows_out[...] = d_rows_ref[0] + own_rows[...]
    gates_out[...] = d_gates_ref[0] + own_gates[...]
    third[1].start()
    third[2].start()
    routes_out[0] = routes_ref[...]
    for copy in third:
        copy.wait_recv()
    rows_out[...] += last_rows[...]
    gates_out[...] += last_gates[...]
    for copy in far:
        copy.wait()
    for copy in first + second + third:
        copy.wait_send()


def near_return(d_rows, d_gates, slot_gates, routes, dp_size):
    vmem = pl.BlockSpec(memory_space=pltpu.VMEM)
    rows = jax.ShapeDtypeStruct(d_rows.shape[1:], F32)
    gates = jax.ShapeDtypeStruct(d_gates.shape[1:], F32)
    return pl.pallas_call(
        near_return_kernel,
        in_specs=[vmem] * 4, out_specs=[vmem] * 4,
        out_shape=[rows, gates, jax.ShapeDtypeStruct((dp_size - 1,) + slot_gates.shape, F32), jax.ShapeDtypeStruct((dp_size,) + routes.shape, BF16)],
        scratch_shapes=[pltpu.VMEM(rows.shape, F32)] * 4 + [pltpu.VMEM(gates.shape, F32)] * 4
        + [pltpu.SemaphoreType.DMA((8,)), pltpu.SemaphoreType.DMA((8,)), pltpu.SemaphoreType.DMA((2, dp_size - 1)), pltpu.SemaphoreType.DMA((2, dp_size - 1))],
        compiler_params=pltpu.CompilerParams(collective_id=1, has_side_effects=True, vmem_limit_bytes=40_000_000),
        cost_estimate=pl.CostEstimate(flops=15_000_000_000, bytes_accessed=20_000_000, transcendentals=0),
        name="near_return",
    )(d_rows, d_gates, slot_gates, routes)


def position_kernel(capacity, num_experts, idx_ref, pos_ref, member_scr):
    choices, sources, num_tokens = idx_ref.shape
    block = 256

    @pl.loop(0, num_experts)
    def _(expert):
        hit = idx_ref[0] == expert
        for choice in range(1, choices):
            hit = hit | (idx_ref[choice] == expert)
        member_scr[pl.ds(expert * sources, sources)] = jnp.where(hit, 1.0, 0.0).astype(BF16)

    before = jnp.where(lax.broadcasted_iota(jnp.int32, (num_tokens, num_tokens), 0) < lax.broadcasted_iota(jnp.int32, (num_tokens, num_tokens), 1), 1.0, 0.0).astype(BF16)

    @pl.loop(0, num_experts * sources // block)
    def _(step):
        span = pl.ds(pl.multiple_of(step * block, block), block)
        member = member_scr[span]
        earlier = mat_nn(member, before)
        pos_ref[span] = jnp.where((member.astype(F32) > 0.5) & (earlier < capacity), earlier, -1.0).astype(jnp.int32)


def all_positions(idx_by_choice, num_experts, capacity):
    _, sources, num_tokens = idx_by_choice.shape
    flat = pl.pallas_call(
        functools.partial(position_kernel, capacity, num_experts),
        out_shape=jax.ShapeDtypeStruct((num_experts * sources, num_tokens), jnp.int32),
        scratch_shapes=[pltpu.VMEM((num_experts * sources, num_tokens), BF16)],
        compiler_params=pltpu.CompilerParams(vmem_limit_bytes=32_000_000),
        cost_estimate=pl.CostEstimate(flops=4_000_000_000, bytes_accessed=5_000_000, transcendentals=0),
        name="slot_positions",
    )(idx_by_choice)
    return flat.reshape(num_experts, sources, num_tokens)


def weight_grad_kernel(capacity, group, f_tile, near, chunks, tail, count_ref, place_ref, pos_ref, slot_gate_ref, table_hbm,
                       w_gate_ref, w_up_ref, w_down_ref, near_gate_ref, near_up_ref, near_down_ref,
                       d_w_gate_ref, d_w_up_ref, d_w_down_ref, rows_scr, dy_scr, in_scr, dout_scr, total_scr, load_sem):
    expert = pl.program_id(0)
    member = lax.rem(expert, group)
    far, num_tokens, _ = rows_scr.shape
    sources = far + near
    ff = w_gate_ref.shape[2]
    slot_iota = lax.broadcasted_iota(jnp.int32, (capacity, num_tokens), 0)
    diagonal = lax.broadcasted_iota(jnp.int32, (capacity, 128), 0) == lax.broadcasted_iota(jnp.int32, (capacity, 128), 1)

    def source_of(index):
        return lax.rem(place_ref[0] * near + near + index - lax.rem(index, near), sources) + jnp.bitwise_xor(lax.rem(index, near), place_ref[1])

    def loads(index):
        source = source_of(index)
        return (pltpu.make_async_copy(table_hbm.at[source, pl.ds(0, num_tokens)], rows_scr.at[index], load_sem.at[0, index]),
                pltpu.make_async_copy(table_hbm.at[source, pl.ds(num_tokens, num_tokens)], dy_scr.at[index], load_sem.at[1, index]))

    @pl.when(expert == 0)
    def _():
        @pl.loop(0, far)
        def _(index):
            for copy in loads(index):
                copy.start()

    def select(index):
        selectors, gate_cols = [], []
        for k in range(group):
            selectors.append(jnp.where(slot_iota == pos_ref[k, pl.ds(index + near, 1), :], 1.0, 0.0).astype(BF16))
            gate_cols.append(jnp.sum(jnp.where(diagonal, slot_gate_ref[k, pl.ds(index, 1), :], 0.0), axis=1, keepdims=True))
        return jnp.concatenate(selectors, axis=0), jnp.concatenate(gate_cols, axis=0)

    @pl.when(member == 0)
    def _():
        unroll = 7

        def body(step, starts):
            @pl.when(expert == 0)
            def _():
                for j in range(unroll):
                    for copy in loads(step * unroll + j):
                        copy.wait()

            ahead = select(step * unroll)
            for j in range(unroll):
                index = step * unroll + j
                selector, gate_col = ahead
                if j + 1 < unroll:
                    ahead = select(index + 1)
                slot_rows = mat_nn(selector, rows_scr[index]).astype(BF16)
                scaled_dy = (mat_nn(selector, dy_scr[index]) * gate_col).astype(BF16)
                for k in range(group):
                    span = pl.ds(pl.multiple_of(starts[k], 16), capacity)
                    part = slice(k * capacity, (k + 1) * capacity)
                    in_scr[k, span] = slot_rows[part]
                    dout_scr[k, span] = scaled_dy[part]
                starts = tuple(starts[k] + count_ref[expert + k, index + near] for k in range(group))
            return starts

        ends = lax.fori_loop(0, far // unroll, body, (jnp.int32(0),) * group)
        empty = jnp.zeros((tail, in_scr.shape[2]), BF16)
        for k in range(group):
            total_scr[k] = ends[k]
            span = pl.ds(pl.multiple_of(ends[k], 16), tail)
            in_scr[k, span] = empty
            dout_scr[k, span] = empty

            @pl.loop((ends[k] + tail - 1) // tail, sum(chunks) // tail)
            def _(block):
                span = pl.ds(pl.multiple_of(block * tail, tail), tail)
                in_scr[k, span] = empty
                dout_scr[k, span] = empty

    def forward(start, size, cols):
        slot_rows = in_scr[member, pl.ds(start, size)]
        d_out = dout_scr[member, pl.ds(start, size)]
        return (slot_rows, d_out, mat_nn(slot_rows, w_gate_ref[0, :, cols] * jnp.asarray(0.5, BF16)), mat_nn(slot_rows, w_up_ref[0, :, cols]),
                mat_nt(d_out, w_down_ref[0, cols, :]))

    def accumulate(steps):
        ahead = forward(*steps[0])
        for at, (start, _, cols) in enumerate(steps):
            slot_rows, d_out, half_gate, act_up, d_hidden = ahead
            if at + 1 < len(steps):
                ahead = forward(*steps[at + 1])
            hidden, twice_d_act_gate, d_act_up = swiglu_bwd(half_gate, act_up, d_hidden)
            gate_base, up_base = (near_gate_ref, near_up_ref) if start == 0 else (d_w_gate_ref, d_w_up_ref)
            d_w_gate_ref[0, :, cols] = gate_base[0, :, cols] + 0.5 * mat_tn(slot_rows, twice_d_act_gate)
            d_w_up_ref[0, :, cols] = up_base[0, :, cols] + mat_tn(slot_rows, d_act_up)
            d_w_down_ref[0, cols, :] = (near_down_ref if start == 0 else d_w_down_ref)[0, cols, :] + mat_tn(hidden, d_out)

    tiles = [slice(f, f + f_tile) for f in range(0, ff, f_tile)]
    accumulate([(sum(chunks[:c]), size, cols) for c, size in enumerate(chunks) for cols in tiles])

    @pl.when(total_scr[member] > sum(chunks))
    def _():
        for start in range(sum(chunks), far * capacity, tail):
            accumulate([(start, tail, cols) for cols in tiles])


def weight_grads(positions, counts, place, slot_gates, table, w_gate, w_up, w_down, near_grads, capacity):
    group = 4
    near = 4
    tail = 256
    sources, num_tokens = positions.shape[1:]
    width = table.shape[2]
    far = sources - near
    num_experts, _, _ = w_gate.shape
    chunks = (1024, 1024)
    slots = far * capacity + tail

    def per_step(arr):
        return pl.BlockSpec((1,) + arr.shape[1:], lambda step, *_: (step, 0, 0))

    hbm = pl.BlockSpec(memory_space=pl.ANY)
    weights = (w_gate, w_up, w_down)
    return pl.pallas_call(
        functools.partial(weight_grad_kernel, capacity, group, 256, near, chunks, tail),
        grid_spec=pltpu.PrefetchScalarGridSpec(
            num_scalar_prefetch=2, grid=(num_experts,),
            in_specs=[pl.BlockSpec((group, sources, num_tokens), lambda step, *_: (step // group, 0, 0)),
                      pl.BlockSpec((group, far, 128), lambda step, *_: (step // group, 0, 0)),
                      hbm] + [per_step(arr) for arr in weights] * 2,
            out_specs=[per_step(arr) for arr in weights],
            scratch_shapes=[pltpu.VMEM((far, num_tokens, width), BF16), pltpu.VMEM((far, num_tokens, width), BF16),
                            pltpu.VMEM((group, slots, width), BF16), pltpu.VMEM((group, slots, width), BF16),
                            pltpu.SMEM((group,), jnp.int32), pltpu.SemaphoreType.DMA((2, far))]),
        out_shape=[jax.ShapeDtypeStruct(arr.shape, F32) for arr in weights],
        compiler_params=pltpu.CompilerParams(vmem_limit_bytes=67_000_000, dimension_semantics=("arbitrary",)),
        cost_estimate=pl.CostEstimate(flops=280_000_000_000, bytes_accessed=225_000_000, transcendentals=0),
        name="expert_weight_grads",
    )(counts, place, positions, slot_gates, table, w_gate, w_up, w_down, *near_grads)


def rms_parts(x_f32):
    return lax.rsqrt(jnp.mean(x_f32 * x_f32, axis=-1, keepdims=True) + EPS)


def rms_back(x_f32, inv_rms, gain_row, d_out):
    d_gain = jnp.sum(d_out * x_f32 * inv_rms, axis=0, keepdims=True)
    d_scaled = d_out * gain_row
    d_x = inv_rms * d_scaled - x_f32 * inv_rms ** 3 * jnp.mean(d_scaled * x_f32, axis=-1, keepdims=True)
    return d_x, d_gain


def rope_tables(seq_len):
    half_dim = HEAD_DIM // 2
    lane = jnp.arange(HEAD_DIM, dtype=jnp.int32)
    inv_freq = ROPE_BASE ** (-(lane % half_dim).astype(F32) / half_dim)
    angles = jnp.arange(seq_len, dtype=F32)[:, None] * inv_freq[None, :]
    return jnp.cos(angles), jnp.where(lane < half_dim, -1.0, 1.0) * jnp.sin(angles)


def causal_probs(query, keys, start):
    scores = mat_nt(query, keys) * HEAD_DIM ** -0.5
    rows = lax.broadcasted_iota(jnp.int32, scores.shape, 0) + start
    scores = jnp.where(rows >= lax.broadcasted_iota(jnp.int32, scores.shape, 1), scores, -1e30)
    weights = jnp.exp(scores - jnp.max(scores, axis=1, keepdims=True))
    return weights / jnp.sum(weights, axis=1, keepdims=True)


def router_probs(rows, w_router_t):
    logits = mat_nt(w_router_t, rows)
    weights = jnp.exp(logits - jnp.max(logits, axis=0, keepdims=True))
    return weights / jnp.sum(weights, axis=0, keepdims=True)


def forward_kernel(num_seqs, x_ref, dy_ref, idx_ref, gain1_ref, gain2_ref, w_qkv_ref, w_out_ref, w_router_ref, cos_ref, sin_ref,
                   payload_ref, gates_ref, qkv_ref, context_ref, h_ref, x_scr, w_qkv_scr, w_out_scr, load_sem):
    num_tokens, width = x_ref.shape
    seq_len = num_tokens // num_seqs
    block = 256
    loads = [pltpu.make_async_copy(src, dst, load_sem.at[i]) for i, (src, dst) in enumerate([
        (x_ref, x_scr), (w_qkv_ref, w_qkv_scr), (w_out_ref, w_out_scr), (dy_ref, payload_ref.at[pl.ds(num_tokens, num_tokens)])])]
    for copy in loads:
        copy.start()
    loads[0].wait()
    x_ref = x_scr
    x_f32 = x_ref[...].astype(F32)
    normed1 = (x_f32 * rms_parts(x_f32) * gain1_ref[...].astype(F32)[None]).astype(BF16)
    loads[1].wait()
    for head_col in range(0, 3 * width, HEAD_DIM):
        vals = mat_nn(normed1, w_qkv_scr[:, head_col:head_col + HEAD_DIM])
        for seq in range(num_seqs):
            span = slice(seq * seq_len, (seq + 1) * seq_len)
            part = vals[span]
            if head_col < 2 * width:
                part = part * cos_ref[...] + pltpu.roll(part, HEAD_DIM // 2, 1) * sin_ref[...]
            qkv_ref[span, head_col:head_col + HEAD_DIM] = part.astype(BF16)
    for seq in range(num_seqs):
        for head in range(width // HEAD_DIM):
            cols = [slice(part * width + head * HEAD_DIM, part * width + (head + 1) * HEAD_DIM) for part in range(3)]
            for start in range(0, seq_len, block):
                rows = slice(seq * seq_len + start, seq * seq_len + start + block)
                seen = slice(seq * seq_len, seq * seq_len + start + block)
                probs = causal_probs(qkv_ref[rows, cols[0]], qkv_ref[seen, cols[1]], start).astype(BF16)
                context_ref[rows, cols[0]] = mat_nn(probs, qkv_ref[seen, cols[2]]).astype(BF16)
    loads[2].wait()
    h_rows = (x_f32 + mat_nn(context_ref[...], w_out_scr[...])).astype(BF16)
    h_ref[...] = h_rows
    h_f32 = h_rows.astype(F32)
    normed2 = (h_f32 * rms_parts(h_f32) * gain2_ref[...].astype(F32)[None]).astype(BF16)
    payload_ref[0:num_tokens] = normed2
    probs = router_probs(normed2, w_router_ref[...].T)
    expert_iota = lax.broadcasted_iota(jnp.int32, probs.shape, 0)
    picked = [jnp.sum(jnp.where(expert_iota == idx_ref[choice:choice + 1], probs, 0.0), axis=0, keepdims=True) for choice in range(idx_ref.shape[0])]
    total = functools.reduce(lambda a, b: a + b, picked)
    for choice, part in enumerate(picked):
        gates_ref[choice:choice + 1] = part / total
    loads[3].wait()


def dense_forward(x_rows, dy_rows, idx_cols, num_seqs, norm1_gain, norm2_gain, w_qkv, w_attn_out, w_router, tables):
    num_tokens, width = x_rows.shape
    rows = jax.ShapeDtypeStruct(x_rows.shape, BF16)
    hbm, vmem = pl.BlockSpec(memory_space=pl.ANY), pl.BlockSpec(memory_space=pltpu.VMEM)
    return pl.pallas_call(
        functools.partial(forward_kernel, num_seqs),
        in_specs=[hbm, hbm, vmem, vmem, vmem, hbm, hbm, vmem, vmem, vmem],
        scratch_shapes=[pltpu.VMEM(x_rows.shape, BF16), pltpu.VMEM(w_qkv.shape, BF16), pltpu.VMEM(w_attn_out.shape, BF16), pltpu.SemaphoreType.DMA((4,))],
        out_shape=[jax.ShapeDtypeStruct((2 * num_tokens, width), BF16), jax.ShapeDtypeStruct(idx_cols.shape, F32),
                   jax.ShapeDtypeStruct((num_tokens, 3 * width), BF16), rows, rows],
        compiler_params=pltpu.CompilerParams(vmem_limit_bytes=66_000_000),
        cost_estimate=pl.CostEstimate(flops=10_000_000_000, bytes_accessed=8_000_000, transcendentals=0),
        name="dense_forward",
    )(x_rows, dy_rows, idx_cols, norm1_gain, norm2_gain, w_qkv, w_attn_out, w_router, *tables)


def backward_kernel(num_seqs, x_ref, dy_ref, d_rows_ref, d_gates_ref, idx_ref, payload_ref, qkv_ref, context_ref, h_ref,
                    gain1_ref, gain2_ref, w_qkv_ref, w_out_ref, w_router_ref, cos_ref, sin_ref, d_x_ref, d_w_qkv_ref, d_w_out_ref, packed_ref, d_qkv_scr):
    num_tokens, width = x_ref.shape
    seq_len = num_tokens // num_seqs
    num_experts = w_router_ref.shape[1]
    block = 256
    normed2 = payload_ref[0:num_tokens]
    w_router_t = w_router_ref[...].T
    probs = router_probs(normed2, w_router_t)
    expert_iota = lax.broadcasted_iota(jnp.int32, probs.shape, 0)
    chosen = jnp.zeros(probs.shape, F32)
    d_gate = jnp.zeros(probs.shape, F32)
    for choice in range(idx_ref.shape[0]):
        hit = expert_iota == idx_ref[choice:choice + 1]
        chosen = jnp.where(hit, probs, chosen)
        d_gate = jnp.where(hit, d_gates_ref[choice:choice + 1], d_gate)
    total = jnp.sum(chosen, axis=0, keepdims=True)
    mixed = jnp.sum(d_gate * chosen, axis=0, keepdims=True) / total
    d_weighted = chosen * ((d_gate - mixed) / total)
    d_logits = (d_weighted - probs * jnp.sum(d_weighted, axis=0, keepdims=True)).astype(BF16)
    packed_ref[0:width] = mat_nn(d_logits, normed2).T
    d_normed2 = d_rows_ref[...] + mat_tn(d_logits, w_router_t)
    h_f32 = h_ref[...].astype(F32)
    d_h_part, d_gain2 = rms_back(h_f32, rms_parts(h_f32), gain2_ref[...].astype(F32)[None], d_normed2)
    d_h = (dy_ref[...].astype(F32) + d_h_part).astype(BF16)
    d_w_out_ref[...] = mat_tn(context_ref[...], d_h)
    d_context = mat_nt(d_h, w_out_ref[...]).astype(BF16)
    for seq in range(num_seqs):
        whole = slice(seq * seq_len, (seq + 1) * seq_len)
        for head in range(width // HEAD_DIM):
            cols = [slice(part * width + head * HEAD_DIM, part * width + (head + 1) * HEAD_DIM) for part in range(3)]
            d_key = jnp.zeros((seq_len, HEAD_DIM), F32)
            d_value = jnp.zeros((seq_len, HEAD_DIM), F32)
            for start in reversed(range(0, seq_len, block)):
                rows = slice(seq * seq_len + start, seq * seq_len + start + block)
                seen = slice(seq * seq_len, seq * seq_len + start + block)
                query, keys = qkv_ref[rows, cols[0]], qkv_ref[seen, cols[1]]
                weights = causal_probs(query, keys, start)
                d_out = d_context[rows, cols[0]]
                d_weights = mat_nt(d_out, qkv_ref[seen, cols[2]]).astype(BF16).astype(F32)
                d_scores = (weights * (d_weights - jnp.sum(weights * d_weights, axis=1, keepdims=True)) * HEAD_DIM ** -0.5).astype(BF16)
                d_query = mat_nn(d_scores, keys).astype(BF16).astype(F32)
                at = slice(start, start + block)
                d_query = d_query * cos_ref[at] - pltpu.roll(d_query, HEAD_DIM // 2, 1) * sin_ref[at]
                d_qkv_scr[rows, cols[0]] = d_query.astype(BF16)
                key_part, value_part = mat_tn(d_scores, query), mat_tn(weights.astype(BF16), d_out)
                if start + block == seq_len:
                    d_key, d_value = key_part, value_part
                else:
                    d_key = jnp.concatenate([d_key[:start + block] + key_part, d_key[start + block:]], axis=0)
                    d_value = jnp.concatenate([d_value[:start + block] + value_part, d_value[start + block:]], axis=0)
            d_key = d_key.astype(BF16).astype(F32)
            d_key = d_key * cos_ref[...] - pltpu.roll(d_key, HEAD_DIM // 2, 1) * sin_ref[...]
            d_qkv_scr[whole, cols[1]] = d_key.astype(BF16)
            d_qkv_scr[whole, cols[2]] = d_value.astype(BF16)
    d_qkv = d_qkv_scr[...]
    x_f32 = x_ref[...].astype(F32)
    inv_rms = rms_parts(x_f32)
    gain1 = gain1_ref[...].astype(F32)[None]
    d_w_qkv_ref[...] = mat_tn((x_f32 * inv_rms * gain1).astype(BF16), d_qkv)
    d_x_part, d_gain1 = rms_back(x_f32, inv_rms, gain1, mat_nt(d_qkv, w_qkv_ref[...]))
    d_x_ref[...] = (d_h.astype(F32) + d_x_part).astype(BF16)
    packed_ref[width:] = jnp.zeros((packed_ref.shape[0] - width, num_experts), F32)
    for row, d_gain in enumerate((d_gain1, d_gain2)):
        for part in range(width // num_experts):
            at = width + row * (width // num_experts) + part
            packed_ref[at:at + 1] = d_gain[:, part * num_experts:(part + 1) * num_experts]


def dense_backward(x_rows, dy_rows, d_rows, d_gates, idx_cols, saved, num_seqs, norm1_gain, norm2_gain, w_qkv, w_attn_out, w_router, tables):
    width = x_rows.shape[1]
    num_experts = w_router.shape[1]
    return pl.pallas_call(
        functools.partial(backward_kernel, num_seqs),
        out_shape=[jax.ShapeDtypeStruct(x_rows.shape, BF16), jax.ShapeDtypeStruct(w_qkv.shape, F32),
                   jax.ShapeDtypeStruct(w_attn_out.shape, F32), jax.ShapeDtypeStruct((width + 8 * pl.cdiv(2 * width, 8 * num_experts), num_experts), F32)],
        scratch_shapes=[pltpu.VMEM((x_rows.shape[0], 3 * width), BF16)],
        compiler_params=pltpu.CompilerParams(vmem_limit_bytes=48_000_000),
        cost_estimate=pl.CostEstimate(flops=15_000_000_000, bytes_accessed=12_000_000, transcendentals=0),
        name="dense_backward",
    )(x_rows, dy_rows, d_rows, d_gates, idx_cols, *saved, norm1_gain, norm2_gain, w_qkv, w_attn_out, w_router, *tables)


def unpack_kernel(width, d_w_qkv_ref, d_w_out_ref, packed_ref, d_w_qkv_out, d_w_out_out, d_w_router_out, gains_out):
    d_w_qkv_out[...] = d_w_qkv_ref[...]
    d_w_out_out[...] = d_w_out_ref[...]
    d_w_router_out[...] = packed_ref[0:width]
    lanes = packed_ref.shape[1]
    for row in range(2):
        for part in range(width // lanes):
            at = width + row * (width // lanes) + part
            gains_out[row:row + 1, part * lanes:(part + 1) * lanes] = packed_ref[at:at + 1]


def unpack(d_w_qkv, d_w_out, packed):
    width = d_w_out.shape[0]
    return pl.pallas_call(
        functools.partial(unpack_kernel, width),
        out_shape=[jax.ShapeDtypeStruct(d_w_qkv.shape, F32), jax.ShapeDtypeStruct(d_w_out.shape, F32),
                   jax.ShapeDtypeStruct((width, packed.shape[1]), F32), jax.ShapeDtypeStruct((2, width), F32)],
        name="unpack_grads",
    )(d_w_qkv, d_w_out, packed)


def solution(mesh):
    ep_size = mesh.shape['ep']
    tok_spec = P(('dp', 'ep'), None, None)
    rep_spec = P()
    exp_spec = P('ep', None, None)

    def local_step(x_tokens, dy_tokens, route_idx, norm1_gain, norm2_gain, w_qkv, w_attn_out, w_router, w_gate, w_up, w_down):
        num_seqs, seq_len, model_width = x_tokens.shape
        num_tokens = num_seqs * seq_len
        top_k = route_idx.shape[-1]
        local_experts = w_gate.shape[0]
        num_experts = local_experts * ep_size
        capacity = capacity_rows(num_tokens, top_k, num_experts)
        x_rows = x_tokens.reshape(num_tokens, model_width)
        dy_rows = dy_tokens.reshape(num_tokens, model_width)
        idx_cols = route_idx.reshape(num_tokens, top_k).T
        routes = idx_cols.astype(BF16).reshape(-1, model_width)
        near_part = jnp.concatenate([dy_rows, routes], axis=0)
        from_core, from_chip = [lax.ppermute(near_part, 'ep', [(i, i ^ k) for i in range(ep_size)]) for k in (1, 2)]
        from_far = lax.ppermute(from_chip, 'ep', [(i, i ^ 1) for i in range(ep_size)])
        dy_near = jnp.stack([near_part, from_core, from_chip, from_far])

        def expert_of(gathered):
            return gathered.reshape(-1, top_k, num_tokens).astype(jnp.int32) - lax.axis_index('ep') * local_experts

        idx_near = expert_of(dy_near[:, num_tokens:])
        positions_near = slot_positions(idx_near, local_experts, capacity)
        tables = rope_tables(seq_len)
        dense_weights = (num_seqs, norm1_gain, norm2_gain, w_qkv, w_attn_out, w_router, tables)
        payload, gate_vals, qkv_rows, context, h_rows = dense_forward(x_rows, dy_rows, idx_cols, *dense_weights)
        table = lax.all_gather(payload, ('dp', 'ep'))
        rows_near, gates_near = near_gather(payload, gate_vals, num_tokens)
        d_near, d_gate_near, slot_gates, *near_grads = token_grads(positions_near, idx_near, gates_near, rows_near, dy_near, w_gate, w_up, w_down, capacity)
        d_rows, d_gates, slot_gates_all, routes_all = near_return(d_near, d_gate_near, slot_gates, dy_near[:, num_tokens:], mesh.shape['dp'])
        slot_gates_all = slot_gates_all.transpose(1, 0, 2, 3).reshape(local_experts, -1, 128)
        d_x, *dense_grads = dense_backward(x_rows, dy_rows, d_rows, d_gates, idx_cols, (payload, qkv_rows, context, h_rows), *dense_weights)
        dense_grads, slot_gates_all = lax.optimization_barrier((dense_grads, slot_gates_all))
        positions = all_positions(expert_of(routes_all).transpose(1, 0, 2), local_experts, capacity)
        counts = (jnp.max(positions, axis=2) + 16) // 16 * 16
        place = jnp.stack([lax.axis_index('dp'), lax.axis_index('ep')]).astype(jnp.int32)
        expert_grads = weight_grads(positions, counts, place, slot_gates_all, table, w_gate, w_up, w_down, near_grads, capacity)
        d_w_qkv, d_w_out, d_w_router, gain_rows = unpack(*lax.psum(tuple(dense_grads), ('dp', 'ep')))
        dense_out = (gain_rows[0], gain_rows[1], d_w_qkv, d_w_out, d_w_router)
        return (d_x.reshape(x_tokens.shape),) + dense_out + tuple(expert_grads)

    return jax.shard_map(local_step, mesh=mesh,
                          in_specs=(tok_spec, tok_spec, tok_spec, rep_spec, rep_spec, rep_spec, rep_spec, rep_spec, exp_spec, exp_spec, exp_spec),
                          out_specs=(tok_spec, rep_spec, rep_spec, rep_spec, rep_spec, rep_spec, exp_spec, exp_spec, exp_spec),
                          check_vma=False)
```

```python
import functools

import jax
import jax.numpy as jnp
from jax import lax
from jax.experimental import pallas as pl
from jax.experimental.pallas import tpu as pltpu
from jax.sharding import PartitionSpec as P


F32 = jnp.float32
BF16 = jnp.bfloat16
EPS = 1e-6
HEAD_DIM = 128
ROPE_BASE = 10000.0


def capacity_rows(num_tokens, top_k, num_experts):
    return 8 * ((5 * num_tokens * top_k + 32 * num_experts - 1) // (32 * num_experts))


def slot_positions(local_idx, local_experts, capacity):
    num_tokens = local_idx.shape[-1]
    expert_ids = jnp.arange(local_experts, dtype=jnp.int32)
    member = jnp.any(local_idx[None] == expert_ids[:, None, None, None], axis=2)
    before = (jnp.arange(num_tokens)[:, None] < jnp.arange(num_tokens)[None, :]).astype(BF16)
    earlier = jnp.einsum('est,tv->esv', member.astype(BF16), before, preferred_element_type=F32)
    return jnp.where(member & (earlier < capacity), earlier.astype(jnp.int32), -1)


def mat_nn(left, right):
    return lax.dot_general(left, right, (((1,), (0,)), ((), ())), preferred_element_type=F32)


def mat_nt(left, right):
    return lax.dot_general(left, right, (((1,), (1,)), ((), ())), preferred_element_type=F32)


def mat_tn(left, right):
    return lax.dot_general(left, right, (((0,), (0,)), ((), ())), preferred_element_type=F32)


def swiglu_bwd(half_gate, act_up, d_hidden):
    twice_sig = 1.0 + jnp.tanh(half_gate)
    silu = half_gate * twice_sig
    hidden = (silu * act_up).astype(BF16)
    d_act_up = (d_hidden * silu).astype(BF16)
    twice_d_act_gate = (d_hidden * act_up * (twice_sig + silu * (2.0 - twice_sig))).astype(BF16)
    return hidden, twice_d_act_gate, d_act_up


def token_grad_kernel(capacity, group, f_tile, pos_ref, idx_ref, gate_ref, rows_ref, dy_ref, w_gate_ref, w_up_ref, w_down_ref,
                      d_rows_ref, d_gates_ref, slot_gate_ref, d_w_gate_ref, d_w_up_ref, d_w_down_ref,
                      select_scr, in_scr, raw_scr, dout_scr, din_scr):
    sources, num_tokens, _ = rows_ref.shape
    ff = w_gate_ref.shape[2]
    first = pl.program_id(0) * group
    slot_iota = lax.broadcasted_iota(jnp.int32, (capacity, num_tokens), 0)
    diagonal = lax.broadcasted_iota(jnp.int32, (capacity, 128), 0) == lax.broadcasted_iota(jnp.int32, (capacity, 128), 1)

    @pl.when(pl.program_id(0) == 0)
    def _():
        d_rows_ref[...] = jnp.zeros_like(d_rows_ref)
        d_gates_ref[...] = jnp.zeros_like(d_gates_ref)

    def select(source):
        selectors, gate_cols = [], []
        for member in range(group):
            hit = slot_iota == pos_ref[member, source:source + 1, :]
            gate_row = jnp.sum(jnp.where(idx_ref[source] == first + member, gate_ref[source], 0.0), axis=0, keepdims=True)
            gate_col = jnp.sum(jnp.where(hit, gate_row, 0.0), axis=1, keepdims=True)
            slot_gate_ref[member, source:source + 1, :] = jnp.sum(jnp.where(diagonal, gate_col, 0.0), axis=0, keepdims=True)
            gate_cols.append(gate_col)
            selectors.append(jnp.where(hit, 1.0, 0.0).astype(BF16))
        return jnp.concatenate(selectors, axis=0), jnp.concatenate(gate_cols, axis=0)

    ahead = select(0)
    for source in range(sources):
        selector, gate_col = ahead
        if source + 1 < sources:
            ahead = select(source + 1)
        select_scr[source] = selector
        slot_rows = mat_nn(selector, rows_ref[source]).astype(BF16)
        raw_dy = mat_nn(selector, dy_ref[source, :num_tokens])
        scaled_dy = (raw_dy * gate_col).astype(BF16)
        raw_dy = raw_dy.astype(BF16)
        for member in range(group):
            span = slice(source * capacity, (source + 1) * capacity)
            part = slice(member * capacity, (member + 1) * capacity)
            in_scr[member, span] = slot_rows[part]
            raw_scr[member, span] = raw_dy[part]
            dout_scr[member, span] = scaled_dy[part]

    def forward(member, cols):
        slot_rows = in_scr[member]
        half_w_gate = w_gate_ref[member, :, cols] * jnp.asarray(0.5, BF16)
        return (half_w_gate, mat_nn(slot_rows, half_w_gate), mat_nn(slot_rows, w_up_ref[member, :, cols]),
                mat_nt(dout_scr[member], w_down_ref[member, cols, :]))

    steps = [(member, slice(f, f + f_tile)) for member in range(group) for f in range(0, ff, f_tile)]
    ahead = forward(*steps[0])
    for at, (member, cols) in enumerate(steps):
        half_w_gate, half_gate, act_up, d_hidden = ahead
        if at + 1 < len(steps):
            ahead = forward(*steps[at + 1])
        hidden, twice_d_act_gate, d_act_up = swiglu_bwd(half_gate, act_up, d_hidden)
        out_part = mat_nn(hidden, w_down_ref[member, cols, :])
        in_part = mat_nt(twice_d_act_gate, half_w_gate) + mat_nt(d_act_up, w_up_ref[member, :, cols])
        d_w_gate_ref[member, :, cols] = 0.5 * mat_tn(in_scr[member], twice_d_act_gate)
        d_w_up_ref[member, :, cols] = mat_tn(in_scr[member], d_act_up)
        d_w_down_ref[member, cols, :] = mat_tn(hidden, dout_scr[member])
        out_sum, in_sum = (out_part, in_part) if cols.start == 0 else (out_sum + out_part, in_sum + in_part)
        if cols.stop == ff:
            d_gate = jnp.sum(raw_scr[member].astype(F32) * out_sum.astype(BF16).astype(F32), axis=1, keepdims=True)
            d_in = in_sum.astype(BF16)
            for source in range(sources):
                part = slice(source * capacity, (source + 1) * capacity)
                din_scr[source, member * capacity:(member + 1) * capacity] = d_in[part]
                hit = slot_iota == pos_ref[member, source:source + 1, :]
                d_gate_row = jnp.sum(jnp.where(hit, d_gate[part], 0.0), axis=0, keepdims=True)
                d_gates_ref[source] += jnp.where(idx_ref[source] == first + member, d_gate_row, 0.0)

    for source in range(sources):
        d_rows_ref[source] += mat_tn(select_scr[source], din_scr[source])


def token_grads(positions, local_idx, gates, rows, dy_rows, w_gate, w_up, w_down, capacity):
    group = 4
    sources, num_tokens, width = rows.shape
    num_experts = w_gate.shape[0]
    slots = sources * capacity

    def whole(arr):
        return pl.BlockSpec(arr.shape, lambda step: (0,) * arr.ndim, pipeline_mode=pl.Buffered(1))

    def per_step(arr):
        return pl.BlockSpec((group,) + arr.shape[1:], lambda step: (step, 0, 0))

    slot_gates = jax.ShapeDtypeStruct((num_experts, sources, 128), F32)
    weights = [jax.ShapeDtypeStruct(arr.shape, F32) for arr in (w_gate, w_up, w_down)]
    return pl.pallas_call(
        functools.partial(token_grad_kernel, capacity, group, 256),
        grid=(num_experts // group,),
        in_specs=[per_step(positions), whole(local_idx), whole(gates), whole(rows), whole(dy_rows),
                  per_step(w_gate), per_step(w_up), per_step(w_down)],
        out_specs=[pl.BlockSpec(rows.shape, lambda step: (0, 0, 0)), pl.BlockSpec(gates.shape, lambda step: (0, 0, 0)),
                   per_step(slot_gates)] + [per_step(arr) for arr in weights],
        out_shape=[jax.ShapeDtypeStruct(rows.shape, F32), jax.ShapeDtypeStruct(gates.shape, F32), slot_gates] + weights,
        scratch_shapes=[pltpu.VMEM((sources, group * capacity, num_tokens), BF16),
                        pltpu.VMEM((group, slots, width), BF16), pltpu.VMEM((group, slots, width), BF16),
                        pltpu.VMEM((group, slots, width), BF16), pltpu.VMEM((sources, group * capacity, width), BF16)],
        compiler_params=pltpu.CompilerParams(vmem_limit_bytes=64_000_000, dimension_semantics=("arbitrary",)),
        cost_estimate=pl.CostEstimate(flops=60_000_000_000, bytes_accessed=130_000_000, transcendentals=0),
        name="expert_token_grads",
    )(positions, local_idx, gates, rows, dy_rows, w_gate, w_up, w_down)


def near_peers():
    ep = lax.axis_index('ep')
    return {'ep': ep + 1 - 2 * lax.rem(ep, 2)}, {'ep': lax.rem(ep + 2, 4)}


def meet(peers):
    barrier = pltpu.get_barrier_semaphore()
    for peer in peers:
        pl.semaphore_signal(barrier, inc=1, device_id=peer, device_id_type=pl.DeviceIdType.MESH)
    pl.semaphore_wait(barrier, len(peers))


def remote(src, dst, send_sem, recv_sem, peer):
    return pltpu.make_async_remote_copy(src_ref=src, dst_ref=dst, send_sem=send_sem, recv_sem=recv_sem,
                                        device_id=peer, device_id_type=pl.DeviceIdType.MESH)


def near_gather_kernel(rows_ref, gates_ref, rows_out, gates_out, send_sem, recv_sem):
    core_peer, chip_peer = near_peers()
    meet((core_peer, chip_peer))
    num_tokens = rows_out.shape[1]
    half = num_tokens // 2
    pieces = [(rows_ref.at[pl.ds(0, half)], lambda slot: rows_out.at[slot, pl.ds(0, half)]),
              (rows_ref.at[pl.ds(half, half)], lambda slot: rows_out.at[slot, pl.ds(half, half)]),
              (gates_ref, lambda slot: gates_out.at[slot])]
    across = [remote(src, place(2), send_sem.at[0, i], recv_sem.at[0, i], chip_peer) for i, (src, place) in enumerate(pieces)]
    beside = [remote(src, place(1), send_sem.at[1, i], recv_sem.at[1, i], core_peer) for i, (src, place) in enumerate(pieces)]
    onward = [remote(place(2), place(3), send_sem.at[2, i], recv_sem.at[2, i], core_peer) for i, (_, place) in enumerate(pieces)]
    for copy in across + beside:
        copy.start()
    rows_out[0] = rows_ref[0:num_tokens]
    gates_out[0] = gates_ref[...]
    for copy, forward in zip(across, onward):
        copy.wait_recv()
        forward.start()
    for copy in beside + onward:
        copy.wait()
    for copy in across:
        copy.wait_send()


def near_gather(rows, gates, num_tokens):
    vmem = pl.BlockSpec(memory_space=pltpu.VMEM)
    return pl.pallas_call(
        near_gather_kernel,
        in_specs=[vmem, vmem], out_specs=[vmem, vmem],
        out_shape=[jax.ShapeDtypeStruct((4, num_tokens, rows.shape[1]), rows.dtype), jax.ShapeDtypeStruct((4,) + gates.shape, gates.dtype)],
        scratch_shapes=[pltpu.SemaphoreType.DMA((3, 3)), pltpu.SemaphoreType.DMA((3, 3))],
        compiler_params=pltpu.CompilerParams(collective_id=0, has_side_effects=True),
        cost_estimate=pl.CostEstimate(flops=10_000_000_000, bytes_accessed=10_000_000, transcendentals=0),
        name="near_gather",
    )(rows, gates)


def near_return_kernel(d_rows_ref, d_gates_ref, slot_gates_ref, routes_ref, rows_out, gates_out, slot_gates_out, routes_out,
                       own_rows, pass_rows, sum_rows, last_rows, own_gates, pass_gates, sum_gates, last_gates,
                       send_sem, recv_sem, far_send_sem, far_recv_sem):
    core_peer, chip_peer = near_peers()
    dp = lax.axis_index('dp')
    dp_size = slot_gates_out.shape[0] + 1
    far_peers = [{'dp': lax.rem(dp + k, dp_size)} for k in range(1, dp_size)]
    meet([core_peer, chip_peer] + far_peers)
    half = d_rows_ref.shape[1] // 2
    halves = [pl.ds(0, half), pl.ds(half, half)]
    far = [remote(slot_gates_ref, slot_gates_out.at[dp_size - 2 - k], far_send_sem.at[0, k], far_recv_sem.at[0, k], peer) for k, peer in enumerate(far_peers)]
    far += [remote(routes_ref, routes_out.at[dp_size - 1 - k], far_send_sem.at[1, k], far_recv_sem.at[1, k], peer) for k, peer in enumerate(far_peers)]
    first = [remote(d_rows_ref.at[3, span], pass_rows.at[span], send_sem.at[i], recv_sem.at[i], core_peer) for i, span in enumerate(halves)]
    first.append(remote(d_gates_ref.at[3], pass_gates, send_sem.at[2], recv_sem.at[2], core_peer))
    second = [remote(d_rows_ref.at[1], own_rows, send_sem.at[3], recv_sem.at[3], core_peer),
              remote(d_gates_ref.at[1], own_gates, send_sem.at[4], recv_sem.at[4], core_peer)]
    third = [remote(sum_rows.at[span], last_rows.at[span], send_sem.at[5 + i], recv_sem.at[5 + i], chip_peer) for i, span in enumerate(halves)]
    third.append(remote(sum_gates, last_gates, send_sem.at[7], recv_sem.at[7], chip_peer))
    for copy in first + second + far:
        copy.start()
    first[0].wait_recv()
    sum_rows[halves[0]] = d_rows_ref[2, halves[0]] + pass_rows[halves[0]]
    first[1].wait_recv()
    first[2].wait_recv()
    sum_gates[...] = d_gates_ref[2] + pass_gates[...]
    third[0].start()
    sum_rows[halves[1]] = d_rows_ref[2, halves[1]] + pass_rows[halves[1]]
    for copy in second:
        copy.wait_recv()
    rows_out[...] = d_rows_ref[0] + own_rows[...]
    gates_out[...] = d_gates_ref[0] + own_gates[...]
    third[1].start()
    third[2].start()
    routes_out[0] = routes_ref[...]
    for copy in third:
        copy.wait_recv()
    rows_out[...] += last_rows[...]
    gates_out[...] += last_gates[...]
    for copy in far:
        copy.wait()
    for copy in first + second + third:
        copy.wait_send()


def near_return(d_rows, d_gates, slot_gates, routes, dp_size):
    vmem = pl.BlockSpec(memory_space=pltpu.VMEM)
    rows = jax.ShapeDtypeStruct(d_rows.shape[1:], F32)
    gates = jax.ShapeDtypeStruct(d_gates.shape[1:], F32)
    return pl.pallas_call(
        near_return_kernel,
        in_specs=[vmem] * 4, out_specs=[vmem] * 4,
        out_shape=[rows, gates, jax.ShapeDtypeStruct((dp_size - 1,) + slot_gates.shape, F32), jax.ShapeDtypeStruct((dp_size,) + routes.shape, BF16)],
        scratch_shapes=[pltpu.VMEM(rows.shape, F32)] * 4 + [pltpu.VMEM(gates.shape, F32)] * 4
        + [pltpu.SemaphoreType.DMA((8,)), pltpu.SemaphoreType.DMA((8,)), pltpu.SemaphoreType.DMA((2, dp_size - 1)), pltpu.SemaphoreType.DMA((2, dp_size - 1))],
        compiler_params=pltpu.CompilerParams(collective_id=1, has_side_effects=True, vmem_limit_bytes=40_000_000),
        cost_estimate=pl.CostEstimate(flops=15_000_000_000, bytes_accessed=20_000_000, transcendentals=0),
        name="near_return",
    )(d_rows, d_gates, slot_gates, routes)


def position_kernel(capacity, num_experts, idx_ref, pos_ref, count_ref, member_scr):
    choices, sources, num_tokens = idx_ref.shape
    block = 256

    @pl.loop(0, num_experts)
    def _(expert):
        hit = idx_ref[0] == expert
        for choice in range(1, choices):
            hit = hit | (idx_ref[choice] == expert)
        member_scr[pl.ds(expert * sources, sources)] = jnp.where(hit, 1.0, 0.0).astype(BF16)

    before = jnp.where(lax.broadcasted_iota(jnp.int32, (num_tokens, num_tokens), 0) < lax.broadcasted_iota(jnp.int32, (num_tokens, num_tokens), 1), 1.0, 0.0).astype(BF16)

    @pl.loop(0, num_experts * sources // block)
    def _(step):
        span = pl.ds(pl.multiple_of(step * block, block), block)
        member = member_scr[span]
        earlier = mat_nn(member, before)
        held = jnp.minimum(earlier[:, num_tokens - 1:] + member[:, num_tokens - 1:].astype(F32), capacity).astype(jnp.int32)
        count_ref[span] = jnp.broadcast_to((held + 15) // 16 * 16, (block, 128))
        pos_ref[span] = jnp.where((member.astype(F32) > 0.5) & (earlier < capacity), earlier, -1.0).astype(jnp.int32)


def all_positions(idx_by_choice, num_experts, capacity):
    _, sources, num_tokens = idx_by_choice.shape
    flat, counts = pl.pallas_call(
        functools.partial(position_kernel, capacity, num_experts),
        out_shape=[jax.ShapeDtypeStruct((num_experts * sources, num_tokens), jnp.int32), jax.ShapeDtypeStruct((num_experts * sources, 128), jnp.int32)],
        scratch_shapes=[pltpu.VMEM((num_experts * sources, num_tokens), BF16)],
        compiler_params=pltpu.CompilerParams(vmem_limit_bytes=32_000_000),
        cost_estimate=pl.CostEstimate(flops=4_000_000_000, bytes_accessed=5_000_000, transcendentals=0),
        name="slot_positions",
    )(idx_by_choice)
    return flat.reshape(num_experts, sources, num_tokens), counts[:, 0].reshape(num_experts, sources)


def weight_grad_kernel(capacity, group, f_tile, near, chunks, tail, count_ref, place_ref, pos_ref, slot_gate_ref, table_hbm,
                       w_gate_ref, w_up_ref, w_down_ref, near_gate_ref, near_up_ref, near_down_ref,
                       d_w_gate_ref, d_w_up_ref, d_w_down_ref, rows_scr, dy_scr, in_scr, dout_scr, total_scr, load_sem):
    expert = pl.program_id(0)
    member = lax.rem(expert, group)
    far, num_tokens, _ = rows_scr.shape
    sources = far + near
    ff = w_gate_ref.shape[2]
    slot_iota = lax.broadcasted_iota(jnp.int32, (capacity, num_tokens), 0)
    diagonal = lax.broadcasted_iota(jnp.int32, (capacity, 128), 0) == lax.broadcasted_iota(jnp.int32, (capacity, 128), 1)

    def source_of(index):
        return lax.rem(place_ref[0] * near + near + index - lax.rem(index, near), sources) + jnp.bitwise_xor(lax.rem(index, near), place_ref[1])

    def loads(index):
        source = source_of(index)
        return (pltpu.make_async_copy(table_hbm.at[source, pl.ds(0, num_tokens)], rows_scr.at[index], load_sem.at[0, index]),
                pltpu.make_async_copy(table_hbm.at[source, pl.ds(num_tokens, num_tokens)], dy_scr.at[index], load_sem.at[1, index]))

    @pl.when(expert == 0)
    def _():
        @pl.loop(0, far)
        def _(index):
            for copy in loads(index):
                copy.start()

    def select(index):
        selectors, gate_cols = [], []
        for k in range(group):
            selectors.append(jnp.where(slot_iota == pos_ref[k, pl.ds(index + near, 1), :], 1.0, 0.0).astype(BF16))
            gate_cols.append(jnp.sum(jnp.where(diagonal, slot_gate_ref[k, pl.ds(index, 1), :], 0.0), axis=1, keepdims=True))
        return jnp.concatenate(selectors, axis=0), jnp.concatenate(gate_cols, axis=0)

    @pl.when(member == 0)
    def _():
        unroll = 7

        def body(step, starts):
            @pl.when(expert == 0)
            def _():
                for j in range(unroll):
                    for copy in loads(step * unroll + j):
                        copy.wait()

            ahead = select(step * unroll)
            for j in range(unroll):
                index = step * unroll + j
                selector, gate_col = ahead
                if j + 1 < unroll:
                    ahead = select(index + 1)
                slot_rows = mat_nn(selector, rows_scr[index]).astype(BF16)
                scaled_dy = (mat_nn(selector, dy_scr[index]) * gate_col).astype(BF16)
                for k in range(group):
                    span = pl.ds(pl.multiple_of(starts[k], 16), capacity)
                    part = slice(k * capacity, (k + 1) * capacity)
                    in_scr[k, span] = slot_rows[part]
                    dout_scr[k, span] = scaled_dy[part]
                starts = tuple(starts[k] + count_ref[expert + k, index + near] for k in range(group))
            return starts

        ends = lax.fori_loop(0, far // unroll, body, (jnp.int32(0),) * group)
        empty = jnp.zeros((tail, in_scr.shape[2]), BF16)
        for k in range(group):
            total_scr[k] = ends[k]
            span = pl.ds(pl.multiple_of(ends[k], 16), tail)
            in_scr[k, span] = empty
            dout_scr[k, span] = empty

            @pl.loop((ends[k] + tail - 1) // tail, sum(chunks) // tail)
            def _(block):
                span = pl.ds(pl.multiple_of(block * tail, tail), tail)
                in_scr[k, span] = empty
                dout_scr[k, span] = empty

    def forward(start, size, cols):
        slot_rows = in_scr[member, pl.ds(start, size)]
        d_out = dout_scr[member, pl.ds(start, size)]
        return (slot_rows, d_out, mat_nn(slot_rows, w_gate_ref[0, :, cols] * jnp.asarray(0.5, BF16)), mat_nn(slot_rows, w_up_ref[0, :, cols]),
                mat_nt(d_out, w_down_ref[0, cols, :]))

    def accumulate(steps):
        ahead = forward(*steps[0])
        for at, (start, _, cols) in enumerate(steps):
            slot_rows, d_out, half_gate, act_up, d_hidden = ahead
            if at + 1 < len(steps):
                ahead = forward(*steps[at + 1])
            hidden, twice_d_act_gate, d_act_up = swiglu_bwd(half_gate, act_up, d_hidden)
            gate_base, up_base = (near_gate_ref, near_up_ref) if start == 0 else (d_w_gate_ref, d_w_up_ref)
            d_w_gate_ref[0, :, cols] = gate_base[0, :, cols] + 0.5 * mat_tn(slot_rows, twice_d_act_gate)
            d_w_up_ref[0, :, cols] = up_base[0, :, cols] + mat_tn(slot_rows, d_act_up)
            d_w_down_ref[0, cols, :] = (near_down_ref if start == 0 else d_w_down_ref)[0, cols, :] + mat_tn(hidden, d_out)

    tiles = [slice(f, f + f_tile) for f in range(0, ff, f_tile)]
    accumulate([(sum(chunks[:c]), size, cols) for c, size in enumerate(chunks) for cols in tiles])

    @pl.when(total_scr[member] > sum(chunks))
    def _():
        for start in range(sum(chunks), far * capacity, tail):
            accumulate([(start, tail, cols) for cols in tiles])


def weight_grads(positions, counts, place, slot_gates, table, w_gate, w_up, w_down, near_grads, capacity):
    group = 4
    near = 4
    tail = 256
    sources, num_tokens = positions.shape[1:]
    width = table.shape[2]
    far = sources - near
    num_experts, _, _ = w_gate.shape
    chunks = (1024, 1024)
    slots = far * capacity + tail

    def per_step(arr):
        return pl.BlockSpec((1,) + arr.shape[1:], lambda step, *_: (step, 0, 0))

    hbm = pl.BlockSpec(memory_space=pl.ANY)
    weights = (w_gate, w_up, w_down)
    return pl.pallas_call(
        functools.partial(weight_grad_kernel, capacity, group, 256, near, chunks, tail),
        grid_spec=pltpu.PrefetchScalarGridSpec(
            num_scalar_prefetch=2, grid=(num_experts,),
            in_specs=[pl.BlockSpec((group, sources, num_tokens), lambda step, *_: (step // group, 0, 0)),
                      pl.BlockSpec((group, far, 128), lambda step, *_: (step // group, 0, 0)),
                      hbm] + [per_step(arr) for arr in weights] * 2,
            out_specs=[per_step(arr) for arr in weights],
            scratch_shapes=[pltpu.VMEM((far, num_tokens, width), BF16), pltpu.VMEM((far, num_tokens, width), BF16),
                            pltpu.VMEM((group, slots, width), BF16), pltpu.VMEM((group, slots, width), BF16),
                            pltpu.SMEM((group,), jnp.int32), pltpu.SemaphoreType.DMA((2, far))]),
        out_shape=[jax.ShapeDtypeStruct(arr.shape, F32) for arr in weights],
        compiler_params=pltpu.CompilerParams(vmem_limit_bytes=67_000_000, dimension_semantics=("arbitrary",)),
        cost_estimate=pl.CostEstimate(flops=280_000_000_000, bytes_accessed=225_000_000, transcendentals=0),
        name="expert_weight_grads",
    )(counts, place, positions, slot_gates, table, w_gate, w_up, w_down, *near_grads)


def rms_parts(x_f32):
    return lax.rsqrt(jnp.mean(x_f32 * x_f32, axis=-1, keepdims=True) + EPS)


def rms_back(x_f32, inv_rms, gain_row, d_out):
    d_gain = jnp.sum(d_out * x_f32 * inv_rms, axis=0, keepdims=True)
    d_scaled = d_out * gain_row
    d_x = inv_rms * d_scaled - x_f32 * inv_rms ** 3 * jnp.mean(d_scaled * x_f32, axis=-1, keepdims=True)
    return d_x, d_gain


def rope_tables(seq_len):
    half_dim = HEAD_DIM // 2
    lane = jnp.arange(HEAD_DIM, dtype=jnp.int32)
    inv_freq = ROPE_BASE ** (-(lane % half_dim).astype(F32) / half_dim)
    angles = jnp.arange(seq_len, dtype=F32)[:, None] * inv_freq[None, :]
    return jnp.cos(angles), jnp.where(lane < half_dim, -1.0, 1.0) * jnp.sin(angles)


def causal_probs(query, keys, start):
    scores = mat_nt(query, keys) * HEAD_DIM ** -0.5
    rows = lax.broadcasted_iota(jnp.int32, scores.shape, 0) + start
    scores = jnp.where(rows >= lax.broadcasted_iota(jnp.int32, scores.shape, 1), scores, -1e30)
    weights = jnp.exp(scores - jnp.max(scores, axis=1, keepdims=True))
    return weights / jnp.sum(weights, axis=1, keepdims=True)


def router_probs(rows, w_router_t):
    logits = mat_nt(w_router_t, rows)
    weights = jnp.exp(logits - jnp.max(logits, axis=0, keepdims=True))
    return weights / jnp.sum(weights, axis=0, keepdims=True)


def forward_kernel(num_seqs, x_ref, dy_ref, idx_ref, gain1_ref, gain2_ref, w_qkv_ref, w_out_ref, w_router_ref, cos_ref, sin_ref,
                   payload_ref, gates_ref, qkv_ref, context_ref, h_ref, x_scr, w_qkv_scr, w_out_scr, load_sem):
    num_tokens, width = x_ref.shape
    seq_len = num_tokens // num_seqs
    block = 256
    loads = [pltpu.make_async_copy(src, dst, load_sem.at[i]) for i, (src, dst) in enumerate([
        (x_ref, x_scr), (w_qkv_ref, w_qkv_scr), (w_out_ref, w_out_scr), (dy_ref, payload_ref.at[pl.ds(num_tokens, num_tokens)])])]
    for copy in loads:
        copy.start()
    loads[0].wait()
    x_ref = x_scr
    x_f32 = x_ref[...].astype(F32)
    normed1 = (x_f32 * rms_parts(x_f32) * gain1_ref[...].astype(F32)[None]).astype(BF16)
    loads[1].wait()
    for head_col in range(0, 3 * width, HEAD_DIM):
        vals = mat_nn(normed1, w_qkv_scr[:, head_col:head_col + HEAD_DIM])
        for seq in range(num_seqs):
            span = slice(seq * seq_len, (seq + 1) * seq_len)
            part = vals[span]
            if head_col < 2 * width:
                part = part * cos_ref[...] + pltpu.roll(part, HEAD_DIM // 2, 1) * sin_ref[...]
            qkv_ref[span, head_col:head_col + HEAD_DIM] = part.astype(BF16)
    for seq in range(num_seqs):
        for head in range(width // HEAD_DIM):
            cols = [slice(part * width + head * HEAD_DIM, part * width + (head + 1) * HEAD_DIM) for part in range(3)]
            for start in range(0, seq_len, block):
                rows = slice(seq * seq_len + start, seq * seq_len + start + block)
                seen = slice(seq * seq_len, seq * seq_len + start + block)
                probs = causal_probs(qkv_ref[rows, cols[0]], qkv_ref[seen, cols[1]], start).astype(BF16)
                context_ref[rows, cols[0]] = mat_nn(probs, qkv_ref[seen, cols[2]]).astype(BF16)
    loads[2].wait()
    h_rows = (x_f32 + mat_nn(context_ref[...], w_out_scr[...])).astype(BF16)
    h_ref[...] = h_rows
    h_f32 = h_rows.astype(F32)
    normed2 = (h_f32 * rms_parts(h_f32) * gain2_ref[...].astype(F32)[None]).astype(BF16)
    payload_ref[0:num_tokens] = normed2
    probs = router_probs(normed2, w_router_ref[...].T)
    expert_iota = lax.broadcasted_iota(jnp.int32, probs.shape, 0)
    picked = [jnp.sum(jnp.where(expert_iota == idx_ref[choice:choice + 1], probs, 0.0), axis=0, keepdims=True) for choice in range(idx_ref.shape[0])]
    total = functools.reduce(lambda a, b: a + b, picked)
    for choice, part in enumerate(picked):
        gates_ref[choice:choice + 1] = part / total
    loads[3].wait()


def dense_forward(x_rows, dy_rows, idx_cols, num_seqs, norm1_gain, norm2_gain, w_qkv, w_attn_out, w_router, tables):
    num_tokens, width = x_rows.shape
    rows = jax.ShapeDtypeStruct(x_rows.shape, BF16)
    hbm, vmem = pl.BlockSpec(memory_space=pl.ANY), pl.BlockSpec(memory_space=pltpu.VMEM)
    return pl.pallas_call(
        functools.partial(forward_kernel, num_seqs),
        in_specs=[hbm, hbm, vmem, vmem, vmem, hbm, hbm, vmem, vmem, vmem],
        scratch_shapes=[pltpu.VMEM(x_rows.shape, BF16), pltpu.VMEM(w_qkv.shape, BF16), pltpu.VMEM(w_attn_out.shape, BF16), pltpu.SemaphoreType.DMA((4,))],
        out_shape=[jax.ShapeDtypeStruct((2 * num_tokens, width), BF16), jax.ShapeDtypeStruct(idx_cols.shape, F32),
                   jax.ShapeDtypeStruct((num_tokens, 3 * width), BF16), rows, rows],
        compiler_params=pltpu.CompilerParams(vmem_limit_bytes=66_000_000),
        cost_estimate=pl.CostEstimate(flops=10_000_000_000, bytes_accessed=8_000_000, transcendentals=0),
        name="dense_forward",
    )(x_rows, dy_rows, idx_cols, norm1_gain, norm2_gain, w_qkv, w_attn_out, w_router, *tables)


def backward_kernel(num_seqs, x_ref, dy_ref, d_rows_ref, d_gates_ref, idx_ref, payload_ref, qkv_ref, context_ref, h_ref,
                    gain1_ref, gain2_ref, w_qkv_ref, w_out_ref, w_router_ref, cos_ref, sin_ref, d_x_ref, d_w_qkv_ref, d_w_out_ref, packed_ref, d_qkv_scr):
    num_tokens, width = x_ref.shape
    seq_len = num_tokens // num_seqs
    num_experts = w_router_ref.shape[1]
    block = 256
    normed2 = payload_ref[0:num_tokens]
    w_router_t = w_router_ref[...].T
    probs = router_probs(normed2, w_router_t)
    expert_iota = lax.broadcasted_iota(jnp.int32, probs.shape, 0)
    chosen = jnp.zeros(probs.shape, F32)
    d_gate = jnp.zeros(probs.shape, F32)
    for choice in range(idx_ref.shape[0]):
        hit = expert_iota == idx_ref[choice:choice + 1]
        chosen = jnp.where(hit, probs, chosen)
        d_gate = jnp.where(hit, d_gates_ref[choice:choice + 1], d_gate)
    total = jnp.sum(chosen, axis=0, keepdims=True)
    mixed = jnp.sum(d_gate * chosen, axis=0, keepdims=True) / total
    d_weighted = chosen * ((d_gate - mixed) / total)
    d_logits = (d_weighted - probs * jnp.sum(d_weighted, axis=0, keepdims=True)).astype(BF16)
    packed_ref[0:width] = mat_nn(d_logits, normed2).T
    d_normed2 = d_rows_ref[...] + mat_tn(d_logits, w_router_t)
    h_f32 = h_ref[...].astype(F32)
    d_h_part, d_gain2 = rms_back(h_f32, rms_parts(h_f32), gain2_ref[...].astype(F32)[None], d_normed2)
    d_h = (dy_ref[...].astype(F32) + d_h_part).astype(BF16)
    d_w_out_ref[...] = mat_tn(context_ref[...], d_h)
    d_context = mat_nt(d_h, w_out_ref[...]).astype(BF16)
    for seq in range(num_seqs):
        whole = slice(seq * seq_len, (seq + 1) * seq_len)
        for head in range(width // HEAD_DIM):
            cols = [slice(part * width + head * HEAD_DIM, part * width + (head + 1) * HEAD_DIM) for part in range(3)]
            d_key = jnp.zeros((seq_len, HEAD_DIM), F32)
            d_value = jnp.zeros((seq_len, HEAD_DIM), F32)
            for start in reversed(range(0, seq_len, block)):
                rows = slice(seq * seq_len + start, seq * seq_len + start + block)
                seen = slice(seq * seq_len, seq * seq_len + start + block)
                query, keys = qkv_ref[rows, cols[0]], qkv_ref[seen, cols[1]]
                weights = causal_probs(query, keys, start)
                d_out = d_context[rows, cols[0]]
                d_weights = mat_nt(d_out, qkv_ref[seen, cols[2]]).astype(BF16).astype(F32)
                d_scores = (weights * (d_weights - jnp.sum(weights * d_weights, axis=1, keepdims=True)) * HEAD_DIM ** -0.5).astype(BF16)
                d_query = mat_nn(d_scores, keys).astype(BF16).astype(F32)
                at = slice(start, start + block)
                d_query = d_query * cos_ref[at] - pltpu.roll(d_query, HEAD_DIM // 2, 1) * sin_ref[at]
                d_qkv_scr[rows, cols[0]] = d_query.astype(BF16)
                key_part, value_part = mat_tn(d_scores, query), mat_tn(weights.astype(BF16), d_out)
                if start + block == seq_len:
                    d_key, d_value = key_part, value_part
                else:
                    d_key = jnp.concatenate([d_key[:start + block] + key_part, d_key[start + block:]], axis=0)
                    d_value = jnp.concatenate([d_value[:start + block] + value_part, d_value[start + block:]], axis=0)
            d_key = d_key.astype(BF16).astype(F32)
            d_key = d_key * cos_ref[...] - pltpu.roll(d_key, HEAD_DIM // 2, 1) * sin_ref[...]
            d_qkv_scr[whole, cols[1]] = d_key.astype(BF16)
            d_qkv_scr[whole, cols[2]] = d_value.astype(BF16)
    d_qkv = d_qkv_scr[...]
    x_f32 = x_ref[...].astype(F32)
    inv_rms = rms_parts(x_f32)
    gain1 = gain1_ref[...].astype(F32)[None]
    d_w_qkv_ref[...] = mat_tn((x_f32 * inv_rms * gain1).astype(BF16), d_qkv)
    d_x_part, d_gain1 = rms_back(x_f32, inv_rms, gain1, mat_nt(d_qkv, w_qkv_ref[...]))
    d_x_ref[...] = (d_h.astype(F32) + d_x_part).astype(BF16)
    packed_ref[width:] = jnp.zeros((packed_ref.shape[0] - width, num_experts), F32)
    for row, d_gain in enumerate((d_gain1, d_gain2)):
        for part in range(width // num_experts):
            at = width + row * (width // num_experts) + part
            packed_ref[at:at + 1] = d_gain[:, part * num_experts:(part + 1) * num_experts]


def dense_backward(x_rows, dy_rows, d_rows, d_gates, idx_cols, saved, num_seqs, norm1_gain, norm2_gain, w_qkv, w_attn_out, w_router, tables):
    width = x_rows.shape[1]
    num_experts = w_router.shape[1]
    return pl.pallas_call(
        functools.partial(backward_kernel, num_seqs),
        out_shape=[jax.ShapeDtypeStruct(x_rows.shape, BF16), jax.ShapeDtypeStruct(w_qkv.shape, F32),
                   jax.ShapeDtypeStruct(w_attn_out.shape, F32), jax.ShapeDtypeStruct((width + 8 * pl.cdiv(2 * width, 8 * num_experts), num_experts), F32)],
        scratch_shapes=[pltpu.VMEM((x_rows.shape[0], 3 * width), BF16)],
        compiler_params=pltpu.CompilerParams(vmem_limit_bytes=48_000_000),
        cost_estimate=pl.CostEstimate(flops=15_000_000_000, bytes_accessed=12_000_000, transcendentals=0),
        name="dense_backward",
    )(x_rows, dy_rows, d_rows, d_gates, idx_cols, *saved, norm1_gain, norm2_gain, w_qkv, w_attn_out, w_router, *tables)


def unpack_kernel(width, d_w_qkv_ref, d_w_out_ref, packed_ref, d_w_qkv_out, d_w_out_out, d_w_router_out, gains_out):
    d_w_qkv_out[...] = d_w_qkv_ref[...]
    d_w_out_out[...] = d_w_out_ref[...]
    d_w_router_out[...] = packed_ref[0:width]
    lanes = packed_ref.shape[1]
    for row in range(2):
        for part in range(width // lanes):
            at = width + row * (width // lanes) + part
            gains_out[row:row + 1, part * lanes:(part + 1) * lanes] = packed_ref[at:at + 1]


def unpack(d_w_qkv, d_w_out, packed):
    width = d_w_out.shape[0]
    return pl.pallas_call(
        functools.partial(unpack_kernel, width),
        out_shape=[jax.ShapeDtypeStruct(d_w_qkv.shape, F32), jax.ShapeDtypeStruct(d_w_out.shape, F32),
                   jax.ShapeDtypeStruct((width, packed.shape[1]), F32), jax.ShapeDtypeStruct((2, width), F32)],
        name="unpack_grads",
    )(d_w_qkv, d_w_out, packed)


def solution(mesh):
    ep_size = mesh.shape['ep']
    tok_spec = P(('dp', 'ep'), None, None)
    rep_spec = P()
    exp_spec = P('ep', None, None)

    def local_step(x_tokens, dy_tokens, route_idx, norm1_gain, norm2_gain, w_qkv, w_attn_out, w_router, w_gate, w_up, w_down):
        num_seqs, seq_len, model_width = x_tokens.shape
        num_tokens = num_seqs * seq_len
        top_k = route_idx.shape[-1]
        local_experts = w_gate.shape[0]
        num_experts = local_experts * ep_size
        capacity = capacity_rows(num_tokens, top_k, num_experts)
        x_rows = x_tokens.reshape(num_tokens, model_width)
        dy_rows = dy_tokens.reshape(num_tokens, model_width)
        idx_cols = route_idx.reshape(num_tokens, top_k).T
        routes = idx_cols.astype(BF16).reshape(-1, model_width)
        near_part = jnp.concatenate([dy_rows, routes], axis=0)
        from_core, from_chip = [lax.ppermute(near_part, 'ep', [(i, i ^ k) for i in range(ep_size)]) for k in (1, 2)]
        from_far = lax.ppermute(from_chip, 'ep', [(i, i ^ 1) for i in range(ep_size)])
        dy_near = jnp.stack([near_part, from_core, from_chip, from_far])

        def expert_of(gathered):
            return gathered.reshape(-1, top_k, num_tokens).astype(jnp.int32) - lax.axis_index('ep') * local_experts

        idx_near = expert_of(dy_near[:, num_tokens:])
        positions_near = slot_positions(idx_near, local_experts, capacity)
        tables = rope_tables(seq_len)
        dense_weights = (num_seqs, norm1_gain, norm2_gain, w_qkv, w_attn_out, w_router, tables)
        payload, gate_vals, qkv_rows, context, h_rows = dense_forward(x_rows, dy_rows, idx_cols, *dense_weights)
        table = lax.all_gather(payload, ('dp', 'ep'))
        rows_near, gates_near = near_gather(payload, gate_vals, num_tokens)
        d_near, d_gate_near, slot_gates, *near_grads = token_grads(positions_near, idx_near, gates_near, rows_near, dy_near, w_gate, w_up, w_down, capacity)
        d_rows, d_gates, slot_gates_all, routes_all = near_return(d_near, d_gate_near, slot_gates, dy_near[:, num_tokens:], mesh.shape['dp'])
        slot_gates_all = slot_gates_all.transpose(1, 0, 2, 3).reshape(local_experts, -1, 128)
        d_x, *dense_grads = dense_backward(x_rows, dy_rows, d_rows, d_gates, idx_cols, (payload, qkv_rows, context, h_rows), *dense_weights)
        dense_grads, slot_gates_all = lax.optimization_barrier((dense_grads, slot_gates_all))
        positions, counts = all_positions(expert_of(routes_all).transpose(1, 0, 2), local_experts, capacity)
        place = jnp.stack([lax.axis_index('dp'), lax.axis_index('ep')]).astype(jnp.int32)
        expert_grads = weight_grads(positions, counts, place, slot_gates_all, table, w_gate, w_up, w_down, near_grads, capacity)
        d_w_qkv, d_w_out, d_w_router, gain_rows = unpack(*lax.psum(tuple(dense_grads), ('dp', 'ep')))
        dense_out = (gain_rows[0], gain_rows[1], d_w_qkv, d_w_out, d_w_router)
        return (d_x.reshape(x_tokens.shape),) + dense_out + tuple(expert_grads)

    return jax.shard_map(local_step, mesh=mesh,
                          in_specs=(tok_spec, tok_spec, tok_spec, rep_spec, rep_spec, rep_spec, rep_spec, rep_spec, exp_spec, exp_spec, exp_spec),
                          out_specs=(tok_spec, rep_spec, rep_spec, rep_spec, rep_spec, rep_spec, exp_spec, exp_spec, exp_spec),
                          check_vma=False)
```
